32 devices in a mesh: dp: 16 (over z, y, x), mp: 2 (over core).
Axes of the slice: x: 2, y: 2, z: 4, core: 2. Of those that a mesh axis runs over, the one named last changes fastest.
Arguments:
- tokens: bfloat16 [100864, 384], P(('dp', 'mp')), may hold values from -6 to 6
- w_query: bfloat16 [384, 384], P('dp', 'mp'), may hold values from -0.3125 to 0.3125
- w_key: bfloat16 [384, 384], P('dp', 'mp'), may hold values from -0.3125 to 0.3125
- w_value: bfloat16 [384, 384], P('dp', 'mp'), may hold values from -0.3125 to 0.3125
- w_out: bfloat16 [384, 384], P('mp', 'dp'), may hold values from -1.25 to 1.25
- w_up: bfloat16 [384, 1536], P('dp', 'mp'), may hold values from -0.3125 to 0.3125
- w_down: bfloat16 [1536, 384], P('mp', 'dp'), may hold values from -0.3125 to 0.3125
- ln1_gain: bfloat16 [384], P('dp'), may hold values from 0.5 to 1.5
- ln1_bias: bfloat16 [384], P('dp'), may hold values from -3 to 3
- b_query: bfloat16 [384], P('dp'), may hold values from -3 to 3
- b_value: bfloat16 [384], P('dp'), may hold values from -3 to 3
- b_out: bfloat16 [384], P('dp'), may hold values from -3 to 3
- ln2_gain: bfloat16 [384], P('dp'), may hold values from 0.5 to 1.5
- ln2_bias: bfloat16 [384], P('dp'), may hold values from -3 to 3
- b_up: bfloat16 [1536], P('dp'), may hold values from -3 to 3
- b_down: bfloat16 [384], P('dp'), may hold values from -3 to 3
- cotangent: bfloat16 [100864, 384], P(('dp', 'mp')), may hold values from -6 to 6
Outputs:
- out: bfloat16 [100864, 384], P(('dp', 'mp'))
- grad_tokens: float32 [100864, 384], P(('dp', 'mp'))
- grad_w_query: float32 [384, 384], P('dp', 'mp')
- grad_w_key: float32 [384, 384], P('dp', 'mp')
- grad_w_value: float32 [384, 384], P('dp', 'mp')
- grad_w_out: float32 [384, 384], P('mp', 'dp')
- grad_w_up: float32 [384, 1536], P('dp', 'mp')
- grad_w_down: float32 [1536, 384], P('mp', 'dp')
- grad_ln1_gain: float32 [384], P(('dp', 'mp'))
- grad_ln1_bias: float32 [384], P(('dp', 'mp'))
- grad_b_query: float32 [384], P(('dp', 'mp'))
- grad_b_value: float32 [384], P(('dp', 'mp'))
- grad_b_out: float32 [384], P(('dp', 'mp'))
- grad_ln2_gain: float32 [384], P(('dp', 'mp'))
- grad_ln2_bias: float32 [384], P(('dp', 'mp'))
- grad_b_up: float32 [1536], P(('dp', 'mp'))
- grad_b_down: float32 [384], P(('dp', 'mp'))
The draws below stay inside these ranges and needn't reach their ends.
All inputs are finite; a program needn't handle non-finite values.
Results may differ from the reference program's by a relative error of at most 0.012.
Values may be sent and summed in bfloat16 or wider, within the bound.
A program may use at most 256 MiB of HBM per device.

```python
import math
import jax
import jax.numpy as jnp
from jax import lax

D = 384
HEADS = 6
HD = 64
FF = 1536
S = 197
IMG_BLK = 4
TOKENS = 100864


def draw_ln1_gain(key, part):
    values = jnp.clip(1.0 + 0.15 * jax.random.normal(key, (D,), jnp.float32), 0.5, 1.5)
    return values.astype(jnp.bfloat16)


def strengthened(result, rng, source, target, parts, factor):
    owner, partner = [(jnp.arange(result.shape[axis_at]) // (result.shape[axis_at] // parts)).reshape([-1 if axis == axis_at else 1 for axis in range(result.ndim)]) for axis_at in (source, target)]
    chosen = jax.random.permutation(rng, parts)[partner]
    strong = (owner == chosen) | (owner == (partner + parts // 2) % parts)
    return jnp.where(strong, factor * result, result)


def steps_of(rng, shape, split, smallest, largest):
    def one(position, blocks):
        steps = jax.random.uniform(jax.random.fold_in(jax.random.fold_in(rng, 6), position), (blocks,), jnp.float32, smallest / len(split), largest / len(split))
        return jnp.repeat(jnp.exp(steps), shape[position] // blocks).reshape((-1,) + (1,) * (len(shape) - position - 1))

    gain = one(*split[0])
    for cut in split[1:]:
        gain = gain * one(*cut)
    return gain


def gaussian(key, shape, width, limit, shards=(), held_as=jnp.bfloat16):
    entries = jax.random.normal(key, shape, jnp.float32) * width
    if len(shards) > 0:
        entries = steps_of(key, shape, shards, -0.22, 0.18) * entries
    return jnp.clip(entries, min=-limit, max=limit).astype(held_as)


def noise_with(rng, dims, scale, most, pieces, heavy, held_as=jnp.bfloat16):
    entries = scale * jax.random.normal(rng, dims, jnp.float32)
    if pieces:
        entries = entries * steps_of(rng, dims, pieces, -0.22, 0.18)
    return jnp.clip(strengthened(entries, jax.random.fold_in(rng, 3), *heavy), -most, most).astype(held_as)


def setup_inputs(seed: int = 0) -> dict:
    arg_keys = jax.random.split(jax.random.key(seed), 18)
    return {
        "tokens": noise_with(arg_keys[0], (TOKENS, D), 1.0, 6.0, ((0, 32),), (0, 1, 32, 2.75)),
        "w_query": gaussian(arg_keys[1], (D, D), D ** -0.5, 0.3125, ((0, 16), (1, 2))),
        "w_key": gaussian(arg_keys[2], (D, D), D ** -0.5, 0.3125, ((0, 16), (1, 2))),
        "w_value": gaussian(arg_keys[3], (D, D), D ** -0.5, 0.3125, ((0, 16), (1, 2))),
        "w_out": gaussian(arg_keys[4], (D, D), (D // 14) ** -0.5, 1.25, ((0, 2), (1, 16))),
        "w_up": gaussian(arg_keys[5], (D, FF), D ** -0.5, 0.3125, ((0, 16), (1, 2))),
        "w_down": gaussian(arg_keys[6], (FF, D), (FF // 4) ** -0.5, 0.3125, ((0, 2), (1, 16))),
        "ln1_gain": draw_ln1_gain(jax.random.fold_in(arg_keys[17], 71), 0),
        "ln1_bias": gaussian(arg_keys[8], (D,), 0.3, 3.0, ((0, 16),)),
        "b_query": gaussian(arg_keys[9], (D,), 0.5, 3.0, ((0, 16),)),
        "b_value": gaussian(arg_keys[10], (D,), 0.5, 3.0, ((0, 16),)),
        "b_out": gaussian(arg_keys[11], (D,), 0.5, 3.0, ((0, 16),)),
        "ln2_gain": jnp.clip(1.0 + 0.1 * jax.random.normal(arg_keys[12], (D,), jnp.float32), 0.5, 1.5).astype(jnp.bfloat16),
        "ln2_bias": gaussian(arg_keys[13], (D,), 0.3, 3.0, ((0, 16),)),
        "b_up": gaussian(arg_keys[14], (FF,), 0.5, 3.0, ((0, 16),)),
        "b_down": gaussian(arg_keys[15], (D,), 0.5, 3.0, ((0, 16),)),
        "cotangent": noise_with(arg_keys[16], (TOKENS, D), 1.0, 6.0, ((0, 32),), (0, 1, 32, 2.75)),
    }


epsilon = 1e-06
inv_root_two = 0.7071067811865476
inv_root_tau = 0.3989422804014327

def norm_forward(values, gain_row, shift_row):
    row_mean = lax.optimization_barrier(jnp.mean(values, axis=-1, keepdims=True))
    centred = values - row_mean
    variance = lax.optimization_barrier(jnp.mean(centred * centred, axis=-1, keepdims=True))
    inv_std = lax.rsqrt(variance + epsilon)
    normed = centred * inv_std
    return (normed, inv_std, normed * gain_row + shift_row)

def norm_backward(grad_out, normed, inv_std, gain_row):
    scaled = grad_out * gain_row
    return inv_std * (scaled - lax.optimization_barrier(jnp.mean(scaled, axis=-1, keepdims=True)) - normed * lax.optimization_barrier(jnp.mean(scaled * normed, axis=-1, keepdims=True)))

def gelu_value(pre_act):
    return 0.5 * pre_act * (1.0 + jax.scipy.special.erf(pre_act * inv_root_two))

def gelu_slope(pre_act):
    return 0.5 * (1.0 + jax.scipy.special.erf(pre_act * inv_root_two)) + pre_act * jnp.exp(-0.5 * pre_act * pre_act) * inv_root_tau

def attend(query_rows, key_rows, value_rows):
    score_scale = 1.0 / math.sqrt(query_rows.shape[-1])
    scores = jnp.einsum('bqhd,bkhd->bhqk', query_rows.astype(jnp.float32), key_rows.astype(jnp.float32)) * score_scale
    row_max = lax.optimization_barrier(jnp.max(scores, axis=-1, keepdims=True))
    log_total = row_max + jnp.log(lax.optimization_barrier(jnp.sum(jnp.exp(scores - row_max), axis=-1, keepdims=True)))
    attn_probs = lax.optimization_barrier(jnp.exp(scores - log_total).astype(jnp.bfloat16)).astype(jnp.float32)
    mixed_rows = jnp.einsum('bhqk,bkhd->bqhd', attn_probs, value_rows.astype(jnp.float32)).astype(jnp.bfloat16)
    return (mixed_rows, log_total[..., 0])

def attend_back(query_rows, key_rows, value_rows, log_total, grad_mixed):
    score_scale = 1.0 / math.sqrt(query_rows.shape[-1])
    query_f = query_rows.astype(jnp.float32)
    key_f = key_rows.astype(jnp.float32)
    grad_f = grad_mixed.astype(jnp.float32)
    scores = jnp.einsum('bqhd,bkhd->bhqk', query_f, key_f) * score_scale
    attn_probs = jnp.exp(scores - log_total[..., None])
    prob_rows = lax.optimization_barrier(attn_probs.astype(jnp.bfloat16)).astype(jnp.float32)
    grad_value = jnp.einsum('bhqk,bqhd->bkhd', prob_rows, grad_f)
    grad_probs = jnp.einsum('bqhd,bkhd->bhqk', grad_f, value_rows.astype(jnp.float32))
    row_delta = lax.optimization_barrier(jnp.sum(attn_probs * grad_probs, axis=-1, keepdims=True))
    grad_scores = lax.optimization_barrier((attn_probs * (grad_probs - row_delta) * score_scale).astype(jnp.bfloat16)).astype(jnp.float32)
    grad_query = jnp.einsum('bhqk,bkhd->bqhd', grad_scores, key_f)
    grad_key = jnp.einsum('bhqk,bqhd->bkhd', grad_scores, query_f)
    return (grad_query, grad_key, grad_value)

def reference(tokens, w_query, w_key, w_value, w_out, w_up, w_down, ln1_gain, ln1_bias, b_query, b_value, b_out, ln2_gain, ln2_bias, b_up, b_down, cotangent):
    gain_one = ln1_gain.astype(jnp.float32)
    shift_one = ln1_bias.astype(jnp.float32)
    gain_two = ln2_gain.astype(jnp.float32)
    shift_two = ln2_bias.astype(jnp.float32)
    bias_query = b_query.astype(jnp.float32)
    bias_value = b_value.astype(jnp.float32)
    bias_out = b_out.astype(jnp.float32)
    bias_up = b_up.astype(jnp.float32)
    bias_down = b_down.astype(jnp.float32)
    rows_blk = IMG_BLK * S
    blocks = TOKENS // rows_blk

    def view(rows):
        return rows.reshape(IMG_BLK, S, HEADS, HD)

    def one_block(totals, inputs):
        tok_blk, cot_blk = inputs
        tok_f = tok_blk.astype(jnp.float32)
        normed_one, inv_one, pre_one = norm_forward(tok_f, gain_one, shift_one)
        normed_rows = pre_one.astype(jnp.bfloat16)
        query_rows = (jnp.dot(normed_rows, w_query, preferred_element_type=jnp.float32) + bias_query).astype(jnp.bfloat16)
        key_rows = jnp.dot(normed_rows, w_key, preferred_element_type=jnp.float32).astype(jnp.bfloat16)
        value_rows = (jnp.dot(normed_rows, w_value, preferred_element_type=jnp.float32) + bias_value).astype(jnp.bfloat16)
        mixed_heads, log_total = attend(view(query_rows), view(key_rows), view(value_rows))
        mixed_rows = mixed_heads.reshape(rows_blk, D)
        resid_one = tok_f + jnp.dot(mixed_rows, w_out, preferred_element_type=jnp.float32) + bias_out
        normed_two, inv_two, pre_two = norm_forward(resid_one, gain_two, shift_two)
        hidden_in = pre_two.astype(jnp.bfloat16)
        pre_act = jnp.dot(hidden_in, w_up, preferred_element_type=jnp.float32) + bias_up
        active = gelu_value(pre_act).astype(jnp.bfloat16)
        block_out = resid_one + jnp.dot(active, w_down, preferred_element_type=jnp.float32) + bias_down
        grad_top = cot_blk.astype(jnp.float32)
        grad_active = jnp.dot(cot_blk, w_down.T, preferred_element_type=jnp.float32)
        grad_pre = grad_active * gelu_slope(pre_act)
        grad_pre_rows = grad_pre.astype(jnp.bfloat16)
        grad_hidden = jnp.dot(grad_pre_rows, w_up.T, preferred_element_type=jnp.float32)
        grad_resid = grad_top + norm_backward(grad_hidden, normed_two, inv_two, gain_two)
        grad_resid_rows = grad_resid.astype(jnp.bfloat16)
        grad_mixed = jnp.dot(grad_resid_rows, w_out.T, preferred_element_type=jnp.float32).astype(jnp.bfloat16)
        grad_query, grad_key, grad_value = attend_back(view(query_rows), view(key_rows), view(value_rows), log_total, view(grad_mixed))
        grad_query = grad_query.reshape(rows_blk, D)
        grad_key = grad_key.reshape(rows_blk, D)
        grad_value = grad_value.reshape(rows_blk, D)
        query_grad_rows = grad_query.astype(jnp.bfloat16)
        key_grad_rows = grad_key.astype(jnp.bfloat16)
        value_grad_rows = grad_value.astype(jnp.bfloat16)
        grad_normed = jnp.dot(query_grad_rows, w_query.T, preferred_element_type=jnp.float32) + jnp.dot(key_grad_rows, w_key.T, preferred_element_type=jnp.float32) + jnp.dot(value_grad_rows, w_value.T, preferred_element_type=jnp.float32)
        grad_input = grad_resid + norm_backward(grad_normed, normed_one, inv_one, gain_one)
        terms = (jnp.dot(normed_rows.T, query_grad_rows, preferred_element_type=jnp.float32), jnp.dot(normed_rows.T, key_grad_rows, preferred_element_type=jnp.float32), jnp.dot(normed_rows.T, value_grad_rows, preferred_element_type=jnp.float32), jnp.dot(mixed_rows.T, grad_resid_rows, preferred_element_type=jnp.float32), jnp.dot(hidden_in.T, grad_pre_rows, preferred_element_type=jnp.float32), jnp.dot(active.T, cot_blk, preferred_element_type=jnp.float32), lax.optimization_barrier(jnp.sum(grad_normed * normed_one, axis=0)), lax.optimization_barrier(jnp.sum(grad_normed, axis=0)), lax.optimization_barrier(jnp.sum(grad_query, axis=0)), lax.optimization_barrier(jnp.sum(grad_value, axis=0)), lax.optimization_barrier(jnp.sum(grad_resid, axis=0)), lax.optimization_barrier(jnp.sum(grad_hidden * normed_two, axis=0)), lax.optimization_barrier(jnp.sum(grad_hidden, axis=0)), lax.optimization_barrier(jnp.sum(grad_pre, axis=0)), lax.optimization_barrier(jnp.sum(grad_top, axis=0)))
        totals = tuple((total + term for total, term in zip(totals, terms)))
        return (totals, (block_out.astype(jnp.bfloat16), grad_input))
    init = (jnp.zeros((D, D), jnp.float32), jnp.zeros((D, D), jnp.float32), jnp.zeros((D, D), jnp.float32), jnp.zeros((D, D), jnp.float32), jnp.zeros((D, FF), jnp.float32), jnp.zeros((FF, D), jnp.float32), jnp.zeros((D,), jnp.float32), jnp.zeros((D,), jnp.float32), jnp.zeros((D,), jnp.float32), jnp.zeros((D,), jnp.float32), jnp.zeros((D,), jnp.float32), jnp.zeros((D,), jnp.float32), jnp.zeros((D,), jnp.float32), jnp.zeros((FF,), jnp.float32), jnp.zeros((D,), jnp.float32))
    totals, outputs = lax.scan(one_block, init, (tokens.reshape(blocks, rows_blk, D), cotangent.reshape(blocks, rows_blk, D)))
    out_blocks, grad_blocks = outputs
    return (out_blocks.reshape(TOKENS, D), grad_blocks.reshape(TOKENS, D), totals[0], totals[1], totals[2], totals[3], totals[4], totals[5], totals[6], totals[7], totals[8], totals[9], totals[10], totals[11], totals[12], totals[13], totals[14])
```

```python
import functools
import math

import jax
import jax.numpy as jnp
from jax import lax
from jax.experimental import pallas as pl
from jax.experimental.pallas import tpu as pltpu
from jax.sharding import PartitionSpec as P

D = 384
HD = 64
FF = 1536
S = 197
HEADS = D // HD
PAIRS = HEADS // 2

SP = 208
WIN = 224

EPS = 1e-06
RSQRT2 = 0.7071067811865476
RSQRT_TAU = 0.3989422804014327
LOG2E = 1.4426950408889634
Q_SCALE = LOG2E / math.sqrt(HD)
BF = jnp.bfloat16
F32 = jnp.float32


def dot_nn(a, b):
    return lax.dot_general(a, b, (((1,), (0,)), ((), ())), preferred_element_type=F32)


def dot_nt(a, b):
    return lax.dot_general(a, b, (((1,), (1,)), ((), ())), preferred_element_type=F32)


def dot_tn(a, b):
    return lax.dot_general(a, b, (((0,), (0,)), ((), ())), preferred_element_type=F32)


def window_of(i, rows):
    start = i * S
    base = jnp.minimum((start // 16) * 16, rows - WIN)
    return pl.multiple_of(base, 16), start - base


def load_image(ref, i):
    base, off = window_of(i, ref.shape[0])
    rows = ref[pl.ds(base, WIN), :].astype(F32)
    rows = pltpu.roll(rows, WIN - off, axis=0)[:SP]
    live = lax.broadcasted_iota(jnp.int32, rows.shape, 0) < S
    return jnp.where(live, rows, 0.0)


def store_image(ref, i, rows):
    base, off = window_of(i, ref.shape[0])
    rows = jnp.concatenate([rows, jnp.zeros((WIN - SP, rows.shape[1]), F32)], axis=0)
    rows = pltpu.roll(rows, off, axis=0)
    old = ref[pl.ds(base, WIN), :].astype(F32)
    mine = lax.broadcasted_iota(jnp.int32, rows.shape, 0) >= off
    ref[pl.ds(base, WIN), :] = jnp.where(mine, rows, old).astype(ref.dtype)


def norm_stats(x):
    mean = jnp.mean(x, axis=-1, keepdims=True)
    centred = x - mean
    inv = lax.rsqrt(jnp.mean(centred * centred, axis=-1, keepdims=True) + EPS)
    return centred * inv, inv


def norm_backward(grad, normed, inv, gain):
    e = grad * gain
    return inv * (
        e
        - jnp.mean(e, axis=-1, keepdims=True)
        - normed * jnp.mean(e * normed, axis=-1, keepdims=True)
    )


def row_sum(x):
    return jnp.sum(x, axis=0, keepdims=True)


def attn_fwd_kernel(tok_ref, w_ref, vec_ref, qkv_ref, e_ref, mixed_ref, linv_ref):
    i = pl.program_id(0)
    x = load_image(tok_ref, i)
    normed, _ = norm_stats(x)
    h1 = (normed * vec_ref[0:1, :] + vec_ref[1:2, :]).astype(BF)
    q = ((dot_nn(h1, w_ref[:, 0:D]) + vec_ref[2:3, :]) * Q_SCALE).astype(BF)
    k = dot_nn(h1, w_ref[:, D : 2 * D]).astype(BF)
    v = (dot_nn(h1, w_ref[:, 2 * D :]) + vec_ref[3:4, :]).astype(BF)
    qkv_ref[0, :, 0:D] = q
    qkv_ref[0, :, D : 2 * D] = k
    qkv_ref[0, :, 2 * D :] = v
    lane = lax.broadcasted_iota(jnp.int32, (SP, 2 * HD), 1)
    is_key = lax.broadcasted_iota(jnp.int32, (SP, SP), 1) < S
    zero = jnp.zeros((SP, 2 * HD), BF)
    one = jnp.ones((SP, 2 * HD), BF)
    for p in range(PAIRS):
        cols = slice(2 * HD * p, 2 * HD * (p + 1))
        total = None
        for h in range(2):
            own = (lane < HD) if h == 0 else (lane >= HD)
            kh = jnp.where(own, k[:, cols], zero)
            vh = jnp.where(own, v[:, cols], zero)
            scores = dot_nt(q[:, cols], kh)
            scores = jnp.where(is_key, scores, -1e30)
            top = jnp.max(scores, axis=-1, keepdims=True)
            e = jnp.exp2(scores - top).astype(BF)
            e_ref[0, 2 * p + h] = e
            part = dot_nn(e, jnp.concatenate([vh, jnp.where(own, one, zero)], axis=1))
            total = part if total is None else total + part
        linv = 1.0 / total[:, 2 * HD :]
        linv_ref[0, :, cols] = linv
        mixed_ref[0, :, cols] = (total[:, : 2 * HD] * linv).astype(BF)


def mlp_kernel(
    tok_ref, cot_ref, mixed_ref, wot_ref, wup_ref, wdt_ref, vec_ref, bup_ref,
    out_ref, gres_ref, gmix_ref, dwot_ref, dwup_ref, dwdt_ref, dvec_ref, dbup_ref,
    act_ref, gp_ref,
):
    i = pl.program_id(0)

    @pl.when(i == 0)
    def _():
        dwot_ref[...] = jnp.zeros_like(dwot_ref)
        dwup_ref[...] = jnp.zeros_like(dwup_ref)
        dwdt_ref[...] = jnp.zeros_like(dwdt_ref)
        dvec_ref[...] = jnp.zeros_like(dvec_ref)
        dbup_ref[...] = jnp.zeros_like(dbup_ref)

    mixed = mixed_ref[0]
    cot_f = load_image(cot_ref, i)
    cot = cot_f.astype(BF)
    resid = load_image(tok_ref, i) + dot_nt(mixed, wot_ref[...]) + vec_ref[4:5, :]
    normed, inv = norm_stats(resid)
    h2 = (normed * vec_ref[5:6, :] + vec_ref[6:7, :]).astype(BF)
    step = 256
    for j in range(FF // step):
        cols = slice(step * j, step * (j + 1))
        u = dot_nn(h2, wup_ref[:, cols]) + bup_ref[:, cols]
        ga = dot_nn(cot, wdt_ref[:, cols])
        cdf = 0.5 * (1.0 + lax.erf(u * RSQRT2))
        act_ref[:, cols] = (u * cdf).astype(BF)
        gp = ga * (cdf + u * jnp.exp(-0.5 * u * u) * RSQRT_TAU)
        dbup_ref[:, cols] += row_sum(gp)
        gp_ref[:, cols] = gp.astype(BF)
    out = resid + dot_nt(act_ref[...], wdt_ref[...]) + vec_ref[7:8, :]
    store_image(out_ref, i, out)
    gh2 = dot_nt(gp_ref[...], wup_ref[...])
    gres = cot_f + norm_backward(gh2, normed, inv, vec_ref[5:6, :])
    gres_ref[0] = gres
    gr = gres.astype(BF)
    gmix_ref[0] = dot_nn(gr, wot_ref[...]).astype(BF)
    dwot_ref[...] += dot_tn(gr, mixed)
    dwup_ref[...] += dot_tn(h2, gp_ref[...])
    dwdt_ref[...] += dot_tn(cot, act_ref[...])
    dvec_ref[0:1, :] += row_sum(gres)
    dvec_ref[1:2, :] += row_sum(gh2 * normed)
    dvec_ref[2:3, :] += row_sum(gh2)
    dvec_ref[3:4, :] += row_sum(cot_f)


def attn_bwd_kernel(
    tok_ref, qkv_ref, e_ref, mixed_ref, linv_ref, gmix_ref, gres_ref, w_ref, vec_ref,
    gtok_ref, dw_ref, dvec_ref, g_ref,
):
    i = pl.program_id(0)

    @pl.when(i == 0)
    def _():
        dw_ref[...] = jnp.zeros_like(dw_ref)
        dvec_ref[...] = jnp.zeros_like(dvec_ref)

    lane = lax.broadcasted_iota(jnp.int32, (SP, 2 * HD), 1)
    zero = jnp.zeros((SP, 2 * HD), BF)
    minus = jnp.full((SP, 2 * HD), -1.0, BF)
    for p in range(PAIRS):
        lo, hi = 2 * HD * p, 2 * HD * (p + 1)
        q = qkv_ref[0, :, lo:hi]
        k = qkv_ref[0, :, D + lo : D + hi]
        v = qkv_ref[0, :, 2 * D + lo : 2 * D + hi]
        go_f = gmix_ref[0, :, lo:hi].astype(F32) * linv_ref[0, :, lo:hi]
        go = go_f.astype(BF)
        god = jnp.concatenate(
            [go, (go_f * mixed_ref[0, :, lo:hi].astype(F32)).astype(BF)], axis=1
        )
        gq = gk = gv = None
        for h in range(2):
            own = (lane < HD) if h == 0 else (lane >= HD)
            e = e_ref[0, 2 * p + h]
            vd = jnp.concatenate(
                [jnp.where(own, v, zero), jnp.where(own, minus, zero)], axis=1
            )
            ds = e * dot_nt(god, vd).astype(BF)
            part_q = dot_nn(ds, jnp.where(own, k, zero))
            part_k = dot_tn(ds, jnp.where(own, q, zero))
            part_v = dot_tn(e, jnp.where(own, go, zero))
            gq = part_q if gq is None else gq + part_q
            gk = part_k if gk is None else gk + part_k
            gv = part_v if gv is None else gv + part_v
        gq = gq * (1.0 / math.sqrt(HD))
        dvec_ref[0:1, lo:hi] += row_sum(gq)
        dvec_ref[1:2, lo:hi] += row_sum(gv)
        g_ref[:, lo:hi] = gq.astype(BF)
        g_ref[:, D + lo : D + hi] = (gk * (1.0 / LOG2E)).astype(BF)
        g_ref[:, 2 * D + lo : 2 * D + hi] = gv.astype(BF)
    normed, inv = norm_stats(load_image(tok_ref, i))
    h1 = (normed * vec_ref[0:1, :] + vec_ref[1:2, :]).astype(BF)
    dw_ref[...] += dot_tn(h1, g_ref[...])
    gh1 = dot_nt(g_ref[...], w_ref[...])
    gtok = gres_ref[0] + norm_backward(gh1, normed, inv, vec_ref[0:1, :])
    store_image(gtok_ref, i, gtok)
    dvec_ref[2:3, :] += row_sum(gh1 * normed)
    dvec_ref[3:4, :] += row_sum(gh1)


def whole(shape):
    return pl.BlockSpec(shape, lambda i: (0,) * len(shape))


def per_image(*shape):
    return pl.BlockSpec((1, *shape), lambda i: (i,) + (0,) * len(shape))


def params():
    return pltpu.CompilerParams(
        dimension_semantics=("arbitrary",), vmem_limit_bytes=62 * 1024 * 1024
    )


def attn_fwd(tokens, wqkv, vec):
    rows = tokens.shape[0]
    n = rows // S
    return pl.pallas_call(
        attn_fwd_kernel,
        grid=(n,),
        in_specs=[whole((rows, D)), whole((D, 3 * D)), whole((8, D))],
        out_specs=[
            per_image(SP, 3 * D), per_image(HEADS, SP, SP), per_image(SP, D), per_image(SP, D),
        ],
        out_shape=[
            jax.ShapeDtypeStruct((n, SP, 3 * D), BF),
            jax.ShapeDtypeStruct((n, HEADS, SP, SP), BF),
            jax.ShapeDtypeStruct((n, SP, D), BF),
            jax.ShapeDtypeStruct((n, SP, D), F32),
        ],
        compiler_params=params(),
        name="attn_fwd",
    )(tokens, wqkv, vec)


def mlp(tokens, cot, mixed, wot, wup, wdt, vec, bup):
    rows = tokens.shape[0]
    n = rows // S
    return pl.pallas_call(
        mlp_kernel,
        grid=(n,),
        in_specs=[
            whole((rows, D)), whole((rows, D)), per_image(SP, D), whole((D, D)), whole((D, FF)),
            whole((D, FF)), whole((8, D)), whole((1, FF)),
        ],
        out_specs=[
            whole((rows, D)), per_image(SP, D), per_image(SP, D), whole((D, D)), whole((D, FF)),
            whole((D, FF)), whole((8, D)), whole((1, FF)),
        ],
        out_shape=[
            jax.ShapeDtypeStruct((rows, D), BF),
            jax.ShapeDtypeStruct((n, SP, D), F32),
            jax.ShapeDtypeStruct((n, SP, D), BF),
            jax.ShapeDtypeStruct((D, D), F32),
            jax.ShapeDtypeStruct((D, FF), F32),
            jax.ShapeDtypeStruct((D, FF), F32),
            jax.ShapeDtypeStruct((8, D), F32),
            jax.ShapeDtypeStruct((1, FF), F32),
        ],
        scratch_shapes=[pltpu.VMEM((SP, FF), BF), pltpu.VMEM((SP, FF), BF)],
        compiler_params=params(),
        name="mlp",
    )(tokens, cot, mixed, wot, wup, wdt, vec, bup)


def attn_bwd(tokens, qkv, e, mixed, linv, gmix, gres, wqkv, vec):
    rows = tokens.shape[0]
    n = rows // S
    return pl.pallas_call(
        attn_bwd_kernel,
        grid=(n,),
        in_specs=[
            whole((rows, D)), per_image(SP, 3 * D), per_image(HEADS, SP, SP), per_image(SP, D),
            per_image(SP, D), per_image(SP, D), per_image(SP, D), whole((D, 3 * D)), whole((8, D)),
        ],
        out_specs=[whole((rows, D)), whole((D, 3 * D)), whole((8, D))],
        out_shape=[
            jax.ShapeDtypeStruct((rows, D), F32),
            jax.ShapeDtypeStruct((D, 3 * D), F32),
            jax.ShapeDtypeStruct((8, D), F32),
        ],
        scratch_shapes=[pltpu.VMEM((SP, 3 * D), BF)],
        compiler_params=params(),
        name="attn_bwd",
    )(tokens, qkv, e, mixed, linv, gmix, gres, wqkv, vec)


PARTS = (D // 2, D // 2, D // 2, D // 2, FF // 2, FF // 2)
WIDE = sum(PARTS)
CUT = WIDE // 2
MESH = pl.DeviceIdType.MESH


def chip_grid(dp):
    side = math.isqrt(dp // 4)
    return 4, side, side


class Mover:
    def __init__(self, send, recv):
        self.send, self.recv, self.used = send, recv, 0

    def start(self, src, dst, device):
        copy = pltpu.make_async_remote_copy(
            src_ref=src, dst_ref=dst, send_sem=self.send.at[self.used],
            recv_sem=self.recv.at[self.used], device_id=device, device_id_type=MESH,
        )
        copy.start()
        self.used += 1
        return copy


def place_of(dims):
    _, ny, nx = dims
    dp, mp = lax.axis_index("dp"), lax.axis_index("mp")
    return dp // (ny * nx), (dp // nx) % ny, dp % nx, mp


def peers_of(dims, place):
    (nz, ny, nx), (z, y, x, mp) = dims, place

    def at(a, b, c, m):
        return ((a * ny + b) * nx + c, m)

    along = {
        "z": [((z + o) % nz, at((z + o) % nz, y, x, mp)) for o in range(1, nz)],
        "y": [((y + o) % ny, at(z, (y + o) % ny, x, mp)) for o in range(1, ny)],
        "x": [((x + o) % nx, at(z, y, (x + o) % nx, mp)) for o in range(1, nx)],
    }
    return along, at(z, y, x, 1 - mp)


def meet(along, other):
    barrier = pltpu.get_barrier_semaphore()
    devices = [d for peers in along.values() for _, d in peers] + [other]
    for device in devices:
        pl.semaphore_signal(barrier, inc=1, device_id=device, device_id_type=MESH)
    pl.semaphore_wait(barrier, len(devices))


def gather_kernel(dims, *refs):
    (wq, wk, wv, wo, wu, wd), vectors, bup = refs[:6], refs[6:14], refs[14]
    wqkv_ref, wot_ref, wup_ref, wdt_ref, vec_ref, bup_ref = refs[15:21]
    w, v, send, recv = refs[21:]
    nz, ny, nx = dims
    place = place_of(dims)
    z, y, x, mp = place
    rows = w.shape[4]
    along, other = peers_of(dims, place)
    w[z, y, x, mp] = jnp.concatenate(
        [wq[...], wk[...], wv[...], wo[...].astype(F32).T.astype(BF), wu[...],
         wd[...].astype(F32).T.astype(BF)],
        axis=1,
    )
    for j, vector in enumerate(vectors):
        v[z, y, x, j : j + 1, :rows] = vector[...].astype(F32)
    v[z, y, x, 8:9, : bup.shape[1]] = bup[...].astype(F32)
    meet(along, other)

    mover = Mover(send, recv)
    low, high = pl.ds(0, CUT), pl.ds(CUT, WIDE - CUT)
    sent = []

    def spread(buffer, index, axis):
        return [mover.start(buffer.at[index], buffer.at[index], d) for _, d in along[axis]]

    def share(index):
        sent.append(mover.start(w.at[index], w.at[index], other))
        return sent[-1]

    def arrived(copies):
        for c in copies:
            c.wait_recv()
        sent.extend(copies)

    every = slice(None)
    first = spread(w, (z, y, x, mp), "z") + spread(v, (z, y, x), "z")
    arrived(first)
    shared = [share((every, y, x, mp))]
    second_low = spread(w, (every, y, x, mp, every, low), "y") + spread(v, (every, y, x), "y")
    second_high = spread(w, (every, y, x, mp, every, high), "x")
    arrived(second_low)
    third_low = spread(w, (every, every, x, mp, every, low), "x") + spread(
        v, (every, every, x), "x"
    )
    arrived(second_high)
    third_high = spread(w, (every, y, every, mp, every, high), "y")
    for b, _ in along["y"]:
        shared.append(share((every, b, x, mp, every, low)))
    for c, _ in along["x"]:
        shared.append(share((every, y, c, mp, every, high)))
    arrived(third_low)
    for c, _ in along["x"]:
        shared.append(share((every, every, c, mp, every, low)))
    arrived(third_high)
    for b, _ in along["y"]:
        shared.append(share((every, b, every, mp, every, high)))

    n = nz * ny * nx
    spots = [(a, b, c) for a in range(nz) for b in range(ny) for c in range(nx)]
    vec_ref[...] = jnp.concatenate([v[s][0:8, :rows] for s in spots], axis=1)
    bup_ref[...] = jnp.concatenate([v[s][8:9, : bup.shape[1]] for s in spots], axis=1)
    for c in shared:
        c.wait_recv()

    group = 48 // rows
    ends = [sum(PARTS[: i + 1]) for i in range(len(PARTS))]
    for t in range(n // group):
        block = [
            jnp.concatenate(
                [w[s + (m,)].astype(F32) for s in spots[t * group : (t + 1) * group]], axis=0
            )
            for m in range(2)
        ]
        at = pl.ds(48 * t, 48)

        def both(i):
            lo, hi = ends[i] - PARTS[i], ends[i]
            return jnp.concatenate([half[:, lo:hi] for half in block], axis=1).astype(BF)

        for i in range(3):
            wqkv_ref[at, D * i : D * (i + 1)] = both(i)
        wot_ref[at, :] = both(3)
        wup_ref[at, :] = both(4)
        wdt_ref[at, :] = both(5)
    for c in sent:
        c.wait_send()


def gather(mats, vectors, bup, dp):
    dims = chip_grid(dp)
    nz, ny, nx = dims
    rows = D // dp
    copies = 2 * (nz + ny + nx) + 3 * (ny + nx) + 2
    vmem = pl.BlockSpec(memory_space=pltpu.VMEM)
    return pl.pallas_call(
        functools.partial(gather_kernel, dims),
        in_specs=[vmem] * 15,
        out_specs=[vmem] * 6,
        out_shape=[
            jax.ShapeDtypeStruct((D, 3 * D), BF),
            jax.ShapeDtypeStruct((D, D), BF),
            jax.ShapeDtypeStruct((D, FF), BF),
            jax.ShapeDtypeStruct((D, FF), BF),
            jax.ShapeDtypeStruct((8, D), F32),
            jax.ShapeDtypeStruct((1, FF), F32),
        ],
        scratch_shapes=[
            pltpu.VMEM((nz, ny, nx, 2, rows, WIDE), BF),
            pltpu.VMEM((nz, ny, nx, 16, 128), F32),
            pltpu.SemaphoreType.DMA((copies,)),
            pltpu.SemaphoreType.DMA((copies,)),
        ],
        compiler_params=pltpu.CompilerParams(
            collective_id=0, has_side_effects=True, vmem_limit_bytes=62 * 1024 * 1024
        ),
        name="gather",
    )(*mats, *vectors, bup)


def reduce_kernel(
    dims, dqkv, dwot, dwup, dwdt, dvec1, dvec2, dbup, out_ref, vec_ref,
    s, p, a1, b1, a2, b2, ra1, rb1, ra2, rb2, rz, f, vs, vr, send, recv,
):
    nz, ny, nx = dims
    place = place_of(dims)
    z, y, x, mp = place
    rows = s.shape[4]
    along, other = peers_of(dims, place)
    spots = [(i, j, k) for i in range(nz) for j in range(ny) for k in range(nx)]
    group = 48 // rows
    for t in range(len(spots) // group):
        at = pl.ds(48 * t, 48)
        for m in range(2):
            parts = [dqkv[at, D * i : D * (i + 1)] for i in range(3)]
            parts += [dwot[at, :], dwup[at, :], dwdt[at, :]]
            block = jnp.concatenate(
                [q[:, m * n : (m + 1) * n] for q, n in zip(parts, PARTS)], axis=1
            )
            for g in range(group):
                s[(m,) + spots[t * group + g]] = block[g * rows : (g + 1) * rows].astype(BF)
    vs[0, 0:4] = dvec1[0:4]
    vs[0, 4:8] = dvec2[0:4]
    for j in range(FF // D):
        vs[0, 8 + j : 9 + j] = dbup[:, D * j : D * (j + 1)]
    vs[0, 12:16] = jnp.zeros((4, D), F32)
    meet(along, other)

    mover = Mover(send, recv)
    sent = []

    def arrived(copies):
        for c in copies:
            c.wait_recv()
        sent.extend(copies)

    def vec_send(stage, devices, base):
        return [
            mover.start(vs.at[stage], vr.at[base + i], d) for i, d in enumerate(devices)
        ]

    def vec_add(stage, base, n):
        total = vs[stage]
        for i in range(n):
            total = total + vr[base + i]
        if stage < 3:
            vs[stage + 1] = total
        else:
            vec_ref[...] = total

    pair = [mover.start(s.at[1 - mp], p, other)] + vec_send(0, [other], 0)
    arrived(pair)
    for i in range(nz):
        for j in range(ny):
            for k in range(nx):
                p[i, j, k] = (s[mp, i, j, k].astype(F32) + p[i, j, k].astype(F32)).astype(BF)
    vec_add(0, 0, 1)

    every = slice(None)
    low, high = pl.ds(0, CUT), pl.ds(CUT, WIDE - CUT)
    first_low = [
        mover.start(p.at[every, every, c, every, low], ra1.at[o], d)
        for o, (c, d) in enumerate(along["x"])
    ] + vec_send(1, [d for _, d in along["x"]], 1)
    first_high = [
        mover.start(p.at[every, b, every, every, high], rb1.at[o], d)
        for o, (b, d) in enumerate(along["y"])
    ]
    arrived(first_low)
    for i in range(nz):
        for j in range(ny):
            total = p[i, j, x, :, :CUT].astype(F32)
            for o in range(nx - 1):
                total = total + ra1[o, i, j].astype(F32)
            a1[i, j] = total.astype(BF)
    vec_add(1, 1, nx - 1)
    second_low = [
        mover.start(a1.at[every, b], ra2.at[o], d) for o, (b, d) in enumerate(along["y"])
    ] + vec_send(2, [d for _, d in along["y"]], nx)
    arrived(first_high)
    for i in range(nz):
        for k in range(nx):
            total = p[i, y, k, :, CUT:].astype(F32)
            for o in range(ny - 1):
                total = total + rb1[o, i, k].astype(F32)
            b1[i, k] = total.astype(BF)
    second_high = [
        mover.start(b1.at[every, c], rb2.at[o], d) for o, (c, d) in enumerate(along["x"])
    ]
    arrived(second_low)
    for i in range(nz):
        total = a1[i, y].astype(F32)
        for o in range(ny - 1):
            total = total + ra2[o, i].astype(F32)
        f[i, :, :CUT] = total.astype(BF)
    vec_add(2, nx, ny - 1)
    arrived(second_high)
    for i in range(nz):
        total = b1[i, x].astype(F32)
        for o in range(nx - 1):
            total = total + rb2[o, i].astype(F32)
        f[i, :, CUT:] = total.astype(BF)
    third = [
        mover.start(f.at[a], rz.at[o], d) for o, (a, d) in enumerate(along["z"])
    ] + vec_send(3, [d for _, d in along["z"]], nx + ny - 1)
    arrived(third)
    total = f[z].astype(F32)
    for o in range(nz - 1):
        total = total + rz[o].astype(F32)
    out_ref[...] = total
    vec_add(3, nx + ny - 1, nz - 1)
    for c in sent:
        c.wait_send()


def reduce(dqkv, dwot, dwup, dwdt, dvec1, dvec2, dbup, dp):
    dims = chip_grid(dp)
    nz, ny, nx = dims
    rows = D // dp
    copies = 2 * (nz + ny + nx) + ny + nx
    vmem = pl.BlockSpec(memory_space=pltpu.VMEM)

    def buf(*shape):
        return pltpu.VMEM((*shape, rows, CUT), BF)

    return pl.pallas_call(
        functools.partial(reduce_kernel, dims),
        in_specs=[vmem] * 7,
        out_specs=[vmem] * 2,
        out_shape=[
            jax.ShapeDtypeStruct((rows, WIDE), F32),
            jax.ShapeDtypeStruct((16, D), F32),
        ],
        scratch_shapes=[
            pltpu.VMEM((2, nz, ny, nx, rows, WIDE), BF),
            pltpu.VMEM((nz, ny, nx, rows, WIDE), BF),
            buf(nz, ny), buf(nz, nx), buf(nz), buf(nz),
            buf(nx - 1, nz, ny), buf(ny - 1, nz, nx), buf(ny - 1, nz), buf(nx - 1, nz),
            pltpu.VMEM((nz - 1, rows, WIDE), BF),
            pltpu.VMEM((nz, rows, WIDE), BF),
            pltpu.VMEM((4, 16, D), F32),
            pltpu.VMEM((nz + ny + nx, 16, D), F32),
            pltpu.SemaphoreType.DMA((copies,)),
            pltpu.SemaphoreType.DMA((copies,)),
        ],
        compiler_params=pltpu.CompilerParams(
            collective_id=1, has_side_effects=True, vmem_limit_bytes=62 * 1024 * 1024
        ),
        name="reduce",
    )(dqkv, dwot, dwup, dwdt, dvec1, dvec2, dbup)


def split_kernel(n, mat_ref, vec_ref, *outs):
    at = 0
    for i, (width, out) in enumerate(zip(PARTS, outs)):
        part = mat_ref[:, at : at + width]
        out[...] = part.T if i in (3, 5) else part
        at += width
    index = lax.axis_index("dp") * 2 + lax.axis_index("mp")
    per = D // n
    vec = pltpu.roll(vec_ref[...], D - index * per, axis=1)
    for row, out in zip((2, 3, 0, 1, 4, 5, 6, 7), outs[6:]):
        out[...] = vec[row : row + 1, :per]
    wide = jnp.concatenate([vec_ref[8 + j : 9 + j, :] for j in range(FF // D)], axis=1)
    wide = pltpu.roll(jnp.broadcast_to(wide, (8, FF)), FF - index * (FF // n), axis=1)
    outs[14][...] = wide[0:1, : FF // n]


def split(mat, vec, n):
    rows = mat.shape[0]
    vmem = pl.BlockSpec(memory_space=pltpu.VMEM)
    shapes = [(w, rows) if i in (3, 5) else (rows, w) for i, w in enumerate(PARTS)]
    shapes += [(1, D // n)] * 8 + [(1, FF // n)]
    return pl.pallas_call(
        functools.partial(split_kernel, n),
        in_specs=[vmem] * 2,
        out_specs=[vmem] * 15,
        out_shape=[jax.ShapeDtypeStruct(s, F32) for s in shapes],
        name="split",
    )(mat, vec)


def on_device(
    tokens, w_query, w_key, w_value, w_out, w_up, w_down, ln1_gain, ln1_bias, b_query, b_value,
    b_out, ln2_gain, ln2_bias, b_up, b_down, cotangent,
):
    dp = lax.axis_size("dp")
    vectors = (ln1_gain, ln1_bias, b_query, b_value, b_out, ln2_gain, ln2_bias, b_down)
    wqkv, wot, wup, wdt, vec, bup = gather(
        (w_query, w_key, w_value, w_out, w_up, w_down), [v[None] for v in vectors], b_up[None], dp
    )
    qkv, e, mixed, linv = attn_fwd(tokens, wqkv, vec)
    out, gres, gmix, dwot, dwup, dwdt, dvec2, dbup = mlp(
        tokens, cotangent, mixed, wot, wup, wdt, vec, bup
    )
    gtok, dwqkv, dvec1 = attn_bwd(tokens, qkv, e, mixed, linv, gmix, gres, wqkv, vec)
    mat, sums = reduce(dwqkv, dwot, dwup, dwdt, dvec1, dvec2, dbup, dp)
    grads = split(mat, sums, dp * lax.axis_size("mp"))
    vecs = [g.reshape(-1) for g in grads[6:]]
    return (out, gtok, *grads[:6], *vecs[:7], vecs[8], vecs[7])


def solution(mesh):
    row, mat, tam, vec = P(("dp", "mp"), None), P("dp", "mp"), P("mp", "dp"), P("dp")
    part = P(("dp", "mp"))
    return jax.shard_map(
        on_device,
        mesh=mesh,
        in_specs=(row, mat, mat, mat, tam, mat, tam, *([vec] * 9), row),
        out_specs=(row, row, mat, mat, mat, tam, mat, tam, *([part] * 9)),
        check_vma=False,
    )
```

```python
import functools
import math

import jax
import jax.numpy as jnp
from jax import lax
from jax.experimental import pallas as pl
from jax.experimental.pallas import tpu as pltpu
from jax.sharding import PartitionSpec as P

D = 384
HD = 64
FF = 1536
S = 197
HEADS = D // HD
PAIRS = HEADS // 2

SP = 208
WIN = 224

EPS = 1e-06
RSQRT2 = 0.7071067811865476
RSQRT_TAU = 0.3989422804014327
LOG2E = 1.4426950408889634
Q_SCALE = LOG2E / math.sqrt(HD)
BF = jnp.bfloat16
F32 = jnp.float32


def dot_nn(a, b):
    return lax.dot_general(a, b, (((1,), (0,)), ((), ())), preferred_element_type=F32)


def dot_nt(a, b):
    return lax.dot_general(a, b, (((1,), (1,)), ((), ())), preferred_element_type=F32)


def dot_tn(a, b):
    return lax.dot_general(a, b, (((0,), (0,)), ((), ())), preferred_element_type=F32)


def window_of(i, rows):
    start = i * S
    base = jnp.minimum((start // 16) * 16, rows - WIN)
    return pl.multiple_of(base, 16), start - base


def load_image(ref, i):
    base, off = window_of(i, ref.shape[0])
    rows = ref[pl.ds(base, WIN), :].astype(F32)
    rows = pltpu.roll(rows, WIN - off, axis=0)[:SP]
    live = lax.broadcasted_iota(jnp.int32, rows.shape, 0) < S
    return jnp.where(live, rows, 0.0)


def store_image(ref, i, rows):
    base, off = window_of(i, ref.shape[0])
    rows = jnp.concatenate([rows, jnp.zeros((WIN - SP, rows.shape[1]), F32)], axis=0)
    rows = pltpu.roll(rows, off, axis=0)
    old = ref[pl.ds(base, WIN), :].astype(F32)
    mine = lax.broadcasted_iota(jnp.int32, rows.shape, 0) >= off
    ref[pl.ds(base, WIN), :] = jnp.where(mine, rows, old).astype(ref.dtype)


def norm_stats(x):
    mean = jnp.mean(x, axis=-1, keepdims=True)
    centred = x - mean
    inv = lax.rsqrt(jnp.mean(centred * centred, axis=-1, keepdims=True) + EPS)
    return centred * inv, inv


def norm_backward(grad, normed, inv, gain):
    e = grad * gain
    return inv * (
        e
        - jnp.mean(e, axis=-1, keepdims=True)
        - normed * jnp.mean(e * normed, axis=-1, keepdims=True)
    )


def row_sum(x):
    return jnp.sum(x, axis=0, keepdims=True)


THIRD = D // 2
HALF = FF // 2
NARROW = 640
NARROW_CUT = 384
OUT_PAD = 256
WIDE = OUT_PAD + 2 * HALF
WIDE_CUT = 896
MESH = pl.DeviceIdType.MESH
EVERY = slice(None)


def chip_grid(dp):
    side = math.isqrt(dp // 4)
    return 4, side, side


def place_of(dims):
    _, ny, nx = dims
    dp, mp = lax.axis_index("dp"), lax.axis_index("mp")
    return dp // (ny * nx), (dp // nx) % ny, dp % nx, mp


def peers_of(dims, place):
    (nz, ny, nx), (z, y, x, mp) = dims, place

    def at(a, b, c, m):
        return ((a * ny + b) * nx + c, m)

    along = {
        "z": [((z + o) % nz, at((z + o) % nz, y, x, mp)) for o in range(1, nz)],
        "y": [((y + o) % ny, at(z, (y + o) % ny, x, mp)) for o in range(1, ny)],
        "x": [((x + o) % nx, at(z, y, (x + o) % nx, mp)) for o in range(1, nx)],
    }
    return along, at(z, y, x, 1 - mp)


def meet(along, other):
    barrier = pltpu.get_barrier_semaphore()
    devices = [d for peers in along.values() for _, d in peers] + [other]
    for device in devices:
        pl.semaphore_signal(barrier, inc=1, device_id=device, device_id_type=MESH)
    pl.semaphore_wait(barrier, len(devices))


class Copies:
    def __init__(self, send, recv):
        self.send, self.recv, self.groups, self.count = send, recv, {}, 0

    def plan(self, name, makers):
        self.groups[name] = [(self.count + i, m) for i, m in enumerate(makers)]
        self.count += len(makers)

    def each(self, names):
        for name in names:
            for index, make in self.groups[name]:
                src, dst, device = make()
                yield pltpu.make_async_remote_copy(
                    src_ref=src, dst_ref=dst, send_sem=self.send.at[index],
                    recv_sem=self.recv.at[index], device_id=device, device_id_type=MESH,
                )

    def start(self, *names):
        for copy in self.each(names):
            copy.start()

    def arrived(self, *names):
        for copy in self.each(names):
            copy.wait_recv()

    def left(self, *names):
        for copy in self.each(names):
            copy.wait_send()


def plan_gather(copies, tag, w, own, cut, along, other, place):
    z, y, x, mp = place
    low, high = pl.ds(0, cut), pl.ds(cut, w.shape[-1] - cut)

    def same(index, device):
        return lambda: (w.at[index], w.at[index], device)

    def spread(index, axis):
        return [same(index, d) for _, d in along[axis]]

    def shares(indices):
        return [same(index, other) for index in indices]

    copies.plan(tag + "1", [lambda d=d: (own, w.at[mp, z, y, x], d) for _, d in along["z"]])
    copies.plan(tag + "2l", spread((mp, EVERY, y, x, EVERY, low), "y"))
    copies.plan(tag + "2h", spread((mp, EVERY, y, x, EVERY, high), "x"))
    copies.plan(tag + "3l", spread((mp, EVERY, EVERY, x, EVERY, low), "x"))
    copies.plan(tag + "3h", spread((mp, EVERY, y, EVERY, EVERY, high), "y"))
    copies.plan(tag + "s1", shares([(mp, EVERY, y, x)]))
    copies.plan(tag + "s2l", shares([(mp, EVERY, b, x, EVERY, low) for b, _ in along["y"]]))
    copies.plan(tag + "s2h", shares([(mp, EVERY, y, c, EVERY, high) for c, _ in along["x"]]))
    copies.plan(tag + "s3l", shares([(mp, EVERY, EVERY, c, EVERY, low) for c, _ in along["x"]]))
    copies.plan(tag + "s3h", shares([(mp, EVERY, b, EVERY, EVERY, high) for b, _ in along["y"]]))


def attn_fwd_kernel(dims, n, *refs):
    (wq, wk, wv, wot, wu, wdt), vectors, bup_in, tok_ref = refs[:6], refs[6:14], refs[14], refs[15]
    (qkv_ref, e_ref, mixed_ref, linv_ref, normed_ref, inv_ref, w_ref, vec_ref, bup_ref, wide) = refs[
        16:26
    ]
    narrow, v, own, normed_all, inv_all, send, recv, sem = refs[26:]
    i = pl.program_id(0)
    nz, ny, nx = dims
    place = place_of(dims)
    z, y, x, mp = place
    rows = own.shape[0]
    along, other = peers_of(dims, place)
    copies = Copies(send, recv)
    plan_gather(copies, "n", narrow, narrow.at[mp, z, y, x], NARROW_CUT, along, other, place)
    plan_gather(copies, "w", wide, own, WIDE_CUT, along, other, place)

    def vec_spread(index, axis):
        return [lambda d=d: (v.at[index], v.at[index], d) for _, d in along[axis]]

    copies.plan("v1", vec_spread((z, y, x), "z"))
    copies.plan("v2", vec_spread((EVERY, y, x), "y"))
    copies.plan("v3", vec_spread((EVERY, EVERY, x), "x"))
    keep = pltpu.make_async_copy(own, wide.at[mp, z, y, x], sem)

    def norms(first, last):
        @pl.loop(first, last)
        def _(j):
            normed, inv = norm_stats(load_image(tok_ref, j))
            normed_all[j] = normed
            inv_all[j] = jnp.broadcast_to(inv, (SP, 128))

    @pl.when(i == 0)
    def _():
        narrow[mp, z, y, x] = jnp.concatenate(
            [wq[...], wk[...], wv[...], jnp.zeros((rows, NARROW - 3 * THIRD), BF)], axis=1
        )
        own[...] = jnp.concatenate(
            [wot[...], jnp.zeros((rows, OUT_PAD - THIRD), BF), wu[...], wdt[...]], axis=1
        )
        v[z, y, x] = jnp.zeros((16, 128), F32)
        for j, vector in enumerate(vectors):
            v[z, y, x, j : j + 1, :rows] = vector[...].astype(F32)
        v[z, y, x, 8:9, : bup_in.shape[1]] = bup_in[...].astype(F32)
        meet(along, other)
        copies.start("v1", "n1")
        keep.start()
        norms(0, n // 4)
        copies.arrived("v1", "n1")
        copies.start("v2", "n2l", "n2h", "w1", "ns1")
        norms(n // 4, n // 2)
        copies.arrived("v2", "n2l", "n2h")
        copies.start("v3", "n3l", "n3h", "ns2l", "ns2h")
        norms(n // 2, n)
        copies.arrived("v3", "n3l")
        copies.start("ns3l")
        copies.arrived("n3h")
        copies.start("ns3h")
        spots = [(a, b, c) for a in range(nz) for b in range(ny) for c in range(nx)]
        vec_ref[...] = jnp.concatenate([v[s][0:8, :rows] for s in spots], axis=1)
        bup_ref[...] = jnp.concatenate([v[s][8:9, : bup_in.shape[1]] for s in spots], axis=1)
        copies.arrived("ns1", "ns2l", "ns2h", "ns3l", "ns3h")
        group = 48 // rows
        for t in range(len(spots) // group):
            block = [
                jnp.concatenate(
                    [narrow[(m,) + s].astype(F32) for s in spots[t * group : (t + 1) * group]], axis=0
                )
                for m in range(2)
            ]
            for j in range(3):
                cols = slice(THIRD * j, THIRD * (j + 1))
                w_ref[48 * t : 48 * (t + 1), D * j : D * (j + 1)] = jnp.concatenate(
                    [half[:, cols] for half in block], axis=1
                ).astype(BF)

    @pl.when(i == 2)
    def _():
        keep.wait()
        copies.arrived("w1")
        copies.start("w2l", "w2h", "ws1")

    @pl.when(i == n // 4 + 1)
    def _():
        copies.arrived("w2l", "w2h")
        copies.start("w3l", "w3h", "ws2l", "ws2h")

    normed = normed_all[i]
    normed_ref[0] = normed
    inv_ref[0] = inv_all[i]
    h1 = (normed * vec_ref[0:1, :] + vec_ref[1:2, :]).astype(BF)
    q = ((dot_nn(h1, w_ref[:, 0:D]) + vec_ref[2:3, :]) * Q_SCALE).astype(BF)
    k = dot_nn(h1, w_ref[:, D : 2 * D]).astype(BF)
    value = (dot_nn(h1, w_ref[:, 2 * D :]) + vec_ref[3:4, :]).astype(BF)
    qkv_ref[0, :, 0:D] = q
    qkv_ref[0, :, D : 2 * D] = k
    qkv_ref[0, :, 2 * D :] = value
    lane = lax.broadcasted_iota(jnp.int32, (SP, 2 * HD), 1)
    is_key = lax.broadcasted_iota(jnp.int32, (SP, SP), 1) < S
    zero = jnp.zeros((SP, 2 * HD), BF)
    one = jnp.ones((SP, 2 * HD), BF)
    for p in range(PAIRS):
        cols = slice(2 * HD * p, 2 * HD * (p + 1))
        total = None
        for h in range(2):
            mine = (lane < HD) if h == 0 else (lane >= HD)
            kh = jnp.where(mine, k[:, cols], zero)
            vh = jnp.where(mine, value[:, cols], zero)
            scores = dot_nt(q[:, cols], kh)
            scores = jnp.where(is_key, scores, -1e30)
            top = jnp.max(scores, axis=-1, keepdims=True)
            e = jnp.exp2(scores - top).astype(BF)
            e_ref[0, 2 * p + h] = e
            part = dot_nn(e, jnp.concatenate([vh, jnp.where(mine, one, zero)], axis=1))
            total = part if total is None else total + part
        linv = 1.0 / total[:, 2 * HD :]
        linv_ref[0, :, cols] = linv
        mixed_ref[0, :, cols] = (total[:, : 2 * HD] * linv).astype(BF)

    @pl.when(i == (3 * n) // 4)
    def _():
        copies.arrived("w3l", "w3h")
        copies.start("ws3l", "ws3h")

    @pl.when(i == n - 1)
    def _():
        copies.arrived("ws1", "ws2l", "ws2h", "ws3l", "ws3h")
        copies.left(*copies.groups)


def attn_fwd(mats, vectors, bup, tokens, dp):
    dims = chip_grid(dp)
    nz, ny, nx = dims
    rows = D // dp
    n = tokens.shape[0] // S
    count = 2 * (nz - 1 + 4 * (ny - 1) + 4 * (nx - 1) + 1) + nz + ny + nx - 3
    inputs = (*mats, *vectors, bup, tokens)
    return pl.pallas_call(
        functools.partial(attn_fwd_kernel, dims, n),
        grid=(n,),
        in_specs=[whole(a.shape) for a in inputs],
        out_specs=[
            per_image(SP, 3 * D), per_image(HEADS, SP, SP), per_image(SP, D), per_image(SP, D),
            per_image(SP, D), per_image(SP, 128), whole((D, 3 * D)), whole((8, D)), whole((1, FF)),
            pl.BlockSpec(memory_space=pl.ANY),
        ],
        out_shape=[
            jax.ShapeDtypeStruct((n, SP, 3 * D), BF),
            jax.ShapeDtypeStruct((n, HEADS, SP, SP), BF),
            jax.ShapeDtypeStruct((n, SP, D), BF),
            jax.ShapeDtypeStruct((n, SP, D), F32),
            jax.ShapeDtypeStruct((n, SP, D), F32),
            jax.ShapeDtypeStruct((n, SP, 128), F32),
            jax.ShapeDtypeStruct((D, 3 * D), BF),
            jax.ShapeDtypeStruct((8, D), F32),
            jax.ShapeDtypeStruct((1, FF), F32),
            jax.ShapeDtypeStruct((2, nz, ny, nx, rows, WIDE), BF),
        ],
        scratch_shapes=[
            pltpu.VMEM((2, nz, ny, nx, rows, NARROW), BF),
            pltpu.VMEM((nz, ny, nx, 16, 128), F32),
            pltpu.VMEM((rows, WIDE), BF),
            pltpu.VMEM((n, SP, D), F32),
            pltpu.VMEM((n, SP, 128), F32),
            pltpu.SemaphoreType.DMA((count,)),
            pltpu.SemaphoreType.DMA((count,)),
            pltpu.SemaphoreType.DMA,
        ],
        compiler_params=params(collective_id=0),
        name="attn_fwd",
    )(*inputs)


def mlp_kernel(
    dims, n, tok_ref, cot_ref, mixed_ref, w_ref, vec_ref, bup_ref,
    out_ref, gres_ref, gmix_ref, grads_ref, dvec_ref, dbup_ref,
    act_ref, gp_ref, wot_ref, dwot_ref, dwup_ref, dwdt_ref,
):
    i = pl.program_id(0)

    @pl.when(i == 0)
    def _():
        wot_ref[...] = jnp.concatenate([w_ref[0, :, :THIRD], w_ref[1, :, :THIRD]], axis=1)
        dwot_ref[...] = jnp.zeros_like(dwot_ref)
        dwup_ref[...] = jnp.zeros_like(dwup_ref)
        dwdt_ref[...] = jnp.zeros_like(dwdt_ref)
        dvec_ref[...] = jnp.zeros_like(dvec_ref)
        dbup_ref[...] = jnp.zeros_like(dbup_ref)

    mixed = mixed_ref[0]
    cot_f = load_image(cot_ref, i)
    cot = cot_f.astype(BF)
    resid = load_image(tok_ref, i) + dot_nt(mixed, wot_ref[...]) + vec_ref[4:5, :]
    normed, inv = norm_stats(resid)
    h2 = (normed * vec_ref[5:6, :] + vec_ref[6:7, :]).astype(BF)
    step = 256
    for j in range(FF // step):
        cols = slice(step * j, step * (j + 1))
        m, at = divmod(step * j, HALF)
        u = dot_nn(h2, w_ref[m, :, OUT_PAD + at : OUT_PAD + at + step]) + bup_ref[:, cols]
        ga = dot_nn(cot, w_ref[m, :, OUT_PAD + HALF + at : OUT_PAD + HALF + at + step])
        cdf = 0.5 * (1.0 + lax.erf(u * RSQRT2))
        act_ref[:, cols] = (u * cdf).astype(BF)
        gp = ga * (cdf + u * jnp.exp(-0.5 * u * u) * RSQRT_TAU)
        dbup_ref[:, cols] += row_sum(gp)
        gp_ref[:, cols] = gp.astype(BF)
    out = resid + vec_ref[7:8, :]
    gh2 = None
    for m in range(2):
        cols = slice(HALF * m, HALF * (m + 1))
        out = out + dot_nt(act_ref[:, cols], w_ref[m, :, OUT_PAD + HALF :])
        part = dot_nt(gp_ref[:, cols], w_ref[m, :, OUT_PAD : OUT_PAD + HALF])
        gh2 = part if gh2 is None else gh2 + part
    store_image(out_ref, i, out)
    gres = cot_f + norm_backward(gh2, normed, inv, vec_ref[5:6, :])
    gres_ref[0] = gres
    gr = gres.astype(BF)
    gmix_ref[0] = dot_nn(gr, wot_ref[...]).astype(BF)
    dwot_ref[...] += dot_tn(gr, mixed)
    dwup_ref[...] += dot_tn(h2, gp_ref[...])
    dwdt_ref[...] += dot_tn(cot, act_ref[...])
    dvec_ref[0:1, :] += row_sum(gres)
    dvec_ref[1:2, :] += row_sum(gh2 * normed)
    dvec_ref[2:3, :] += row_sum(gh2)
    dvec_ref[3:4, :] += row_sum(cot_f)

    @pl.when(i == n - 1)
    def _():
        nz, ny, nx = dims
        rows = grads_ref.shape[4]
        spots = [(a, b, c) for a in range(nz) for b in range(ny) for c in range(nx)]
        group = 48 // rows
        for t in range(len(spots) // group):
            at = slice(48 * t, 48 * (t + 1))
            for m in range(2):
                parts = [
                    dwot_ref[at, THIRD * m : THIRD * (m + 1)],
                    jnp.zeros((48, OUT_PAD - THIRD), F32),
                    dwup_ref[at, HALF * m : HALF * (m + 1)],
                    dwdt_ref[at, HALF * m : HALF * (m + 1)],
                ]
                block = jnp.concatenate(parts, axis=1)
                for g in range(group):
                    grads_ref[(m,) + spots[t * group + g]] = block[
                        g * rows : (g + 1) * rows
                    ].astype(BF)


def mlp(tokens, cot, mixed, wide, vec, bup, dp):
    dims = chip_grid(dp)
    rows = tokens.shape[0]
    n = rows // S
    packed = (2, *dims, D // dp, WIDE)
    return pl.pallas_call(
        functools.partial(mlp_kernel, dims, n),
        grid=(n,),
        in_specs=[
            whole((rows, D)), whole((rows, D)), per_image(SP, D), whole((2, D, WIDE)), whole((8, D)),
            whole((1, FF)),
        ],
        out_specs=[
            whole((rows, D)), per_image(SP, D), per_image(SP, D), whole(packed), whole((8, D)),
            whole((1, FF)),
        ],
        out_shape=[
            jax.ShapeDtypeStruct((rows, D), BF),
            jax.ShapeDtypeStruct((n, SP, D), F32),
            jax.ShapeDtypeStruct((n, SP, D), BF),
            jax.ShapeDtypeStruct(packed, BF),
            jax.ShapeDtypeStruct((8, D), F32),
            jax.ShapeDtypeStruct((1, FF), F32),
        ],
        scratch_shapes=[
            pltpu.VMEM((SP, FF), BF), pltpu.VMEM((SP, FF), BF), pltpu.VMEM((D, D), BF),
            pltpu.VMEM((D, D), F32), pltpu.VMEM((D, FF), F32), pltpu.VMEM((D, FF), F32),
        ],
        compiler_params=params(),
        name="mlp",
    )(tokens, cot, mixed, wide, vec, bup)


class Reduction:
    def __init__(self, dims, copies, packed, bufs, cut):
        self.dims, self.copies, self.packed, self.cut = dims, copies, packed, cut
        self.place = place_of(dims)
        self.along, self.other = peers_of(dims, self.place)
        z, y, x, mp = self.place
        self.p, self.a1, self.b1, self.ra1, self.rb1, self.ra2, self.rb2, self.f, self.rz = bufs
        low, high = pl.ds(0, cut), pl.ds(cut, packed.shape[-1] - cut)
        along = self.along
        copies.plan("pair", [lambda: (packed.at[1 - mp], self.p, self.other)])
        copies.plan("1l", [
            lambda o=o, c=c, d=d: (self.p.at[EVERY, EVERY, c, EVERY, low], self.ra1.at[o], d)
            for o, (c, d) in enumerate(along["x"])
        ])
        copies.plan("1h", [
            lambda o=o, b=b, d=d: (self.p.at[EVERY, b, EVERY, EVERY, high], self.rb1.at[o], d)
            for o, (b, d) in enumerate(along["y"])
        ])
        copies.plan("2l", [
            lambda o=o, b=b, d=d: (self.a1.at[EVERY, b], self.ra2.at[o], d)
            for o, (b, d) in enumerate(along["y"])
        ])
        copies.plan("2h", [
            lambda o=o, c=c, d=d: (self.b1.at[EVERY, c], self.rb2.at[o], d)
            for o, (c, d) in enumerate(along["x"])
        ])
        copies.plan("3", [
            lambda o=o, a=a, d=d: (self.f.at[a], self.rz.at[o], d)
            for o, (a, d) in enumerate(along["z"])
        ])

    @staticmethod
    def count(dims):
        nz, ny, nx = dims
        return 1 + 2 * (ny - 1) + 2 * (nx - 1) + nz - 1

    @staticmethod
    def scratch(dims, rows, width, cut):
        nz, ny, nx = dims

        def buf(w, *shape):
            return pltpu.VMEM((*shape, rows, w), BF)

        rest = width - cut
        return [
            buf(width, nz, ny, nx), buf(cut, nz, ny), buf(rest, nz, nx),
            buf(cut, nx - 1, nz, ny), buf(rest, ny - 1, nz, nx),
            buf(cut, ny - 1, nz), buf(rest, nx - 1, nz), buf(width, nz), buf(width, nz - 1),
        ]

    def add_pair(self, mine):
        nz, ny, nx = self.dims
        for i in range(nz):
            for j in range(ny):
                for k in range(nx):
                    total = mine[i, j, k].astype(F32) + self.p[i, j, k].astype(F32)
                    self.p[i, j, k] = total.astype(BF)

    def add_first_low(self):
        nz, ny, nx = self.dims
        x = self.place[2]
        for i in range(nz):
            for j in range(ny):
                total = self.p[i, j, x, :, : self.cut].astype(F32)
                for o in range(nx - 1):
                    total = total + self.ra1[o, i, j].astype(F32)
                self.a1[i, j] = total.astype(BF)

    def add_first_high(self):
        nz, ny, nx = self.dims
        y = self.place[1]
        for i in range(nz):
            for k in range(nx):
                total = self.p[i, y, k, :, self.cut :].astype(F32)
                for o in range(ny - 1):
                    total = total + self.rb1[o, i, k].astype(F32)
                self.b1[i, k] = total.astype(BF)

    def add_second(self):
        nz, ny, nx = self.dims
        _, y, x, _ = self.place
        for i in range(nz):
            total = self.a1[i, y].astype(F32)
            for o in range(ny - 1):
                total = total + self.ra2[o, i].astype(F32)
            self.f[i, :, : self.cut] = total.astype(BF)
            total = self.b1[i, x].astype(F32)
            for o in range(nx - 1):
                total = total + self.rb2[o, i].astype(F32)
            self.f[i, :, self.cut :] = total.astype(BF)

    def add_third(self):
        total = self.f[self.place[0]].astype(F32)
        for o in range(self.dims[0] - 1):
            total = total + self.rz[o].astype(F32)
        return total


def attn_bwd_kernel(dims, n, qkv_ref, e_ref, mixed_ref, linv_ref, gmix_ref, packed, *refs):
    g_ref, dvec_ref, sum_ref = refs[:3]
    bufs, mine, send, recv, sem = refs[3:12], refs[12], refs[13], refs[14], refs[15]
    i = pl.program_id(0)
    copies = Copies(send, recv)
    red = Reduction(dims, copies, packed, bufs, WIDE_CUT)
    keep = pltpu.make_async_copy(packed.at[red.place[3]], mine, sem)

    @pl.when(i == 0)
    def _():
        dvec_ref[...] = jnp.zeros_like(dvec_ref)
        meet(red.along, red.other)
        copies.start("pair")
        keep.start()

    @pl.when(i == 2)
    def _():
        keep.wait()
        copies.arrived("pair")
        red.add_pair(mine)
        copies.start("1l", "1h")

    @pl.when(i == n // 2 - 1)
    def _():
        copies.arrived("1l", "1h")
        red.add_first_low()
        red.add_first_high()
        copies.start("2l", "2h")

    @pl.when(i == n // 2 + 2)
    def _():
        copies.arrived("2l", "2h")
        red.add_second()
        copies.start("3")

    lane = lax.broadcasted_iota(jnp.int32, (SP, 2 * HD), 1)
    zero = jnp.zeros((SP, 2 * HD), BF)
    minus = jnp.full((SP, 2 * HD), -1.0, BF)
    for p in range(PAIRS):
        lo, hi = 2 * HD * p, 2 * HD * (p + 1)
        q = qkv_ref[0, :, lo:hi]
        k = qkv_ref[0, :, D + lo : D + hi]
        v = qkv_ref[0, :, 2 * D + lo : 2 * D + hi]
        go_f = gmix_ref[0, :, lo:hi].astype(F32) * linv_ref[0, :, lo:hi]
        go = go_f.astype(BF)
        god = jnp.concatenate(
            [go, (go_f * mixed_ref[0, :, lo:hi].astype(F32)).astype(BF)], axis=1
        )
        gq = gk = gv = None
        for h in range(2):
            own = (lane < HD) if h == 0 else (lane >= HD)
            e = e_ref[0, 2 * p + h]
            vd = jnp.concatenate(
                [jnp.where(own, v, zero), jnp.where(own, minus, zero)], axis=1
            )
            ds = e * dot_nt(god, vd).astype(BF)
            part_q = dot_nn(ds, jnp.where(own, k, zero))
            part_k = dot_tn(ds, jnp.where(own, q, zero))
            part_v = dot_tn(e, jnp.where(own, go, zero))
            gq = part_q if gq is None else gq + part_q
            gk = part_k if gk is None else gk + part_k
            gv = part_v if gv is None else gv + part_v
        gq = gq * (1.0 / math.sqrt(HD))
        dvec_ref[0:1, lo:hi] += row_sum(gq)
        dvec_ref[1:2, lo:hi] += row_sum(gv)
        g_ref[0, :, lo:hi] = gq.astype(BF)
        g_ref[0, :, D + lo : D + hi] = (gk * (1.0 / LOG2E)).astype(BF)
        g_ref[0, :, 2 * D + lo : 2 * D + hi] = gv.astype(BF)

    @pl.when(i == n - 1)
    def _():
        copies.arrived("3")
        sum_ref[...] = red.add_third()
        copies.left(*copies.groups)


def attn_bwd(qkv, e, mixed, linv, gmix, packed, dp):
    dims = chip_grid(dp)
    n = qkv.shape[0]
    rows = D // dp
    count = Reduction.count(dims)
    return pl.pallas_call(
        functools.partial(attn_bwd_kernel, dims, n),
        grid=(n,),
        in_specs=[
            per_image(SP, 3 * D), per_image(HEADS, SP, SP), per_image(SP, D), per_image(SP, D),
            per_image(SP, D), pl.BlockSpec(memory_space=pl.ANY),
        ],
        out_specs=[per_image(SP, 3 * D), whole((8, D)), whole((rows, WIDE))],
        out_shape=[
            jax.ShapeDtypeStruct((n, SP, 3 * D), BF),
            jax.ShapeDtypeStruct((8, D), F32),
            jax.ShapeDtypeStruct((rows, WIDE), F32),
        ],
        scratch_shapes=[
            *Reduction.scratch(dims, rows, WIDE, WIDE_CUT),
            pltpu.VMEM((*dims, rows, WIDE), BF),
            pltpu.SemaphoreType.DMA((count,)),
            pltpu.SemaphoreType.DMA((count,)),
            pltpu.SemaphoreType.DMA,
        ],
        compiler_params=params(collective_id=1),
        name="attn_bwd",
    )(qkv, e, mixed, linv, gmix, packed)


def tokens_kernel(
    dims, n, g_ref, normed_ref, inv_ref, gres_ref, w_ref, vec_ref, dvec1_ref, dvec2_ref, dbup_ref,
    gtok_ref, packed_ref, sums_ref, dw_ref, dvec_ref,
):
    i = pl.program_id(0)

    @pl.when(i == 0)
    def _():
        dw_ref[...] = jnp.zeros_like(dw_ref)
        dvec_ref[...] = jnp.zeros_like(dvec_ref)

    g = g_ref[0]
    normed = normed_ref[0]
    inv = inv_ref[0]
    inv = jnp.concatenate([inv, inv, inv], axis=1)
    h1 = (normed * vec_ref[0:1, :] + vec_ref[1:2, :]).astype(BF)
    gh1 = dot_nt(g, w_ref[...])
    dw_ref[...] += dot_tn(h1, g)
    gtok = gres_ref[0] + norm_backward(gh1, normed, inv, vec_ref[0:1, :])
    store_image(gtok_ref, i, gtok)
    dvec_ref[0:1, :] += row_sum(gh1 * normed)
    dvec_ref[1:2, :] += row_sum(gh1)

    @pl.when(i == n - 1)
    def _():
        nz, ny, nx = dims
        rows = packed_ref.shape[4]
        spots = [(a, b, c) for a in range(nz) for b in range(ny) for c in range(nx)]
        group = 48 // rows
        for t in range(len(spots) // group):
            at = slice(48 * t, 48 * (t + 1))
            for m in range(2):
                parts = [
                    dw_ref[at, D * j + THIRD * m : D * j + THIRD * (m + 1)] for j in range(3)
                ]
                parts.append(jnp.zeros((48, NARROW - 3 * THIRD), F32))
                block = jnp.concatenate(parts, axis=1)
                for k in range(group):
                    packed_ref[(m,) + spots[t * group + k]] = block[
                        k * rows : (k + 1) * rows
                    ].astype(BF)
        sums_ref[0:2] = dvec1_ref[0:2]
        sums_ref[2:4] = dvec_ref[0:2]
        sums_ref[4:8] = dvec2_ref[0:4]
        for j in range(FF // D):
            sums_ref[8 + j : 9 + j] = dbup_ref[:, D * j : D * (j + 1)]
        sums_ref[12:16] = jnp.zeros((4, D), F32)


def tokens_grad(g, normed, inv, gres, wqkv, vec, dvec1, dvec2, dbup, rows, dp):
    dims = chip_grid(dp)
    n = g.shape[0]
    packed = (2, *dims, D // dp, NARROW)
    return pl.pallas_call(
        functools.partial(tokens_kernel, dims, n),
        grid=(n,),
        in_specs=[
            per_image(SP, 3 * D), per_image(SP, D), per_image(SP, 128), per_image(SP, D),
            whole((D, 3 * D)), whole((8, D)), whole((8, D)), whole((8, D)), whole((1, FF)),
        ],
        out_specs=[whole((rows, D)), whole(packed), whole((16, D))],
        out_shape=[
            jax.ShapeDtypeStruct((rows, D), F32),
            jax.ShapeDtypeStruct(packed, BF),
            jax.ShapeDtypeStruct((16, D), F32),
        ],
        scratch_shapes=[pltpu.VMEM((D, 3 * D), F32), pltpu.VMEM((8, D), F32)],
        compiler_params=params(),
        name="tokens_grad",
    )(g, normed, inv, gres, wqkv, vec, dvec1, dvec2, dbup)


def reduce_kernel(dims, packed, sums, out_ref, vec_ref, *refs):
    bufs, vs, vr, send, recv = refs[:9], refs[9], refs[10], refs[11], refs[12]
    nz, ny, nx = dims
    copies = Copies(send, recv)
    red = Reduction(dims, copies, packed, bufs, NARROW_CUT)
    mp = red.place[3]
    along, other = red.along, red.other
    stages = [[other], *([d for _, d in along[axis]] for axis in "xyz")]
    base = 0
    bases = []
    for s, devices in enumerate(stages):
        copies.plan("v%d" % s, [
            lambda s=s, at=base + o, d=d: (sums if s == 0 else vs.at[s - 1], vr.at[at], d)
            for o, d in enumerate(devices)
        ])
        bases.append((base, len(devices)))
        base += len(devices)

    def vec_add(stage):
        total = sums[...] if stage == 0 else vs[stage - 1]
        first, count = bases[stage]
        for o in range(count):
            total = total + vr[first + o]
        if stage < 3:
            vs[stage] = total
        else:
            vec_ref[...] = total

    meet(along, other)
    copies.start("pair", "v0")
    copies.arrived("pair", "v0")
    red.add_pair(packed.at[mp])
    vec_add(0)
    copies.start("1l", "1h", "v1")
    copies.arrived("1l", "v1")
    red.add_first_low()
    vec_add(1)
    copies.start("2l", "v2")
    copies.arrived("1h")
    red.add_first_high()
    copies.start("2h")
    copies.arrived("2l", "2h", "v2")
    red.add_second()
    vec_add(2)
    copies.start("3", "v3")
    copies.arrived("3", "v3")
    out_ref[...] = red.add_third()
    vec_add(3)
    copies.left(*copies.groups)


def reduce(packed, sums, dp):
    dims = chip_grid(dp)
    nz, ny, nx = dims
    rows = D // dp
    count = Reduction.count(dims) + nz + ny + nx - 2
    vmem = pl.BlockSpec(memory_space=pltpu.VMEM)
    return pl.pallas_call(
        functools.partial(reduce_kernel, dims),
        in_specs=[vmem] * 2,
        out_specs=[vmem] * 2,
        out_shape=[
            jax.ShapeDtypeStruct((rows, NARROW), F32),
            jax.ShapeDtypeStruct((16, D), F32),
        ],
        scratch_shapes=[
            *Reduction.scratch(dims, rows, NARROW, NARROW_CUT),
            pltpu.VMEM((3, 16, D), F32),
            pltpu.VMEM((nz + ny + nx - 2, 16, D), F32),
            pltpu.SemaphoreType.DMA((count,)),
            pltpu.SemaphoreType.DMA((count,)),
        ],
        compiler_params=pltpu.CompilerParams(
            collective_id=2, has_side_effects=True, vmem_limit_bytes=48 * 1024 * 1024
        ),
        name="reduce",
    )(packed, sums)


def split_kernel(n, narrow_ref, wide_ref, vec_ref, *outs):
    for j in range(3):
        outs[j][...] = narrow_ref[:, THIRD * j : THIRD * (j + 1)]
    outs[3][...] = wide_ref[:, :THIRD]
    outs[4][...] = wide_ref[:, OUT_PAD : OUT_PAD + HALF]
    outs[5][...] = wide_ref[:, OUT_PAD + HALF :]
    index = lax.axis_index("dp") * 2 + lax.axis_index("mp")
    per = D // n
    vec = pltpu.roll(vec_ref[...], D - index * per, axis=1)
    for row, out in zip((2, 3, 0, 1, 4, 5, 6, 7), outs[6:]):
        out[...] = vec[row : row + 1, :per]
    wide = jnp.concatenate([vec_ref[8 + j : 9 + j, :] for j in range(FF // D)], axis=1)
    wide = pltpu.roll(jnp.broadcast_to(wide, (8, FF)), FF - index * (FF // n), axis=1)
    outs[14][...] = wide[0:1, : FF // n]


def split(narrow, wide, vec, n):
    rows = narrow.shape[0]
    vmem = pl.BlockSpec(memory_space=pltpu.VMEM)
    shapes = [(rows, THIRD)] * 4 + [(rows, HALF)] * 2 + [(1, D // n)] * 8 + [(1, FF // n)]
    return pl.pallas_call(
        functools.partial(split_kernel, n),
        in_specs=[vmem] * 3,
        out_specs=[vmem] * 15,
        out_shape=[jax.ShapeDtypeStruct(s, F32) for s in shapes],
        name="split",
    )(narrow, wide, vec)


def whole(shape):
    return pl.BlockSpec(shape, lambda i: (0,) * len(shape))


def per_image(*shape):
    return pl.BlockSpec((1, *shape), lambda i: (i,) + (0,) * len(shape))


def params(collective_id=None):
    return pltpu.CompilerParams(
        dimension_semantics=("arbitrary",), vmem_limit_bytes=62 * 1024 * 1024,
        collective_id=collective_id, has_side_effects=collective_id is not None,
    )


def on_device(
    tokens, w_query, w_key, w_value, w_out, w_up, w_down, ln1_gain, ln1_bias, b_query, b_value,
    b_out, ln2_gain, ln2_bias, b_up, b_down, cotangent,
):
    dp = lax.axis_size("dp")
    vectors = (ln1_gain, ln1_bias, b_query, b_value, b_out, ln2_gain, ln2_bias, b_down)
    qkv, e, mixed, linv, normed, inv, wqkv, vec, bup, wide = attn_fwd(
        (w_query, w_key, w_value, w_out.T, w_up, w_down.T), [v[None] for v in vectors], b_up[None],
        tokens, dp,
    )
    out, gres, gmix, packed, dvec2, dbup = mlp(
        tokens, cotangent, mixed, wide.reshape(2, D, WIDE), vec, bup, dp
    )
    g, dvec1, wide_sum = attn_bwd(qkv, e, mixed, linv, gmix, packed, dp)
    gtok, packed, sums = tokens_grad(
        g, normed, inv, gres, wqkv, vec, dvec1, dvec2, dbup, tokens.shape[0], dp
    )
    narrow_sum, sums = reduce(packed, sums, dp)
    grads = split(narrow_sum, wide_sum, sums, dp * lax.axis_size("mp"))
    vecs = [v.reshape(-1) for v in grads[6:]]
    return (
        out, gtok, grads[0], grads[1], grads[2], grads[3].T, grads[4], grads[5].T,
        *vecs[:7], vecs[8], vecs[7],
    )


def solution(mesh):
    row, mat, tam, vec = P(("dp", "mp"), None), P("dp", "mp"), P("mp", "dp"), P("dp")
    part = P(("dp", "mp"))
    return jax.shard_map(
        on_device,
        mesh=mesh,
        in_specs=(row, mat, mat, mat, tam, mat, tam, *([vec] * 9), row),
        out_specs=(row, row, mat, mat, mat, tam, mat, tam, *([part] * 9)),
        check_vma=False,
    )
```

```python
import functools
import math

import jax
import jax.numpy as jnp
from jax import lax
from jax.experimental import pallas as pl
from jax.experimental.pallas import tpu as pltpu
from jax.sharding import PartitionSpec as P

D = 384
HD = 64
FF = 1536
S = 197
HEADS = D // HD
PAIRS = HEADS // 2

SP = 208
WIN = 224

EPS = 1e-06
RSQRT2 = 0.7071067811865476
RSQRT_TAU = 0.3989422804014327
LOG2E = 1.4426950408889634
Q_SCALE = LOG2E / math.sqrt(HD)
BF = jnp.bfloat16
F32 = jnp.float32


def dot_nn(a, b):
    return lax.dot_general(a, b, (((1,), (0,)), ((), ())), preferred_element_type=F32)


def dot_nt(a, b):
    return lax.dot_general(a, b, (((1,), (1,)), ((), ())), preferred_element_type=F32)


def dot_tn(a, b):
    return lax.dot_general(a, b, (((0,), (0,)), ((), ())), preferred_element_type=F32)


def window_of(i, rows):
    start = i * S
    base = jnp.minimum((start // 16) * 16, rows - WIN)
    return pl.multiple_of(base, 16), start - base


def load_image(ref, i):
    base, off = window_of(i, ref.shape[0])
    rows = ref[pl.ds(base, WIN), :].astype(F32)
    rows = pltpu.roll(rows, WIN - off, axis=0)[:SP]
    live = lax.broadcasted_iota(jnp.int32, rows.shape, 0) < S
    return jnp.where(live, rows, 0.0)


def store_image(ref, i, rows):
    base, off = window_of(i, ref.shape[0])
    rows = jnp.concatenate([rows, jnp.zeros((WIN - SP, rows.shape[1]), F32)], axis=0)
    rows = pltpu.roll(rows, off, axis=0)
    old = ref[pl.ds(base, WIN), :].astype(F32)
    mine = lax.broadcasted_iota(jnp.int32, rows.shape, 0) >= off
    ref[pl.ds(base, WIN), :] = jnp.where(mine, rows, old).astype(ref.dtype)


def norm_stats(x):
    mean = jnp.mean(x, axis=-1, keepdims=True)
    centred = x - mean
    inv = lax.rsqrt(jnp.mean(centred * centred, axis=-1, keepdims=True) + EPS)
    return centred * inv, inv


def norm_backward(grad, normed, inv, gain):
    e = grad * gain
    return inv * (
        e
        - jnp.mean(e, axis=-1, keepdims=True)
        - normed * jnp.mean(e * normed, axis=-1, keepdims=True)
    )


def row_sum(x):
    return jnp.sum(x, axis=0, keepdims=True)


THIRD = D // 2
HALF = FF // 2
NARROW = 640
NARROW_CUT = 384
OUT_PAD = 256
WIDE = OUT_PAD + 2 * HALF
WIDE_CUT = 896
MESH = pl.DeviceIdType.MESH
EVERY = slice(None)


def chip_grid(dp):
    side = math.isqrt(dp // 4)
    return 4, side, side


def place_of(dims):
    _, ny, nx = dims
    dp, mp = lax.axis_index("dp"), lax.axis_index("mp")
    return dp // (ny * nx), (dp // nx) % ny, dp % nx, mp


def peers_of(dims, place):
    (nz, ny, nx), (z, y, x, mp) = dims, place

    def at(a, b, c, m):
        return ((a * ny + b) * nx + c, m)

    along = {
        "z": [((z + o) % nz, at((z + o) % nz, y, x, mp)) for o in range(1, nz)],
        "y": [((y + o) % ny, at(z, (y + o) % ny, x, mp)) for o in range(1, ny)],
        "x": [((x + o) % nx, at(z, y, (x + o) % nx, mp)) for o in range(1, nx)],
    }
    return along, at(z, y, x, 1 - mp)


def greet(along, other):
    for device in [d for peers in along.values() for _, d in peers] + [other]:
        pl.semaphore_signal(
            pltpu.get_barrier_semaphore(), inc=1, device_id=device, device_id_type=MESH
        )


def met(along):
    count = sum(len(peers) for peers in along.values()) + 1
    pl.semaphore_wait(pltpu.get_barrier_semaphore(), count)


class Copies:
    def __init__(self, send, recv):
        self.send, self.recv, self.groups, self.count = send, recv, {}, 0

    def plan(self, name, makers):
        self.groups[name] = [(self.count + i, m) for i, m in enumerate(makers)]
        self.count += len(makers)

    def each(self, names):
        for name in names:
            for index, make in self.groups[name]:
                src, dst, device = make()
                yield pltpu.make_async_remote_copy(
                    src_ref=src, dst_ref=dst, send_sem=self.send.at[index],
                    recv_sem=self.recv.at[index], device_id=device, device_id_type=MESH,
                )

    def start(self, *names):
        for copy in self.each(names):
            copy.start()

    def arrived(self, *names):
        for copy in self.each(names):
            copy.wait_recv()

    def left(self, *names):
        for copy in self.each(names):
            copy.wait_send()


def plan_gather(copies, tag, w, own, cut, along, other, place):
    z, y, x, mp = place
    low, high = pl.ds(0, cut), pl.ds(cut, w.shape[-1] - cut)

    def same(index, device):
        return lambda: (w.at[index], w.at[index], device)

    def spread(index, axis):
        return [same(index, d) for _, d in along[axis]]

    def shares(indices):
        return [same(index, other) for index in indices]

    copies.plan(tag + "1", [lambda d=d: (own, w.at[mp, z, y, x], d) for _, d in along["z"]])
    copies.plan(tag + "2l", spread((mp, EVERY, y, x, EVERY, low), "y"))
    copies.plan(tag + "2h", spread((mp, EVERY, y, x, EVERY, high), "x"))
    copies.plan(tag + "3l", spread((mp, EVERY, EVERY, x, EVERY, low), "x"))
    copies.plan(tag + "3h", spread((mp, EVERY, y, EVERY, EVERY, high), "y"))
    copies.plan(tag + "s1", shares([(mp, EVERY, y, x)]))
    copies.plan(tag + "s2l", shares([(mp, EVERY, b, x, EVERY, low) for b, _ in along["y"]]))
    copies.plan(tag + "s2h", shares([(mp, EVERY, y, c, EVERY, high) for c, _ in along["x"]]))
    copies.plan(tag + "s3l", shares([(mp, EVERY, EVERY, c, EVERY, low) for c, _ in along["x"]]))
    copies.plan(tag + "s3h", shares([(mp, EVERY, b, EVERY, EVERY, high) for b, _ in along["y"]]))


def attn_fwd_kernel(dims, n, *refs):
    (wq, wk, wv, wot, wu, wdt), vectors, bup_in, tok_ref = refs[:6], refs[6:14], refs[14], refs[15]
    (qkv_ref, e_ref, mixed_ref, linv_ref, normed_ref, inv_ref, w_ref, vec_ref, bup_ref, wide) = refs[
        16:26
    ]
    narrow, v, own, normed_all, inv_all, send, recv, sem = refs[26:]
    i = pl.program_id(0)
    nz, ny, nx = dims
    place = place_of(dims)
    z, y, x, mp = place
    rows = own.shape[0]
    along, other = peers_of(dims, place)
    copies = Copies(send, recv)
    plan_gather(copies, "n", narrow, narrow.at[mp, z, y, x], NARROW_CUT, along, other, place)
    plan_gather(copies, "w", wide, own, WIDE_CUT, along, other, place)

    def vec_spread(index, axis):
        return [lambda d=d: (v.at[index], v.at[index], d) for _, d in along[axis]]

    copies.plan("v1", vec_spread((z, y, x), "z"))
    copies.plan("v2", vec_spread((EVERY, y, x), "y"))
    copies.plan("v3", vec_spread((EVERY, EVERY, x), "x"))
    keep = pltpu.make_async_copy(own, wide.at[mp, z, y, x], sem)

    def norms(first, last):
        @pl.loop(first, last)
        def _(j):
            normed, inv = norm_stats(load_image(tok_ref, j))
            normed_all[j] = normed
            inv_all[j] = jnp.broadcast_to(inv, (SP, 128))

    @pl.when(i == 0)
    def _():
        narrow[mp, z, y, x] = jnp.concatenate(
            [wq[...], wk[...], wv[...], jnp.zeros((rows, NARROW - 3 * THIRD), BF)], axis=1
        )
        own[...] = jnp.concatenate(
            [wot[...], jnp.zeros((rows, OUT_PAD - THIRD), BF), wu[...], wdt[...]], axis=1
        )
        v[z, y, x] = jnp.zeros((16, 128), F32)
        for j, vector in enumerate(vectors):
            v[z, y, x, j : j + 1, :rows] = vector[...].astype(F32)
        v[z, y, x, 8:9, : bup_in.shape[1]] = bup_in[...].astype(F32)
        greet(along, other)
        keep.start()
        norms(0, n // 4)
        met(along)
        copies.start("v1", "n1")
        norms(n // 4, n // 2)
        copies.arrived("v1", "n1")
        copies.start("v2", "n2l", "n2h", "w1", "ns1")
        norms(n // 2, (3 * n) // 4)
        copies.arrived("v2", "n2l", "n2h")
        copies.start("v3", "n3l", "n3h", "ns2l", "ns2h")
        norms((3 * n) // 4, n)
        copies.arrived("v3", "n3l")
        copies.start("ns3l")
        copies.arrived("n3h")
        copies.start("ns3h")
        keep.wait()
        copies.arrived("w1")
        copies.start("w2l", "w2h", "ws1")
        spots = [(a, b, c) for a in range(nz) for b in range(ny) for c in range(nx)]
        vec_ref[...] = jnp.concatenate([v[s][0:8, :rows] for s in spots], axis=1)
        bup_ref[...] = jnp.concatenate([v[s][8:9, : bup_in.shape[1]] for s in spots], axis=1)
        copies.arrived("ns1", "ns2l", "ns2h", "ns3l", "ns3h")
        group = 48 // rows
        for t in range(len(spots) // group):
            block = [
                jnp.concatenate(
                    [narrow[(m,) + s].astype(F32) for s in spots[t * group : (t + 1) * group]], axis=0
                )
                for m in range(2)
            ]
            for j in range(3):
                cols = slice(THIRD * j, THIRD * (j + 1))
                w_ref[48 * t : 48 * (t + 1), D * j : D * (j + 1)] = jnp.concatenate(
                    [half[:, cols] for half in block], axis=1
                ).astype(BF)

    @pl.when(i == 3)
    def _():
        copies.arrived("w2l", "w2h")
        copies.start("w3l", "w3h", "ws2l", "ws2h")

    normed = normed_all[i]
    normed_ref[0] = normed
    inv_ref[0] = inv_all[i]
    h1 = (normed * vec_ref[0:1, :] + vec_ref[1:2, :]).astype(BF)
    q = ((dot_nn(h1, w_ref[:, 0:D]) + vec_ref[2:3, :]) * Q_SCALE).astype(BF)
    k = dot_nn(h1, w_ref[:, D : 2 * D]).astype(BF)
    value = (dot_nn(h1, w_ref[:, 2 * D :]) + vec_ref[3:4, :]).astype(BF)
    qkv_ref[0, :, 0:D] = q
    qkv_ref[0, :, D : 2 * D] = k
    qkv_ref[0, :, 2 * D :] = value
    lane = lax.broadcasted_iota(jnp.int32, (SP, 2 * HD), 1)
    is_key = lax.broadcasted_iota(jnp.int32, (SP, SP), 1) < S
    zero = jnp.zeros((SP, 2 * HD), BF)
    one = jnp.ones((SP, 2 * HD), BF)
    for p in range(PAIRS):
        cols = slice(2 * HD * p, 2 * HD * (p + 1))
        total = None
        for h in range(2):
            mine = (lane < HD) if h == 0 else (lane >= HD)
            kh = jnp.where(mine, k[:, cols], zero)
            vh = jnp.where(mine, value[:, cols], zero)
            scores = dot_nt(q[:, cols], kh)
            scores = jnp.where(is_key, scores, -1e30)
            top = jnp.max(scores, axis=-1, keepdims=True)
            e = jnp.exp2(scores - top).astype(BF)
            e_ref[0, 2 * p + h] = e
            part = dot_nn(e, jnp.concatenate([vh, jnp.where(mine, one, zero)], axis=1))
            total = part if total is None else total + part
        linv = 1.0 / total[:, 2 * HD :]
        linv_ref[0, :, cols] = linv
        mixed_ref[0, :, cols] = (total[:, : 2 * HD] * linv).astype(BF)

    @pl.when(i == n - 5)
    def _():
        copies.arrived("w3l", "w3h")
        copies.start("ws3l", "ws3h")

    @pl.when(i == n - 1)
    def _():
        copies.arrived("ws1", "ws2l", "ws2h", "ws3l", "ws3h")
        copies.left(*copies.groups)


def attn_fwd(mats, vectors, bup, tokens, dp):
    dims = chip_grid(dp)
    nz, ny, nx = dims
    rows = D // dp
    n = tokens.shape[0] // S
    count = 2 * (nz - 1 + 4 * (ny - 1) + 4 * (nx - 1) + 1) + nz + ny + nx - 3
    inputs = (*mats, *vectors, bup, tokens)
    return pl.pallas_call(
        functools.partial(attn_fwd_kernel, dims, n),
        grid=(n,),
        in_specs=[whole(a.shape) for a in inputs],
        out_specs=[
            per_image(SP, 3 * D), per_image(HEADS, SP, SP), per_image(SP, D), per_image(SP, D),
            per_image(SP, D), per_image(SP, 128), whole((D, 3 * D)), whole((8, D)), whole((1, FF)),
            pl.BlockSpec(memory_space=pl.ANY),
        ],
        out_shape=[
            jax.ShapeDtypeStruct((n, SP, 3 * D), BF),
            jax.ShapeDtypeStruct((n, HEADS, SP, SP), BF),
            jax.ShapeDtypeStruct((n, SP, D), BF),
            jax.ShapeDtypeStruct((n, SP, D), F32),
            jax.ShapeDtypeStruct((n, SP, D), F32),
            jax.ShapeDtypeStruct((n, SP, 128), F32),
            jax.ShapeDtypeStruct((D, 3 * D), BF),
            jax.ShapeDtypeStruct((8, D), F32),
            jax.ShapeDtypeStruct((1, FF), F32),
            jax.ShapeDtypeStruct((2, nz, ny, nx, rows, WIDE), BF),
        ],
        scratch_shapes=[
            pltpu.VMEM((2, nz, ny, nx, rows, NARROW), BF),
            pltpu.VMEM((nz, ny, nx, 16, 128), F32),
            pltpu.VMEM((rows, WIDE), BF),
            pltpu.VMEM((n, SP, D), F32),
            pltpu.VMEM((n, SP, 128), F32),
            pltpu.SemaphoreType.DMA((count,)),
            pltpu.SemaphoreType.DMA((count,)),
            pltpu.SemaphoreType.DMA,
        ],
        compiler_params=params(collective_id=0),
        name="attn_fwd",
    )(*inputs)


def mlp_kernel(
    dims, n, tok_ref, cot_ref, mixed_ref, w_ref, vec_ref, bup_ref,
    out_ref, gres_ref, gmix_ref, grads_ref, dvec_ref, dbup_ref,
    act_ref, gp_ref, wot_ref, dwot_ref, dwup_ref, dwdt_ref,
):
    i = pl.program_id(0)

    @pl.when(i == 0)
    def _():
        wot_ref[...] = jnp.concatenate([w_ref[0, :, :THIRD], w_ref[1, :, :THIRD]], axis=1)
        dwot_ref[...] = jnp.zeros_like(dwot_ref)
        dwup_ref[...] = jnp.zeros_like(dwup_ref)
        dwdt_ref[...] = jnp.zeros_like(dwdt_ref)
        dvec_ref[...] = jnp.zeros_like(dvec_ref)
        dbup_ref[...] = jnp.zeros_like(dbup_ref)

    mixed = mixed_ref[0]
    cot_f = load_image(cot_ref, i)
    cot = cot_f.astype(BF)
    resid = load_image(tok_ref, i) + dot_nt(mixed, wot_ref[...]) + vec_ref[4:5, :]
    normed, inv = norm_stats(resid)
    h2 = (normed * vec_ref[5:6, :] + vec_ref[6:7, :]).astype(BF)
    step = 256
    for j in range(FF // step):
        cols = slice(step * j, step * (j + 1))
        m, at = divmod(step * j, HALF)
        u = dot_nn(h2, w_ref[m, :, OUT_PAD + at : OUT_PAD + at + step]) + bup_ref[:, cols]
        ga = dot_nn(cot, w_ref[m, :, OUT_PAD + HALF + at : OUT_PAD + HALF + at + step])
        cdf = 0.5 * (1.0 + lax.erf(u * RSQRT2))
        act_ref[:, cols] = (u * cdf).astype(BF)
        gp = ga * (cdf + u * jnp.exp(-0.5 * u * u) * RSQRT_TAU)
        dbup_ref[:, cols] += row_sum(gp)
        gp_ref[:, cols] = gp.astype(BF)
    out = resid + vec_ref[7:8, :]
    gh2 = None
    for m in range(2):
        cols = slice(HALF * m, HALF * (m + 1))
        out = out + dot_nt(act_ref[:, cols], w_ref[m, :, OUT_PAD + HALF :])
        part = dot_nt(gp_ref[:, cols], w_ref[m, :, OUT_PAD : OUT_PAD + HALF])
        gh2 = part if gh2 is None else gh2 + part
    store_image(out_ref, i, out)
    gres = cot_f + norm_backward(gh2, normed, inv, vec_ref[5:6, :])
    gres_ref[0] = gres
    gr = gres.astype(BF)
    gmix_ref[0] = dot_nn(gr, wot_ref[...]).astype(BF)
    dwot_ref[...] += dot_tn(gr, mixed)
    dwup_ref[...] += dot_tn(h2, gp_ref[...])
    dwdt_ref[...] += dot_tn(cot, act_ref[...])
    dvec_ref[0:1, :] += row_sum(gres)
    dvec_ref[1:2, :] += row_sum(gh2 * normed)
    dvec_ref[2:3, :] += row_sum(gh2)
    dvec_ref[3:4, :] += row_sum(cot_f)

    @pl.when(i == n - 1)
    def _():
        nz, ny, nx = dims
        rows = grads_ref.shape[4]
        spots = [(a, b, c) for a in range(nz) for b in range(ny) for c in range(nx)]
        group = 48 // rows
        for t in range(len(spots) // group):
            at = slice(48 * t, 48 * (t + 1))
            for m in range(2):
                parts = [
                    dwot_ref[at, THIRD * m : THIRD * (m + 1)],
                    jnp.zeros((48, OUT_PAD - THIRD), F32),
                    dwup_ref[at, HALF * m : HALF * (m + 1)],
                    dwdt_ref[at, HALF * m : HALF * (m + 1)],
                ]
                block = jnp.concatenate(parts, axis=1)
                for g in range(group):
                    grads_ref[(m,) + spots[t * group + g]] = block[
                        g * rows : (g + 1) * rows
                    ].astype(BF)


def mlp(tokens, cot, mixed, wide, vec, bup, dp):
    dims = chip_grid(dp)
    rows = tokens.shape[0]
    n = rows // S
    packed = (2, *dims, D // dp, WIDE)
    return pl.pallas_call(
        functools.partial(mlp_kernel, dims, n),
        grid=(n,),
        in_specs=[
            whole((rows, D)), whole((rows, D)), per_image(SP, D), whole((2, D, WIDE)), whole((8, D)),
            whole((1, FF)),
        ],
        out_specs=[
            whole((rows, D)), per_image(SP, D), per_image(SP, D), whole(packed), whole((8, D)),
            whole((1, FF)),
        ],
        out_shape=[
            jax.ShapeDtypeStruct((rows, D), BF),
            jax.ShapeDtypeStruct((n, SP, D), F32),
            jax.ShapeDtypeStruct((n, SP, D), BF),
            jax.ShapeDtypeStruct(packed, BF),
            jax.ShapeDtypeStruct((8, D), F32),
            jax.ShapeDtypeStruct((1, FF), F32),
        ],
        scratch_shapes=[
            pltpu.VMEM((SP, FF), BF), pltpu.VMEM((SP, FF), BF), pltpu.VMEM((D, D), BF),
            pltpu.VMEM((D, D), F32), pltpu.VMEM((D, FF), F32), pltpu.VMEM((D, FF), F32),
        ],
        compiler_params=params(),
        name="mlp",
    )(tokens, cot, mixed, wide, vec, bup)


class Reduction:
    def __init__(self, dims, copies, packed, bufs, cut):
        self.dims, self.copies, self.packed, self.cut = dims, copies, packed, cut
        self.place = place_of(dims)
        self.along, self.other = peers_of(dims, self.place)
        z, y, x, mp = self.place
        self.p, self.a1, self.b1, self.ra1, self.rb1, self.ra2, self.rb2, self.f, self.rz = bufs
        low, high = pl.ds(0, cut), pl.ds(cut, packed.shape[-1] - cut)
        along = self.along
        copies.plan("pair", [lambda: (packed.at[1 - mp], self.p, self.other)])
        copies.plan("1l", [
            lambda o=o, c=c, d=d: (self.p.at[EVERY, EVERY, c, EVERY, low], self.ra1.at[o], d)
            for o, (c, d) in enumerate(along["x"])
        ])
        copies.plan("1h", [
            lambda o=o, b=b, d=d: (self.p.at[EVERY, b, EVERY, EVERY, high], self.rb1.at[o], d)
            for o, (b, d) in enumerate(along["y"])
        ])
        copies.plan("2l", [
            lambda o=o, b=b, d=d: (self.a1.at[EVERY, b], self.ra2.at[o], d)
            for o, (b, d) in enumerate(along["y"])
        ])
        copies.plan("2h", [
            lambda o=o, c=c, d=d: (self.b1.at[EVERY, c], self.rb2.at[o], d)
            for o, (c, d) in enumerate(along["x"])
        ])
        copies.plan("3", [
            lambda o=o, a=a, d=d: (self.f.at[a], self.rz.at[o], d)
            for o, (a, d) in enumerate(along["z"])
        ])

    @staticmethod
    def count(dims):
        nz, ny, nx = dims
        return 1 + 2 * (ny - 1) + 2 * (nx - 1) + nz - 1

    @staticmethod
    def scratch(dims, rows, width, cut):
        nz, ny, nx = dims

        def buf(w, *shape):
            return pltpu.VMEM((*shape, rows, w), BF)

        rest = width - cut
        return [
            buf(width, nz, ny, nx), buf(cut, nz, ny), buf(rest, nz, nx),
            buf(cut, nx - 1, nz, ny), buf(rest, ny - 1, nz, nx),
            buf(cut, ny - 1, nz), buf(rest, nx - 1, nz), buf(width, nz), buf(width, nz - 1),
        ]

    def add_pair(self, mine):
        nz, ny, nx = self.dims
        for i in range(nz):
            for j in range(ny):
                for k in range(nx):
                    total = mine[i, j, k].astype(F32) + self.p[i, j, k].astype(F32)
                    self.p[i, j, k] = total.astype(BF)

    def add_first_low(self):
        nz, ny, nx = self.dims
        x = self.place[2]
        for i in range(nz):
            for j in range(ny):
                total = self.p[i, j, x, :, : self.cut].astype(F32)
                for o in range(nx - 1):
                    total = total + self.ra1[o, i, j].astype(F32)
                self.a1[i, j] = total.astype(BF)

    def add_first_high(self):
        nz, ny, nx = self.dims
        y = self.place[1]
        for i in range(nz):
            for k in range(nx):
                total = self.p[i, y, k, :, self.cut :].astype(F32)
                for o in range(ny - 1):
                    total = total + self.rb1[o, i, k].astype(F32)
                self.b1[i, k] = total.astype(BF)

    def add_second(self):
        nz, ny, nx = self.dims
        _, y, x, _ = self.place
        for i in range(nz):
            total = self.a1[i, y].astype(F32)
            for o in range(ny - 1):
                total = total + self.ra2[o, i].astype(F32)
            self.f[i, :, : self.cut] = total.astype(BF)
            total = self.b1[i, x].astype(F32)
            for o in range(nx - 1):
                total = total + self.rb2[o, i].astype(F32)
            self.f[i, :, self.cut :] = total.astype(BF)

    def add_third(self):
        total = self.f[self.place[0]].astype(F32)
        for o in range(self.dims[0] - 1):
            total = total + self.rz[o].astype(F32)
        return total


def attn_bwd_kernel(
    dims, n, qkv_ref, e_ref, mixed_ref, linv_ref, gmix_ref, normed_ref, w_ref, vec_ref, dvec2_ref,
    dbup_ref, packed, *refs,
):
    g_ref, narrow_ref, sums_ref, sum_ref = refs[:4]
    acc_ref, gsum_ref, bufs, mine, send, recv, sem = refs[4], refs[5], refs[6:15], *refs[15:]
    i = pl.program_id(0)
    copies = Copies(send, recv)
    red = Reduction(dims, copies, packed, bufs, WIDE_CUT)
    keep = pltpu.make_async_copy(packed.at[red.place[3]], mine, sem)

    @pl.when(i == 0)
    def _():
        acc_ref[...] = jnp.zeros_like(acc_ref)
        gsum_ref[...] = jnp.zeros_like(gsum_ref)
        greet(red.along, red.other)
        keep.start()

    @pl.when(i == 1)
    def _():
        met(red.along)
        copies.start("pair")

    @pl.when(i == 3)
    def _():
        keep.wait()
        copies.arrived("pair")
        red.add_pair(mine)
        copies.start("1l", "1h")

    @pl.when(i == n // 2 - 1)
    def _():
        copies.arrived("1l", "1h")
        red.add_first_low()
        red.add_first_high()
        copies.start("2l", "2h")

    @pl.when(i == n // 2 + 2)
    def _():
        copies.arrived("2l", "2h")
        red.add_second()
        copies.start("3")

    lane = lax.broadcasted_iota(jnp.int32, (SP, 2 * HD), 1)
    zero = jnp.zeros((SP, 2 * HD), BF)
    minus = jnp.full((SP, 2 * HD), -1.0, BF)
    for p in range(PAIRS):
        lo, hi = 2 * HD * p, 2 * HD * (p + 1)
        q = qkv_ref[0, :, lo:hi]
        k = qkv_ref[0, :, D + lo : D + hi]
        v = qkv_ref[0, :, 2 * D + lo : 2 * D + hi]
        go_f = gmix_ref[0, :, lo:hi].astype(F32) * linv_ref[0, :, lo:hi]
        go = go_f.astype(BF)
        god = jnp.concatenate(
            [go, (go_f * mixed_ref[0, :, lo:hi].astype(F32)).astype(BF)], axis=1
        )
        gq = gk = gv = None
        for h in range(2):
            own = (lane < HD) if h == 0 else (lane >= HD)
            e = e_ref[0, 2 * p + h]
            vd = jnp.concatenate(
                [jnp.where(own, v, zero), jnp.where(own, minus, zero)], axis=1
            )
            ds = e * dot_nt(god, vd).astype(BF)
            part_q = dot_nn(ds, jnp.where(own, k, zero))
            part_k = dot_tn(ds, jnp.where(own, q, zero))
            part_v = dot_tn(e, jnp.where(own, go, zero))
            gq = part_q if gq is None else gq + part_q
            gk = part_k if gk is None else gk + part_k
            gv = part_v if gv is None else gv + part_v
        gq = gq * (1.0 / math.sqrt(HD))
        gk = gk * (1.0 / LOG2E)
        for j, grad in enumerate((gq, gk, gv)):
            gsum_ref[0:1, D * j + lo : D * j + hi] += row_sum(grad)
            g_ref[0, :, D * j + lo : D * j + hi] = grad.astype(BF)
    acc_ref[...] += dot_tn(normed_ref[0].astype(BF), g_ref[0])

    @pl.when(i == n - 1)
    def _():
        copies.arrived("3")
        sum_ref[...] = red.add_third()
        nz, ny, nx = dims
        rows = narrow_ref.shape[4]
        spots = [(a, b, c) for a in range(nz) for b in range(ny) for c in range(nx)]
        group = 48 // rows
        turned = vec_ref[...].T
        gsum = gsum_ref[0:1, :]
        gains = []
        for t in range(len(spots) // group):
            at = slice(48 * t, 48 * (t + 1))
            acc = acc_ref[at, :]
            gains.append(jnp.sum(acc * w_ref[at, :].astype(F32), axis=1, keepdims=True))
            dw = acc * turned[at, 0:1] + turned[at, 1:2] * gsum
            for m in range(2):
                parts = [dw[:, D * j + THIRD * m : D * j + THIRD * (m + 1)] for j in range(3)]
                parts.append(jnp.zeros((48, NARROW - 3 * THIRD), F32))
                block = jnp.concatenate(parts, axis=1)
                for k in range(group):
                    narrow_ref[(m,) + spots[t * group + k]] = block[
                        k * rows : (k + 1) * rows
                    ].astype(BF)
        high = gsum.astype(BF)
        low = (gsum - high.astype(F32)).astype(BF)
        row = lax.broadcasted_iota(jnp.int32, (16, 3 * D), 0)
        both = jnp.where(row == 0, high, jnp.where(row == 1, low, jnp.zeros((16, 3 * D), BF)))
        sums_ref[0:1] = gsum[:, :D]
        sums_ref[1:2] = gsum[:, 2 * D :]
        gain = jnp.broadcast_to(jnp.concatenate(gains, axis=0), (D, 128)).T
        sums_ref[2:3] = gain[0:1, :]
        sums_ref[3:4] = row_sum(dot_nt(both, w_ref[...]))
        sums_ref[4:8] = dvec2_ref[0:4]
        for j in range(FF // D):
            sums_ref[8 + j : 9 + j] = dbup_ref[:, D * j : D * (j + 1)]
        sums_ref[12:16] = jnp.zeros((4, D), F32)
        copies.left(*copies.groups)


def attn_bwd(qkv, e, mixed, linv, gmix, normed, wqkv, vec, dvec2, dbup, packed, dp):
    dims = chip_grid(dp)
    n = qkv.shape[0]
    rows = D // dp
    count = Reduction.count(dims)
    narrow = (2, *dims, rows, NARROW)
    return pl.pallas_call(
        functools.partial(attn_bwd_kernel, dims, n),
        grid=(n,),
        in_specs=[
            per_image(SP, 3 * D), per_image(HEADS, SP, SP), per_image(SP, D), per_image(SP, D),
            per_image(SP, D), per_image(SP, D), whole((D, 3 * D)), whole((8, D)), whole((8, D)),
            whole((1, FF)), pl.BlockSpec(memory_space=pl.ANY),
        ],
        out_specs=[
            per_image(SP, 3 * D), whole(narrow), whole((16, D)), whole((rows, WIDE)),
        ],
        out_shape=[
            jax.ShapeDtypeStruct((n, SP, 3 * D), BF),
            jax.ShapeDtypeStruct(narrow, BF),
            jax.ShapeDtypeStruct((16, D), F32),
            jax.ShapeDtypeStruct((rows, WIDE), F32),
        ],
        scratch_shapes=[
            pltpu.VMEM((D, 3 * D), F32),
            pltpu.VMEM((8, 3 * D), F32),
            *Reduction.scratch(dims, rows, WIDE, WIDE_CUT),
            pltpu.VMEM((*dims, rows, WIDE), BF),
            pltpu.SemaphoreType.DMA((count,)),
            pltpu.SemaphoreType.DMA((count,)),
            pltpu.SemaphoreType.DMA,
        ],
        compiler_params=params(collective_id=1),
        name="attn_bwd",
    )(qkv, e, mixed, linv, gmix, normed, wqkv, vec, dvec2, dbup, packed)


def tokens_kernel(
    dims, n, g_ref, normed_ref, inv_ref, gres_ref, w_ref, vec_ref, sums, packed, *refs
):
    gtok_ref, sum_ref, total_ref = refs[:3]
    bufs, mine, vs, vr, send, recv, sem = refs[3:12], *refs[12:]
    i = pl.program_id(0)
    copies = Copies(send, recv)
    red = Reduction(dims, copies, packed, bufs, NARROW_CUT)
    keep = pltpu.make_async_copy(packed.at[red.place[3]], mine, sem)
    stages = [[red.other], *([d for _, d in red.along[axis]] for axis in "xyz")]
    bases = [sum(len(s) for s in stages[:k]) for k in range(4)]
    for k, devices in enumerate(stages):
        copies.plan("v%d" % k, [
            lambda k=k, o=o, d=d: (sums if k == 0 else vs.at[k - 1], vr.at[bases[k] + o], d)
            for o, d in enumerate(devices)
        ])

    def vec_add(k):
        total = sums[...] if k == 0 else vs[k - 1]
        for o in range(len(stages[k])):
            total = total + vr[bases[k] + o]
        if k < 3:
            vs[k] = total
        else:
            total_ref[...] = total

    @pl.when(i == 0)
    def _():
        greet(red.along, red.other)
        keep.start()

    @pl.when(i == 2)
    def _():
        met(red.along)
        copies.start("pair", "v0")

    @pl.when(i == 5)
    def _():
        keep.wait()
        copies.arrived("pair", "v0")
        red.add_pair(mine)
        vec_add(0)
        copies.start("1l", "1h", "v1")

    @pl.when(i == n - 6)
    def _():
        copies.arrived("1l", "v1")
        red.add_first_low()
        vec_add(1)
        copies.start("2l", "v2")
        copies.arrived("1h")
        red.add_first_high()
        copies.start("2h")

    @pl.when(i == n - 2)
    def _():
        copies.arrived("2l", "2h", "v2")
        red.add_second()
        vec_add(2)
        copies.start("3", "v3")

    inv = inv_ref[0]
    inv = jnp.concatenate([inv, inv, inv], axis=1)
    gh1 = dot_nt(g_ref[0], w_ref[...])
    store_image(
        gtok_ref, i, gres_ref[0] + norm_backward(gh1, normed_ref[0], inv, vec_ref[0:1, :])
    )

    @pl.when(i == n - 1)
    def _():
        copies.arrived("3", "v3")
        sum_ref[...] = red.add_third()
        vec_add(3)
        copies.left(*copies.groups)


def tokens_grad(g, normed, inv, gres, wqkv, vec, sums, packed, rows, dp):
    dims = chip_grid(dp)
    nz, ny, nx = dims
    n = g.shape[0]
    part = D // dp
    count = Reduction.count(dims) + nz + ny + nx - 2
    return pl.pallas_call(
        functools.partial(tokens_kernel, dims, n),
        grid=(n,),
        in_specs=[
            per_image(SP, 3 * D), per_image(SP, D), per_image(SP, 128), per_image(SP, D),
            whole((D, 3 * D)), whole((8, D)), whole((16, D)), pl.BlockSpec(memory_space=pl.ANY),
        ],
        out_specs=[whole((rows, D)), whole((part, NARROW)), whole((16, D))],
        out_shape=[
            jax.ShapeDtypeStruct((rows, D), F32),
            jax.ShapeDtypeStruct((part, NARROW), F32),
            jax.ShapeDtypeStruct((16, D), F32),
        ],
        scratch_shapes=[
            *Reduction.scratch(dims, part, NARROW, NARROW_CUT),
            pltpu.VMEM((*dims, part, NARROW), BF),
            pltpu.VMEM((3, 16, D), F32),
            pltpu.VMEM((nz + ny + nx - 2, 16, D), F32),
            pltpu.SemaphoreType.DMA((count,)),
            pltpu.SemaphoreType.DMA((count,)),
            pltpu.SemaphoreType.DMA,
        ],
        compiler_params=params(collective_id=2),
        name="tokens_grad",
    )(g, normed, inv, gres, wqkv, vec, sums, packed)


def split_kernel(n, narrow_ref, wide_ref, vec_ref, *outs):
    for j in range(3):
        outs[j][...] = narrow_ref[:, THIRD * j : THIRD * (j + 1)]
    outs[3][...] = wide_ref[:, :THIRD]
    outs[4][...] = wide_ref[:, OUT_PAD : OUT_PAD + HALF]
    outs[5][...] = wide_ref[:, OUT_PAD + HALF :]
    index = lax.axis_index("dp") * 2 + lax.axis_index("mp")
    per = D // n
    vec = pltpu.roll(vec_ref[...], D - index * per, axis=1)
    for row, out in zip((2, 3, 0, 1, 4, 5, 6, 7), outs[6:]):
        out[...] = vec[row : row + 1, :per]
    wide = jnp.concatenate([vec_ref[8 + j : 9 + j, :] for j in range(FF // D)], axis=1)
    wide = pltpu.roll(jnp.broadcast_to(wide, (8, FF)), FF - index * (FF // n), axis=1)
    outs[14][...] = wide[0:1, : FF // n]


def split(narrow, wide, vec, n):
    rows = narrow.shape[0]
    vmem = pl.BlockSpec(memory_space=pltpu.VMEM)
    shapes = [(rows, THIRD)] * 4 + [(rows, HALF)] * 2 + [(1, D // n)] * 8 + [(1, FF // n)]
    return pl.pallas_call(
        functools.partial(split_kernel, n),
        in_specs=[vmem] * 3,
        out_specs=[vmem] * 15,
        out_shape=[jax.ShapeDtypeStruct(s, F32) for s in shapes],
        name="split",
    )(narrow, wide, vec)


def whole(shape):
    return pl.BlockSpec(shape, lambda i: (0,) * len(shape))


def per_image(*shape):
    return pl.BlockSpec((1, *shape), lambda i: (i,) + (0,) * len(shape))


def params(collective_id=None):
    return pltpu.CompilerParams(
        dimension_semantics=("arbitrary",), vmem_limit_bytes=62 * 1024 * 1024,
        collective_id=collective_id, has_side_effects=collective_id is not None,
    )


def on_device(
    tokens, w_query, w_key, w_value, w_out, w_up, w_down, ln1_gain, ln1_bias, b_query, b_value,
    b_out, ln2_gain, ln2_bias, b_up, b_down, cotangent,
):
    dp = lax.axis_size("dp")
    vectors = (ln1_gain, ln1_bias, b_query, b_value, b_out, ln2_gain, ln2_bias, b_down)
    qkv, e, mixed, linv, normed, inv, wqkv, vec, bup, wide = attn_fwd(
        (w_query, w_key, w_value, w_out.T, w_up, w_down.T), [v[None] for v in vectors], b_up[None],
        tokens, dp,
    )
    out, gres, gmix, packed, dvec2, dbup = mlp(
        tokens, cotangent, mixed, wide.reshape(2, D, WIDE), vec, bup, dp
    )
    g, packed, sums, wide_sum = attn_bwd(
        qkv, e, mixed, linv, gmix, normed, wqkv, vec, dvec2, dbup, packed, dp
    )
    gtok, narrow_sum, sums = tokens_grad(
        g, normed, inv, gres, wqkv, vec, sums, packed, tokens.shape[0], dp
    )
    grads = split(narrow_sum, wide_sum, sums, dp * lax.axis_size("mp"))
    vecs = [v.reshape(-1) for v in grads[6:]]
    return (
        out, gtok, grads[0], grads[1], grads[2], grads[3].T, grads[4], grads[5].T,
        *vecs[:7], vecs[8], vecs[7],
    )


def solution(mesh):
    row, mat, tam, vec = P(("dp", "mp"), None), P("dp", "mp"), P("mp", "dp"), P("dp")
    part = P(("dp", "mp"))
    return jax.shard_map(
        on_device,
        mesh=mesh,
        in_specs=(row, mat, mat, mat, tam, mat, tam, *([vec] * 9), row),
        out_specs=(row, row, mat, mat, mat, tam, mat, tam, *([part] * 9)),
        check_vma=False,
    )
```

```python
import functools
import math

import jax
import jax.numpy as jnp
from jax import lax
from jax.experimental import pallas as pl
from jax.experimental.pallas import tpu as pltpu
from jax.sharding import PartitionSpec as P

D = 384
HD = 64
FF = 1536
S = 197
HEADS = D // HD
PAIRS = HEADS // 2

SP = 208
WIN = 224

EPS = 1e-06
RSQRT2 = 0.7071067811865476
RSQRT_TAU = 0.3989422804014327
LOG2E = 1.4426950408889634
Q_SCALE = LOG2E / math.sqrt(HD)
BF = jnp.bfloat16
F32 = jnp.float32


def dot_nn(a, b):
    return lax.dot_general(a, b, (((1,), (0,)), ((), ())), preferred_element_type=F32)


def dot_nt(a, b):
    return lax.dot_general(a, b, (((1,), (1,)), ((), ())), preferred_element_type=F32)


def dot_tn(a, b):
    return lax.dot_general(a, b, (((0,), (0,)), ((), ())), preferred_element_type=F32)


def window_of(i, rows):
    start = i * S
    base = jnp.minimum((start // 16) * 16, rows - WIN)
    return pl.multiple_of(base, 16), start - base


def load_image(ref, i):
    base, off = window_of(i, ref.shape[0])
    rows = ref[pl.ds(base, WIN), :].astype(F32)
    rows = pltpu.roll(rows, WIN - off, axis=0)[:SP]
    live = lax.broadcasted_iota(jnp.int32, rows.shape, 0) < S
    return jnp.where(live, rows, 0.0)


def store_image(ref, i, rows):
    start = i * S
    r = start % 8
    base = start - r
    total = ref.shape[0]
    groups = SP // 8
    turned = pltpu.roll(rows.reshape(groups, 8, D), r, axis=1)
    first = lax.broadcasted_iota(jnp.int32, (8, D), 0) < r
    old = ref[pl.ds(pl.multiple_of(base, 8), 8), :]
    ref[pl.ds(pl.multiple_of(base, 8), 8), :] = jnp.where(first, old, turned[0])
    for g in range(1, groups - 1):
        ref[pl.ds(pl.multiple_of(base + 8 * g, 8), 8), :] = jnp.where(
            first, turned[g - 1], turned[g]
        )
    over = base + SP > total
    here = jnp.where(over, total - 8, base + SP - 8)
    tail = [jnp.where(first, turned[g - 1], turned[g]) for g in (groups - 2, groups - 1)]
    ref[pl.ds(pl.multiple_of(here, 8), 8), :] = jnp.where(over, tail[0], tail[1])


def norm_stats(x):
    mean = jnp.mean(x, axis=-1, keepdims=True)
    centred = x - mean
    inv = lax.rsqrt(jnp.mean(centred * centred, axis=-1, keepdims=True) + EPS)
    return centred * inv, inv


def norm_backward(grad, normed, inv, gain):
    e = grad * gain
    return inv * (
        e
        - jnp.mean(e, axis=-1, keepdims=True)
        - normed * jnp.mean(e * normed, axis=-1, keepdims=True)
    )


def row_sum(x):
    return jnp.sum(x, axis=0, keepdims=True)


THIRD = D // 2
HALF = FF // 2
NARROW = 640
NARROW_CUT = 384
OUT_PAD = 256
WIDE = OUT_PAD + 2 * HALF
WIDE_CUT = 896
MESH = pl.DeviceIdType.MESH
EVERY = slice(None)


def chip_grid(dp):
    side = math.isqrt(dp // 4)
    return 4, side, side


def place_of(dims):
    _, ny, nx = dims
    dp, mp = lax.axis_index("dp"), lax.axis_index("mp")
    return dp // (ny * nx), (dp // nx) % ny, dp % nx, mp


def peers_of(dims, place):
    (nz, ny, nx), (z, y, x, mp) = dims, place

    def at(a, b, c, m):
        return ((a * ny + b) * nx + c, m)

    along = {
        "z": [((z + o) % nz, at((z + o) % nz, y, x, mp)) for o in range(1, nz)],
        "y": [((y + o) % ny, at(z, (y + o) % ny, x, mp)) for o in range(1, ny)],
        "x": [((x + o) % nx, at(z, y, (x + o) % nx, mp)) for o in range(1, nx)],
    }
    return along, at(z, y, x, 1 - mp)


def greet(along, other):
    for device in [d for peers in along.values() for _, d in peers] + [other]:
        pl.semaphore_signal(
            pltpu.get_barrier_semaphore(), inc=1, device_id=device, device_id_type=MESH
        )


def met(along):
    count = sum(len(peers) for peers in along.values()) + 1
    pl.semaphore_wait(pltpu.get_barrier_semaphore(), count)


class Copies:
    def __init__(self, send, recv):
        self.send, self.recv, self.groups, self.count = send, recv, {}, 0

    def plan(self, name, makers):
        self.groups[name] = [(self.count + i, m) for i, m in enumerate(makers)]
        self.count += len(makers)

    def each(self, names):
        for name in names:
            for index, make in self.groups[name]:
                src, dst, device = make()
                yield pltpu.make_async_remote_copy(
                    src_ref=src, dst_ref=dst, send_sem=self.send.at[index],
                    recv_sem=self.recv.at[index], device_id=device, device_id_type=MESH,
                )

    def start(self, *names):
        for copy in self.each(names):
            copy.start()

    def arrived(self, *names):
        for copy in self.each(names):
            copy.wait_recv()

    def left(self, *names):
        for copy in self.each(names):
            copy.wait_send()


def plan_gather(copies, tag, w, own, cut, along, other, place):
    z, y, x, mp = place
    low, high = pl.ds(0, cut), pl.ds(cut, w.shape[-1] - cut)

    def same(index, device):
        return lambda: (w.at[index], w.at[index], device)

    def spread(index, axis):
        return [same(index, d) for _, d in along[axis]]

    def shares(indices):
        return [same(index, other) for index in indices]

    copies.plan(tag + "1", [lambda d=d: (own, w.at[mp, z, y, x], d) for _, d in along["z"]])
    copies.plan(tag + "2l", spread((mp, EVERY, y, x, EVERY, low), "y"))
    copies.plan(tag + "2h", spread((mp, EVERY, y, x, EVERY, high), "x"))
    copies.plan(tag + "3l", spread((mp, EVERY, EVERY, x, EVERY, low), "x"))
    copies.plan(tag + "3h", spread((mp, EVERY, y, EVERY, EVERY, high), "y"))
    copies.plan(tag + "s1", shares([(mp, EVERY, y, x)]))
    copies.plan(tag + "s2l", shares([(mp, EVERY, b, x, EVERY, low) for b, _ in along["y"]]))
    copies.plan(tag + "s2h", shares([(mp, EVERY, y, c, EVERY, high) for c, _ in along["x"]]))
    copies.plan(tag + "s3l", shares([(mp, EVERY, EVERY, c, EVERY, low) for c, _ in along["x"]]))
    copies.plan(tag + "s3h", shares([(mp, EVERY, b, EVERY, EVERY, high) for b, _ in along["y"]]))


def attn_fwd_kernel(dims, n, *refs):
    (wq, wk, wv, wot, wu, wdt), vectors, bup_in = refs[:6], refs[6:14], refs[14]
    tok_ref, cot_ref = refs[15:17]
    (
        qkv_ref, e_ref, mixed_ref, linv_ref, normed_ref, inv_ref, tokp_ref, cotp_ref, w_ref, vec_ref,
        bup_ref, wide,
    ) = refs[17:29]
    narrow, v, own, normed_all, inv_all, tok_all, cot_all, send, recv, sem = refs[29:]
    i = pl.program_id(0)
    nz, ny, nx = dims
    place = place_of(dims)
    z, y, x, mp = place
    rows = own.shape[0]
    along, other = peers_of(dims, place)
    copies = Copies(send, recv)
    plan_gather(copies, "n", narrow, narrow.at[mp, z, y, x], NARROW_CUT, along, other, place)
    plan_gather(copies, "w", wide, own, WIDE_CUT, along, other, place)

    def vec_spread(index, axis):
        return [lambda d=d: (v.at[index], v.at[index], d) for _, d in along[axis]]

    copies.plan("v1", vec_spread((z, y, x), "z"))
    copies.plan("v2", vec_spread((EVERY, y, x), "y"))
    copies.plan("v3", vec_spread((EVERY, EVERY, x), "x"))
    keep = pltpu.make_async_copy(own, wide.at[mp, z, y, x], sem)

    def norms(first, last):
        @pl.loop(first, last)
        def _(j):
            tok = load_image(tok_ref, j)
            normed, inv = norm_stats(tok)
            tok_all[j] = tok.astype(BF)
            cot_all[j] = load_image(cot_ref, j).astype(BF)
            normed_all[j] = normed
            inv_all[j] = jnp.broadcast_to(inv, (SP, 128))

    @pl.when(i == 0)
    def _():
        narrow[mp, z, y, x] = jnp.concatenate(
            [wq[...], wk[...], wv[...], jnp.zeros((rows, NARROW - 3 * THIRD), BF)], axis=1
        )
        own[...] = jnp.concatenate(
            [wot[...], jnp.zeros((rows, OUT_PAD - THIRD), BF), wu[...], wdt[...]], axis=1
        )
        v[z, y, x] = jnp.zeros((16, 128), F32)
        for j, vector in enumerate(vectors):
            v[z, y, x, j : j + 1, :rows] = vector[...].astype(F32)
        v[z, y, x, 8:9, : bup_in.shape[1]] = bup_in[...].astype(F32)
        greet(along, other)
        keep.start()
        norms(0, n // 4)
        met(along)
        copies.start("v1", "n1")
        norms(n // 4, n // 2)
        copies.arrived("v1", "n1")
        copies.start("v2", "n2l", "n2h", "w1", "ns1")
        norms(n // 2, (3 * n) // 4)
        copies.arrived("v2", "n2l", "n2h")
        copies.start("v3", "n3l", "n3h", "ns2l", "ns2h")
        norms((3 * n) // 4, n)
        copies.arrived("v3", "n3l")
        copies.start("ns3l")
        copies.arrived("n3h")
        copies.start("ns3h")
        keep.wait()
        copies.arrived("w1")
        copies.start("w2l", "w2h", "ws1")
        spots = [(a, b, c) for a in range(nz) for b in range(ny) for c in range(nx)]
        vec_ref[...] = jnp.concatenate([v[s][0:8, :rows] for s in spots], axis=1)
        bup_ref[...] = jnp.concatenate([v[s][8:9, : bup_in.shape[1]] for s in spots], axis=1)
        copies.arrived("ns1", "ns2l", "ns2h", "ns3l", "ns3h")
        group = 48 // rows
        for t in range(len(spots) // group):
            block = [
                jnp.concatenate(
                    [narrow[(m,) + s].astype(F32) for s in spots[t * group : (t + 1) * group]], axis=0
                )
                for m in range(2)
            ]
            for j in range(3):
                cols = slice(THIRD * j, THIRD * (j + 1))
                w_ref[48 * t : 48 * (t + 1), D * j : D * (j + 1)] = jnp.concatenate(
                    [half[:, cols] for half in block], axis=1
                ).astype(BF)

    @pl.when(i == 3)
    def _():
        copies.arrived("w2l", "w2h")
        copies.start("w3l", "w3h", "ws2l", "ws2h")

    normed = normed_all[i]
    normed_ref[0] = normed
    inv_ref[0] = inv_all[i]
    tokp_ref[0] = tok_all[i]
    cotp_ref[0] = cot_all[i]
    h1 = (normed * vec_ref[0:1, :] + vec_ref[1:2, :]).astype(BF)
    q = ((dot_nn(h1, w_ref[:, 0:D]) + vec_ref[2:3, :]) * Q_SCALE).astype(BF)
    k = dot_nn(h1, w_ref[:, D : 2 * D]).astype(BF)
    value = (dot_nn(h1, w_ref[:, 2 * D :]) + vec_ref[3:4, :]).astype(BF)
    qkv_ref[0, :, 0:D] = q
    qkv_ref[0, :, D : 2 * D] = k
    qkv_ref[0, :, 2 * D :] = value
    lane = lax.broadcasted_iota(jnp.int32, (SP, 2 * HD), 1)
    is_key = lax.broadcasted_iota(jnp.int32, (SP, SP), 1) < S
    zero = jnp.zeros((SP, 2 * HD), BF)
    one = jnp.ones((SP, 2 * HD), BF)
    for p in range(PAIRS):
        cols = slice(2 * HD * p, 2 * HD * (p + 1))
        total = None
        for h in range(2):
            mine = (lane < HD) if h == 0 else (lane >= HD)
            kh = jnp.where(mine, k[:, cols], zero)
            vh = jnp.where(mine, value[:, cols], zero)
            scores = dot_nt(q[:, cols], kh)
            scores = jnp.where(is_key, scores, -1e30)
            top = jnp.max(scores, axis=-1, keepdims=True)
            e = jnp.exp2(scores - top).astype(BF)
            e_ref[0, 2 * p + h] = e
            part = dot_nn(e, jnp.concatenate([vh, jnp.where(mine, one, zero)], axis=1))
            total = part if total is None else total + part
        linv = 1.0 / total[:, 2 * HD :]
        linv_ref[0, :, cols] = linv
        mixed_ref[0, :, cols] = (total[:, : 2 * HD] * linv).astype(BF)

    @pl.when(i == n - 5)
    def _():
        copies.arrived("w3l", "w3h")
        copies.start("ws3l", "ws3h")

    @pl.when(i == n - 1)
    def _():
        copies.arrived("ws1", "ws2l", "ws2h", "ws3l", "ws3h")
        copies.left(*copies.groups)


def attn_fwd(mats, vectors, bup, tokens, cot, dp):
    dims = chip_grid(dp)
    nz, ny, nx = dims
    rows = D // dp
    n = tokens.shape[0] // S
    count = 2 * (nz - 1 + 4 * (ny - 1) + 4 * (nx - 1) + 1) + nz + ny + nx - 3
    inputs = (*mats, *vectors, bup, tokens, cot)
    return pl.pallas_call(
        functools.partial(attn_fwd_kernel, dims, n),
        grid=(n,),
        in_specs=[whole(a.shape) for a in inputs],
        out_specs=[
            per_image(SP, 3 * D), per_image(HEADS, SP, SP), per_image(SP, D), per_image(SP, D),
            per_image(SP, D), per_image(SP, 128), per_image(SP, D), per_image(SP, D),
            whole((D, 3 * D)), whole((8, D)), whole((1, FF)), pl.BlockSpec(memory_space=pl.ANY),
        ],
        out_shape=[
            jax.ShapeDtypeStruct((n, SP, 3 * D), BF),
            jax.ShapeDtypeStruct((n, HEADS, SP, SP), BF),
            jax.ShapeDtypeStruct((n, SP, D), BF),
            jax.ShapeDtypeStruct((n, SP, D), F32),
            jax.ShapeDtypeStruct((n, SP, D), F32),
            jax.ShapeDtypeStruct((n, SP, 128), F32),
            jax.ShapeDtypeStruct((n, SP, D), BF),
            jax.ShapeDtypeStruct((n, SP, D), BF),
            jax.ShapeDtypeStruct((D, 3 * D), BF),
            jax.ShapeDtypeStruct((8, D), F32),
            jax.ShapeDtypeStruct((1, FF), F32),
            jax.ShapeDtypeStruct((2, nz, ny, nx, rows, WIDE), BF),
        ],
        scratch_shapes=[
            pltpu.VMEM((2, nz, ny, nx, rows, NARROW), BF),
            pltpu.VMEM((nz, ny, nx, 16, 128), F32),
            pltpu.VMEM((rows, WIDE), BF),
            pltpu.VMEM((n, SP, D), F32),
            pltpu.VMEM((n, SP, 128), F32),
            pltpu.VMEM((n, SP, D), BF),
            pltpu.VMEM((n, SP, D), BF),
            pltpu.SemaphoreType.DMA((count,)),
            pltpu.SemaphoreType.DMA((count,)),
            pltpu.SemaphoreType.DMA,
        ],
        compiler_params=params(collective_id=0),
        name="attn_fwd",
    )(*inputs)


def fold(x):
    return jnp.sum(x.reshape(x.shape[0] // 8, 8, x.shape[1]), axis=0)


CHUNK = 16


def mlp_kernel(
    dims, n, tok_ref, cot_ref, mixed_ref, w_ref, vec_ref, bup_ref,
    out_ref, gres_ref, gmix_ref, grads_ref, dvec_ref, dbup_ref,
    act_ref, gp_ref, wot_ref, dwot_ref, dwup_ref, dwdt_ref,
    h2_ref, h2t_ref, cott_ref, mix_ref, gr_ref, outf_ref, out_old, gh2_ref, cotf_ref, norm_ref,
    inv_ref, sums_ref, upsum_ref,
):
    i = pl.program_id(0)
    step = 256
    tiles = FF // step
    chunks = [slice(c, c + CHUNK) for c in range(0, SP, CHUNK)]

    @pl.when(i == 0)
    def _():
        wot_ref[...] = jnp.concatenate([w_ref[0, :, :THIRD], w_ref[1, :, :THIRD]], axis=1)
        for ref in (
            dwot_ref, dwup_ref, dwdt_ref, act_ref, gp_ref, h2t_ref, cott_ref, mix_ref, out_old,
            gh2_ref, cotf_ref, norm_ref, inv_ref, sums_ref, upsum_ref,
        ):
            ref[...] = jnp.zeros_like(ref)

    def weight_tile(j):
        cols = slice(step * j, step * (j + 1))
        dwup_ref[:, cols] += dot_nn(h2t_ref[...], gp_ref[:, cols])
        dwdt_ref[:, cols] += dot_nn(cott_ref[...], act_ref[:, cols])

    def finish(image, beside):
        beside(0)
        slot = image % 2
        for at in chunks:
            gh2, normed, cot = gh2_ref[at, :], norm_ref[at, :], cotf_ref[at, :]
            gres = cot + norm_backward(gh2, normed, inv_ref[at, 0:1], vec_ref[5:6, :])
            gres_ref[slot, at, :] = gres
            gr_ref[at, :] = gres.astype(BF)
            sums_ref[0] += fold(gres)
            sums_ref[1] += fold(gh2 * normed)
            sums_ref[2] += fold(gh2)
            sums_ref[3] += fold(cot)
        beside(1)
        gmix_ref[slot] = dot_nn(gr_ref[...], wot_ref[...]).astype(BF)
        beside(2)
        store_image(outf_ref, image, out_old[...])
        dwot_ref[...] += dot_tn(gr_ref[...], mix_ref[...])
        beside(3)

    finish(jnp.maximum(i - 1, 0), weight_tile)
    weight_tile(4)
    attended = dot_nt(mixed_ref[0], wot_ref[...])
    for at in chunks:
        cot = cot_ref[0, at, :].astype(F32)
        resid = tok_ref[0, at, :].astype(F32) + attended[at] + vec_ref[4:5, :]
        normed, inv = norm_stats(resid)
        h2_ref[at, :] = (normed * vec_ref[5:6, :] + vec_ref[6:7, :]).astype(BF)
        cotf_ref[at, :] = cot
        norm_ref[at, :] = normed
        inv_ref[at, :] = jnp.broadcast_to(inv, (CHUNK, 128))
        out_old[at, :] = resid + vec_ref[7:8, :]
    weight_tile(5)
    mix_ref[...] = mixed_ref[0]
    h2 = h2_ref[...]
    cot = cot_ref[0]
    h2t_ref[...] = h2.T
    cott_ref[...] = cot.T
    for j in range(tiles):
        cols = slice(step * j, step * (j + 1))
        m, at = divmod(step * j, HALF)
        u = dot_nn(h2, w_ref[m, :, OUT_PAD + at : OUT_PAD + at + step]) + bup_ref[:, cols]
        ga = dot_nn(cot, w_ref[m, :, OUT_PAD + HALF + at : OUT_PAD + HALF + at + step])
        cdf = 0.5 * (1.0 + lax.erf(u * RSQRT2))
        act_ref[:, cols] = (u * cdf).astype(BF)
        gp = ga * (cdf + u * jnp.exp(-0.5 * u * u) * RSQRT_TAU)
        upsum_ref[:, cols] += fold(gp)
        gp_ref[:, cols] = gp.astype(BF)
    out = out_old[...]
    gh2 = None
    for m in range(2):
        cols = slice(HALF * m, HALF * (m + 1))
        out = out + dot_nt(act_ref[:, cols], w_ref[m, :, OUT_PAD + HALF :])
        part = dot_nt(gp_ref[:, cols], w_ref[m, :, OUT_PAD : OUT_PAD + HALF])
        gh2 = part if gh2 is None else gh2 + part
    out_old[...] = out
    gh2_ref[...] = gh2

    @pl.when(i == n - 1)
    def _():
        finish(i, weight_tile)
        weight_tile(4)
        weight_tile(5)
        out_ref[...] = outf_ref[...].astype(BF)
        for k in range(4):
            dvec_ref[k : k + 1, :] = row_sum(sums_ref[k])
        dvec_ref[4:8, :] = jnp.zeros((4, D), F32)
        dbup_ref[...] = row_sum(upsum_ref[...])
        nz, ny, nx = dims
        rows = grads_ref.shape[4]
        spots = [(a, b, c) for a in range(nz) for b in range(ny) for c in range(nx)]
        group = 48 // rows
        for t in range(len(spots) // group):
            at = slice(48 * t, 48 * (t + 1))
            for m in range(2):
                parts = [
                    dwot_ref[at, THIRD * m : THIRD * (m + 1)],
                    jnp.zeros((48, OUT_PAD - THIRD), F32),
                    dwup_ref[at, HALF * m : HALF * (m + 1)],
                    dwdt_ref[at, HALF * m : HALF * (m + 1)],
                ]
                block = jnp.concatenate(parts, axis=1)
                for g in range(group):
                    grads_ref[(m,) + spots[t * group + g]] = block[
                        g * rows : (g + 1) * rows
                    ].astype(BF)


def mlp(tok, cot, mixed, wide, vec, bup, rows, dp):
    dims = chip_grid(dp)
    n = rows // S
    packed = (2, *dims, D // dp, WIDE)
    late = pl.BlockSpec((2, SP, D), lambda i: (jnp.maximum(i - 1, 0) // 2, 0, 0))
    return pl.pallas_call(
        functools.partial(mlp_kernel, dims, n),
        grid=(n,),
        in_specs=[
            per_image(SP, D), per_image(SP, D), per_image(SP, D), whole((2, D, WIDE)), whole((8, D)),
            whole((1, FF)),
        ],
        out_specs=[whole((rows, D)), late, late, whole(packed), whole((8, D)), whole((1, FF))],
        out_shape=[
            jax.ShapeDtypeStruct((rows, D), BF),
            jax.ShapeDtypeStruct((n, SP, D), F32),
            jax.ShapeDtypeStruct((n, SP, D), BF),
            jax.ShapeDtypeStruct(packed, BF),
            jax.ShapeDtypeStruct((8, D), F32),
            jax.ShapeDtypeStruct((1, FF), F32),
        ],
        scratch_shapes=[
            pltpu.VMEM((SP, FF), BF), pltpu.VMEM((SP, FF), BF), pltpu.VMEM((D, D), BF),
            pltpu.VMEM((D, D), F32), pltpu.VMEM((D, FF), F32), pltpu.VMEM((D, FF), F32),
            pltpu.VMEM((SP, D), BF), pltpu.VMEM((D, SP), BF), pltpu.VMEM((D, SP), BF),
            pltpu.VMEM((SP, D), BF), pltpu.VMEM((SP, D), BF), pltpu.VMEM((rows, D), F32),
            pltpu.VMEM((SP, D), F32), pltpu.VMEM((SP, D), F32), pltpu.VMEM((SP, D), F32),
            pltpu.VMEM((SP, D), F32), pltpu.VMEM((SP, 128), F32), pltpu.VMEM((4, 8, D), F32),
            pltpu.VMEM((8, FF), F32),
        ],
        compiler_params=params(),
        name="mlp",
    )(tok, cot, mixed, wide, vec, bup)


class Reduction:
    def __init__(self, dims, copies, packed, bufs, cut):
        self.dims, self.copies, self.packed, self.cut = dims, copies, packed, cut
        self.place = place_of(dims)
        self.along, self.other = peers_of(dims, self.place)
        z, y, x, mp = self.place
        self.p, self.a1, self.b1, self.ra1, self.rb1, self.ra2, self.rb2, self.f, self.rz = bufs
        low, high = pl.ds(0, cut), pl.ds(cut, packed.shape[-1] - cut)
        along = self.along
        copies.plan("pair", [lambda: (packed.at[1 - mp], self.p, self.other)])
        copies.plan("1l", [
            lambda o=o, c=c, d=d: (self.p.at[EVERY, EVERY, c, EVERY, low], self.ra1.at[o], d)
            for o, (c, d) in enumerate(along["x"])
        ])
        copies.plan("1h", [
            lambda o=o, b=b, d=d: (self.p.at[EVERY, b, EVERY, EVERY, high], self.rb1.at[o], d)
            for o, (b, d) in enumerate(along["y"])
        ])
        copies.plan("2l", [
            lambda o=o, b=b, d=d: (self.a1.at[EVERY, b], self.ra2.at[o], d)
            for o, (b, d) in enumerate(along["y"])
        ])
        copies.plan("2h", [
            lambda o=o, c=c, d=d: (self.b1.at[EVERY, c], self.rb2.at[o], d)
            for o, (c, d) in enumerate(along["x"])
        ])
        copies.plan("3", [
            lambda o=o, a=a, d=d: (self.f.at[a], self.rz.at[o], d)
            for o, (a, d) in enumerate(along["z"])
        ])

    @staticmethod
    def count(dims):
        nz, ny, nx = dims
        return 1 + 2 * (ny - 1) + 2 * (nx - 1) + nz - 1

    @staticmethod
    def scratch(dims, rows, width, cut):
        nz, ny, nx = dims

        def buf(w, *shape):
            return pltpu.VMEM((*shape, rows, w), BF)

        rest = width - cut
        return [
            buf(width, nz, ny, nx), buf(cut, nz, ny), buf(rest, nz, nx),
            buf(cut, nx - 1, nz, ny), buf(rest, ny - 1, nz, nx),
            buf(cut, ny - 1, nz), buf(rest, nx - 1, nz), buf(width, nz), buf(width, nz - 1),
        ]

    def add_pair(self, mine):
        nz, ny, nx = self.dims
        for i in range(nz):
            for j in range(ny):
                for k in range(nx):
                    total = mine[i, j, k].astype(F32) + self.p[i, j, k].astype(F32)
                    self.p[i, j, k] = total.astype(BF)

    def add_first_low(self):
        nz, ny, nx = self.dims
        x = self.place[2]
        for i in range(nz):
            for j in range(ny):
                total = self.p[i, j, x, :, : self.cut].astype(F32)
                for o in range(nx - 1):
                    total = total + self.ra1[o, i, j].astype(F32)
                self.a1[i, j] = total.astype(BF)

    def add_first_high(self):
        nz, ny, nx = self.dims
        y = self.place[1]
        for i in range(nz):
            for k in range(nx):
                total = self.p[i, y, k, :, self.cut :].astype(F32)
                for o in range(ny - 1):
                    total = total + self.rb1[o, i, k].astype(F32)
                self.b1[i, k] = total.astype(BF)

    def add_second(self):
        nz, ny, nx = self.dims
        _, y, x, _ = self.place
        for i in range(nz):
            total = self.a1[i, y].astype(F32)
            for o in range(ny - 1):
                total = total + self.ra2[o, i].astype(F32)
            self.f[i, :, : self.cut] = total.astype(BF)
            total = self.b1[i, x].astype(F32)
            for o in range(nx - 1):
                total = total + self.rb2[o, i].astype(F32)
            self.f[i, :, self.cut :] = total.astype(BF)

    def add_third(self):
        total = self.f[self.place[0]].astype(F32)
        for o in range(self.dims[0] - 1):
            total = total + self.rz[o].astype(F32)
        return total


def attn_bwd_kernel(
    dims, n, qkv_ref, e_ref, mixed_ref, linv_ref, gmix_ref, normed_ref, w_ref, vec_ref, dvec2_ref,
    dbup_ref, packed, *refs,
):
    g_ref, narrow_ref, sums_ref, sum_ref = refs[:4]
    acc_ref, gsum_ref, bufs, mine, send, recv, sem = refs[4], refs[5], refs[6:15], *refs[15:]
    i = pl.program_id(0)
    copies = Copies(send, recv)
    red = Reduction(dims, copies, packed, bufs, WIDE_CUT)
    keep = pltpu.make_async_copy(packed.at[red.place[3]], mine, sem)

    @pl.when(i == 0)
    def _():
        acc_ref[...] = jnp.zeros_like(acc_ref)
        gsum_ref[...] = jnp.zeros_like(gsum_ref)
        greet(red.along, red.other)
        keep.start()

    @pl.when(i == 1)
    def _():
        met(red.along)
        copies.start("pair")

    @pl.when(i == 3)
    def _():
        keep.wait()
        copies.arrived("pair")
        red.add_pair(mine)
        copies.start("1l", "1h")

    @pl.when(i == n // 2 - 1)
    def _():
        copies.arrived("1l", "1h")
        red.add_first_low()
        red.add_first_high()
        copies.start("2l", "2h")

    @pl.when(i == n // 2 + 2)
    def _():
        copies.arrived("2l", "2h")
        red.add_second()
        copies.start("3")

    lane = lax.broadcasted_iota(jnp.int32, (SP, 2 * HD), 1)
    zero = jnp.zeros((SP, 2 * HD), BF)
    minus = jnp.full((SP, 2 * HD), -1.0, BF)
    for p in range(PAIRS):
        lo, hi = 2 * HD * p, 2 * HD * (p + 1)
        q = qkv_ref[0, :, lo:hi]
        k = qkv_ref[0, :, D + lo : D + hi]
        v = qkv_ref[0, :, 2 * D + lo : 2 * D + hi]
        go_f = gmix_ref[0, :, lo:hi].astype(F32) * linv_ref[0, :, lo:hi]
        go = go_f.astype(BF)
        god = jnp.concatenate(
            [go, (go_f * mixed_ref[0, :, lo:hi].astype(F32)).astype(BF)], axis=1
        )
        gq = gk = gv = None
        for h in range(2):
            own = (lane < HD) if h == 0 else (lane >= HD)
            e = e_ref[0, 2 * p + h]
            vd = jnp.concatenate(
                [jnp.where(own, v, zero), jnp.where(own, minus, zero)], axis=1
            )
            ds = e * dot_nt(god, vd).astype(BF)
            part_q = dot_nn(ds, jnp.where(own, k, zero))
            part_k = dot_tn(ds, jnp.where(own, q, zero))
            part_v = dot_tn(e, jnp.where(own, go, zero))
            gq = part_q if gq is None else gq + part_q
            gk = part_k if gk is None else gk + part_k
            gv = part_v if gv is None else gv + part_v
        gq = gq * (1.0 / math.sqrt(HD))
        gk = gk * (1.0 / LOG2E)
        for j, grad in enumerate((gq, gk, gv)):
            gsum_ref[0:1, D * j + lo : D * j + hi] += row_sum(grad)
            g_ref[0, :, D * j + lo : D * j + hi] = grad.astype(BF)
    acc_ref[...] += dot_tn(normed_ref[0].astype(BF), g_ref[0])

    @pl.when(i == n - 1)
    def _():
        copies.arrived("3")
        sum_ref[...] = red.add_third()
        nz, ny, nx = dims
        rows = narrow_ref.shape[4]
        spots = [(a, b, c) for a in range(nz) for b in range(ny) for c in range(nx)]
        group = 48 // rows
        turned = vec_ref[...].T
        gsum = gsum_ref[0:1, :]
        gains = []
        for t in range(len(spots) // group):
            at = slice(48 * t, 48 * (t + 1))
            acc = acc_ref[at, :]
            gains.append(jnp.sum(acc * w_ref[at, :].astype(F32), axis=1, keepdims=True))
            dw = acc * turned[at, 0:1] + turned[at, 1:2] * gsum
            for m in range(2):
                parts = [dw[:, D * j + THIRD * m : D * j + THIRD * (m + 1)] for j in range(3)]
                parts.append(jnp.zeros((48, NARROW - 3 * THIRD), F32))
                block = jnp.concatenate(parts, axis=1)
                for k in range(group):
                    narrow_ref[(m,) + spots[t * group + k]] = block[
                        k * rows : (k + 1) * rows
                    ].astype(BF)
        high = gsum.astype(BF)
        low = (gsum - high.astype(F32)).astype(BF)
        row = lax.broadcasted_iota(jnp.int32, (16, 3 * D), 0)
        both = jnp.where(row == 0, high, jnp.where(row == 1, low, jnp.zeros((16, 3 * D), BF)))
        sums_ref[0:1] = gsum[:, :D]
        sums_ref[1:2] = gsum[:, 2 * D :]
        gain = jnp.broadcast_to(jnp.concatenate(gains, axis=0), (D, 128)).T
        sums_ref[2:3] = gain[0:1, :]
        sums_ref[3:4] = row_sum(dot_nt(both, w_ref[...]))
        sums_ref[4:8] = dvec2_ref[0:4]
        for j in range(FF // D):
            sums_ref[8 + j : 9 + j] = dbup_ref[:, D * j : D * (j + 1)]
        sums_ref[12:16] = jnp.zeros((4, D), F32)
        copies.left(*copies.groups)


def attn_bwd(qkv, e, mixed, linv, gmix, normed, wqkv, vec, dvec2, dbup, packed, dp):
    dims = chip_grid(dp)
    n = qkv.shape[0]
    rows = D // dp
    count = Reduction.count(dims)
    narrow = (2, *dims, rows, NARROW)
    return pl.pallas_call(
        functools.partial(attn_bwd_kernel, dims, n),
        grid=(n,),
        in_specs=[
            per_image(SP, 3 * D), per_image(HEADS, SP, SP), per_image(SP, D), per_image(SP, D),
            per_image(SP, D), per_image(SP, D), whole((D, 3 * D)), whole((8, D)), whole((8, D)),
            whole((1, FF)), pl.BlockSpec(memory_space=pl.ANY),
        ],
        out_specs=[
            per_image(SP, 3 * D), whole(narrow), whole((16, D)), whole((rows, WIDE)),
        ],
        out_shape=[
            jax.ShapeDtypeStruct((n, SP, 3 * D), BF),
            jax.ShapeDtypeStruct(narrow, BF),
            jax.ShapeDtypeStruct((16, D), F32),
            jax.ShapeDtypeStruct((rows, WIDE), F32),
        ],
        scratch_shapes=[
            pltpu.VMEM((D, 3 * D), F32),
            pltpu.VMEM((8, 3 * D), F32),
            *Reduction.scratch(dims, rows, WIDE, WIDE_CUT),
            pltpu.VMEM((*dims, rows, WIDE), BF),
            pltpu.SemaphoreType.DMA((count,)),
            pltpu.SemaphoreType.DMA((count,)),
            pltpu.SemaphoreType.DMA,
        ],
        compiler_params=params(collective_id=1),
        name="attn_bwd",
    )(qkv, e, mixed, linv, gmix, normed, wqkv, vec, dvec2, dbup, packed)


def tokens_kernel(
    dims, n, g_ref, normed_ref, inv_ref, gres_ref, w_ref, vec_ref, sums, packed, *refs
):
    gtok_ref, sum_ref, total_ref = refs[:3]
    bufs, mine, vs, vr, send, recv, sem = refs[3:12], *refs[12:]
    i = pl.program_id(0)
    copies = Copies(send, recv)
    red = Reduction(dims, copies, packed, bufs, NARROW_CUT)
    keep = pltpu.make_async_copy(packed.at[red.place[3]], mine, sem)
    stages = [[red.other], *([d for _, d in red.along[axis]] for axis in "xyz")]
    bases = [sum(len(s) for s in stages[:k]) for k in range(4)]
    for k, devices in enumerate(stages):
        copies.plan("v%d" % k, [
            lambda k=k, o=o, d=d: (sums if k == 0 else vs.at[k - 1], vr.at[bases[k] + o], d)
            for o, d in enumerate(devices)
        ])

    def vec_add(k):
        total = sums[...] if k == 0 else vs[k - 1]
        for o in range(len(stages[k])):
            total = total + vr[bases[k] + o]
        if k < 3:
            vs[k] = total
        else:
            total_ref[...] = total

    @pl.when(i == 0)
    def _():
        greet(red.along, red.other)
        keep.start()

    @pl.when(i == 2)
    def _():
        met(red.along)
        copies.start("pair", "v0")

    @pl.when(i == 5)
    def _():
        keep.wait()
        copies.arrived("pair", "v0")
        red.add_pair(mine)
        vec_add(0)
        copies.start("1l", "1h", "v1")

    @pl.when(i == n - 6)
    def _():
        copies.arrived("1l", "v1")
        red.add_first_low()
        vec_add(1)
        copies.start("2l", "v2")
        copies.arrived("1h")
        red.add_first_high()
        copies.start("2h")

    @pl.when(i == n - 2)
    def _():
        copies.arrived("2l", "2h", "v2")
        red.add_second()
        vec_add(2)
        copies.start("3", "v3")

    inv = inv_ref[0]
    inv = jnp.concatenate([inv, inv, inv], axis=1)
    gh1 = dot_nt(g_ref[0], w_ref[...])
    store_image(
        gtok_ref, i, gres_ref[0] + norm_backward(gh1, normed_ref[0], inv, vec_ref[0:1, :])
    )

    @pl.when(i == n - 1)
    def _():
        copies.arrived("3", "v3")
        sum_ref[...] = red.add_third()
        vec_add(3)
        copies.left(*copies.groups)


def tokens_grad(g, normed, inv, gres, wqkv, vec, sums, packed, rows, dp):
    dims = chip_grid(dp)
    nz, ny, nx = dims
    n = g.shape[0]
    part = D // dp
    count = Reduction.count(dims) + nz + ny + nx - 2
    return pl.pallas_call(
        functools.partial(tokens_kernel, dims, n),
        grid=(n,),
        in_specs=[
            per_image(SP, 3 * D), per_image(SP, D), per_image(SP, 128), per_image(SP, D),
            whole((D, 3 * D)), whole((8, D)), whole((16, D)), pl.BlockSpec(memory_space=pl.ANY),
        ],
        out_specs=[whole((rows, D)), whole((part, NARROW)), whole((16, D))],
        out_shape=[
            jax.ShapeDtypeStruct((rows, D), F32),
            jax.ShapeDtypeStruct((part, NARROW), F32),
            jax.ShapeDtypeStruct((16, D), F32),
        ],
        scratch_shapes=[
            *Reduction.scratch(dims, part, NARROW, NARROW_CUT),
            pltpu.VMEM((*dims, part, NARROW), BF),
            pltpu.VMEM((3, 16, D), F32),
            pltpu.VMEM((nz + ny + nx - 2, 16, D), F32),
            pltpu.SemaphoreType.DMA((count,)),
            pltpu.SemaphoreType.DMA((count,)),
            pltpu.SemaphoreType.DMA,
        ],
        compiler_params=params(collective_id=2),
        name="tokens_grad",
    )(g, normed, inv, gres, wqkv, vec, sums, packed)


def split_kernel(n, narrow_ref, wide_ref, vec_ref, *outs):
    for j in range(3):
        outs[j][...] = narrow_ref[:, THIRD * j : THIRD * (j + 1)]
    outs[3][...] = wide_ref[:, :THIRD]
    outs[4][...] = wide_ref[:, OUT_PAD : OUT_PAD + HALF]
    outs[5][...] = wide_ref[:, OUT_PAD + HALF :]
    index = lax.axis_index("dp") * 2 + lax.axis_index("mp")
    per = D // n
    vec = pltpu.roll(vec_ref[...], D - index * per, axis=1)
    for row, out in zip((2, 3, 0, 1, 4, 5, 6, 7), outs[6:]):
        out[...] = vec[row : row + 1, :per]
    wide = jnp.concatenate([vec_ref[8 + j : 9 + j, :] for j in range(FF // D)], axis=1)
    wide = pltpu.roll(jnp.broadcast_to(wide, (8, FF)), FF - index * (FF // n), axis=1)
    outs[14][...] = wide[0:1, : FF // n]


def split(narrow, wide, vec, n):
    rows = narrow.shape[0]
    vmem = pl.BlockSpec(memory_space=pltpu.VMEM)
    shapes = [(rows, THIRD)] * 4 + [(rows, HALF)] * 2 + [(1, D // n)] * 8 + [(1, FF // n)]
    return pl.pallas_call(
        functools.partial(split_kernel, n),
        in_specs=[vmem] * 3,
        out_specs=[vmem] * 15,
        out_shape=[jax.ShapeDtypeStruct(s, F32) for s in shapes],
        name="split",
    )(narrow, wide, vec)


def whole(shape):
    return pl.BlockSpec(shape, lambda i: (0,) * len(shape))


def per_image(*shape):
    return pl.BlockSpec((1, *shape), lambda i: (i,) + (0,) * len(shape))


def params(collective_id=None):
    return pltpu.CompilerParams(
        dimension_semantics=("arbitrary",), vmem_limit_bytes=62 * 1024 * 1024,
        collective_id=collective_id, has_side_effects=collective_id is not None,
    )


def on_device(
    tokens, w_query, w_key, w_value, w_out, w_up, w_down, ln1_gain, ln1_bias, b_query, b_value,
    b_out, ln2_gain, ln2_bias, b_up, b_down, cotangent,
):
    dp = lax.axis_size("dp")
    vectors = (ln1_gain, ln1_bias, b_query, b_value, b_out, ln2_gain, ln2_bias, b_down)
    qkv, e, mixed, linv, normed, inv, tok, cot, wqkv, vec, bup, wide = attn_fwd(
        (w_query, w_key, w_value, w_out.T, w_up, w_down.T), [v[None] for v in vectors], b_up[None],
        tokens, cotangent, dp,
    )
    out, gres, gmix, packed, dvec2, dbup = mlp(
        tok, cot, mixed, wide.reshape(2, D, WIDE), vec, bup, tokens.shape[0], dp
    )
    g, packed, sums, wide_sum = attn_bwd(
        qkv, e, mixed, linv, gmix, normed, wqkv, vec, dvec2, dbup, packed, dp
    )
    gtok, narrow_sum, sums = tokens_grad(
        g, normed, inv, gres, wqkv, vec, sums, packed, tokens.shape[0], dp
    )
    grads = split(narrow_sum, wide_sum, sums, dp * lax.axis_size("mp"))
    vecs = [v.reshape(-1) for v in grads[6:]]
    return (
        out, gtok, grads[0], grads[1], grads[2], grads[3].T, grads[4], grads[5].T,
        *vecs[:7], vecs[8], vecs[7],
    )


def solution(mesh):
    row, mat, tam, vec = P(("dp", "mp"), None), P("dp", "mp"), P("mp", "dp"), P("dp")
    part = P(("dp", "mp"))
    return jax.shard_map(
        on_device,
        mesh=mesh,
        in_specs=(row, mat, mat, mat, tam, mat, tam, *([vec] * 9), row),
        out_specs=(row, row, mat, mat, mat, tam, mat, tam, *([part] * 9)),
        check_vma=False,
    )
```

```python
import functools
import math

import jax
import jax.numpy as jnp
from jax import lax
from jax.experimental import pallas as pl
from jax.experimental.pallas import tpu as pltpu
from jax.sharding import PartitionSpec as P

D = 384
HD = 64
FF = 1536
S = 197
HEADS = D // HD
PAIRS = HEADS // 2

SP = 208
WIN = 224

EPS = 1e-06
RSQRT2 = 0.7071067811865476
RSQRT_TAU = 0.3989422804014327
LOG2E = 1.4426950408889634
Q_SCALE = LOG2E / math.sqrt(HD)
BF = jnp.bfloat16
F32 = jnp.float32


def dot_nn(a, b):
    return lax.dot_general(a, b, (((1,), (0,)), ((), ())), preferred_element_type=F32)


def dot_nt(a, b):
    return lax.dot_general(a, b, (((1,), (1,)), ((), ())), preferred_element_type=F32)


def dot_tn(a, b):
    return lax.dot_general(a, b, (((0,), (0,)), ((), ())), preferred_element_type=F32)


def window_of(i, rows):
    start = i * S
    base = jnp.minimum((start // 16) * 16, rows - WIN)
    return pl.multiple_of(base, 16), start - base


def load_image(ref, i):
    base, off = window_of(i, ref.shape[0])
    rows = ref[pl.ds(base, WIN), :].astype(F32)
    rows = pltpu.roll(rows, WIN - off, axis=0)[:SP]
    live = lax.broadcasted_iota(jnp.int32, rows.shape, 0) < S
    return jnp.where(live, rows, 0.0)


def store_image(ref, i, rows):
    start = i * S
    r = start % 8
    base = start - r
    total = ref.shape[0]
    groups = SP // 8
    turned = pltpu.roll(rows.reshape(groups, 8, D), r, axis=1)
    first = lax.broadcasted_iota(jnp.int32, (8, D), 0) < r
    old = ref[pl.ds(pl.multiple_of(base, 8), 8), :]
    ref[pl.ds(pl.multiple_of(base, 8), 8), :] = jnp.where(first, old, turned[0])
    for g in range(1, groups - 1):
        ref[pl.ds(pl.multiple_of(base + 8 * g, 8), 8), :] = jnp.where(
            first, turned[g - 1], turned[g]
        )
    over = base + SP > total
    here = jnp.where(over, total - 8, base + SP - 8)
    tail = [jnp.where(first, turned[g - 1], turned[g]) for g in (groups - 2, groups - 1)]
    ref[pl.ds(pl.multiple_of(here, 8), 8), :] = jnp.where(over, tail[0], tail[1])


def norm_stats(x):
    mean = jnp.mean(x, axis=-1, keepdims=True)
    centred = x - mean
    inv = lax.rsqrt(jnp.mean(centred * centred, axis=-1, keepdims=True) + EPS)
    return centred * inv, inv


def norm_backward(grad, normed, inv, gain):
    e = grad * gain
    return inv * (
        e
        - jnp.mean(e, axis=-1, keepdims=True)
        - normed * jnp.mean(e * normed, axis=-1, keepdims=True)
    )


def row_sum(x):
    return jnp.sum(x, axis=0, keepdims=True)


THIRD = D // 2
HALF = FF // 2
NARROW = 640
NARROW_CUT = 384
OUT_PAD = 256
WIDE = OUT_PAD + 2 * HALF
WIDE_CUT = 896
MESH = pl.DeviceIdType.MESH
EVERY = slice(None)


def chip_grid(dp):
    side = math.isqrt(dp // 4)
    return 4, side, side


def place_of(dims):
    _, ny, nx = dims
    dp, mp = lax.axis_index("dp"), lax.axis_index("mp")
    return dp // (ny * nx), (dp // nx) % ny, dp % nx, mp


def peers_of(dims, place):
    (nz, ny, nx), (z, y, x, mp) = dims, place

    def at(a, b, c, m):
        return ((a * ny + b) * nx + c, m)

    along = {
        "z": [((z + o) % nz, at((z + o) % nz, y, x, mp)) for o in range(1, nz)],
        "y": [((y + o) % ny, at(z, (y + o) % ny, x, mp)) for o in range(1, ny)],
        "x": [((x + o) % nx, at(z, y, (x + o) % nx, mp)) for o in range(1, nx)],
    }
    return along, at(z, y, x, 1 - mp)


def greet(along, other):
    for device in [d for peers in along.values() for _, d in peers] + [other]:
        pl.semaphore_signal(
            pltpu.get_barrier_semaphore(), inc=1, device_id=device, device_id_type=MESH
        )


def met(along):
    count = sum(len(peers) for peers in along.values()) + 1
    pl.semaphore_wait(pltpu.get_barrier_semaphore(), count)


class Copies:
    def __init__(self, send, recv):
        self.send, self.recv, self.groups, self.count = send, recv, {}, 0

    def plan(self, name, makers):
        self.groups[name] = [(self.count + i, m) for i, m in enumerate(makers)]
        self.count += len(makers)

    def each(self, names):
        for name in names:
            for index, make in self.groups[name]:
                src, dst, device = make()
                yield pltpu.make_async_remote_copy(
                    src_ref=src, dst_ref=dst, send_sem=self.send.at[index],
                    recv_sem=self.recv.at[index], device_id=device, device_id_type=MESH,
                )

    def start(self, *names):
        for copy in self.each(names):
            copy.start()

    def arrived(self, *names):
        for copy in self.each(names):
            copy.wait_recv()

    def left(self, *names):
        for copy in self.each(names):
            copy.wait_send()


def plan_gather(copies, tag, w, own, cut, along, other, place):
    z, y, x, mp = place
    low, high = pl.ds(0, cut), pl.ds(cut, w.shape[-1] - cut)

    def same(index, device):
        return lambda: (w.at[index], w.at[index], device)

    def spread(index, axis):
        return [same(index, d) for _, d in along[axis]]

    def shares(indices):
        return [same(index, other) for index in indices]

    copies.plan(tag + "1", [lambda d=d: (own, w.at[mp, z, y, x], d) for _, d in along["z"]])
    copies.plan(tag + "2l", spread((mp, EVERY, y, x, EVERY, low), "y"))
    copies.plan(tag + "2h", spread((mp, EVERY, y, x, EVERY, high), "x"))
    copies.plan(tag + "3l", spread((mp, EVERY, EVERY, x, EVERY, low), "x"))
    copies.plan(tag + "3h", spread((mp, EVERY, y, EVERY, EVERY, high), "y"))
    copies.plan(tag + "s1", shares([(mp, EVERY, y, x)]))
    copies.plan(tag + "s2l", shares([(mp, EVERY, b, x, EVERY, low) for b, _ in along["y"]]))
    copies.plan(tag + "s2h", shares([(mp, EVERY, y, c, EVERY, high) for c, _ in along["x"]]))
    copies.plan(tag + "s3l", shares([(mp, EVERY, EVERY, c, EVERY, low) for c, _ in along["x"]]))
    copies.plan(tag + "s3h", shares([(mp, EVERY, b, EVERY, EVERY, high) for b, _ in along["y"]]))


def attn_fwd_kernel(dims, n, *refs):
    (wq, wk, wv, wot, wu, wdt), vectors, bup_in = refs[:6], refs[6:14], refs[14]
    tok_ref, cot_ref = refs[15:17]
    (
        qkv_ref, e_ref, mixed_ref, linv_ref, normed_ref, inv_ref, tokp_ref, cotp_ref, w_ref, vec_ref,
        bup_ref, wide,
    ) = refs[17:29]
    narrow, v, own, normed_all, inv_all, tok_all, cot_all, send, recv, sem = refs[29:]
    i = pl.program_id(0)
    nz, ny, nx = dims
    place = place_of(dims)
    z, y, x, mp = place
    rows = own.shape[0]
    along, other = peers_of(dims, place)
    copies = Copies(send, recv)
    plan_gather(copies, "n", narrow, narrow.at[mp, z, y, x], NARROW_CUT, along, other, place)
    plan_gather(copies, "w", wide, own, WIDE_CUT, along, other, place)

    def vec_spread(index, axis):
        return [lambda d=d: (v.at[index], v.at[index], d) for _, d in along[axis]]

    copies.plan("v1", vec_spread((z, y, x), "z"))
    copies.plan("v2", vec_spread((EVERY, y, x), "y"))
    copies.plan("v3", vec_spread((EVERY, EVERY, x), "x"))
    keep = pltpu.make_async_copy(own, wide.at[mp, z, y, x], sem)

    def norms(first, last):
        @pl.loop(first, last)
        def _(j):
            tok = load_image(tok_ref, j)
            normed, inv = norm_stats(tok)
            tok_all[j] = tok.astype(BF)
            cot_all[j] = load_image(cot_ref, j).astype(BF)
            normed_all[j] = normed
            inv_all[j] = jnp.broadcast_to(inv, (SP, 128))

    @pl.when(i == 0)
    def _():
        narrow[mp, z, y, x] = jnp.concatenate(
            [wq[...], wk[...], wv[...], jnp.zeros((rows, NARROW - 3 * THIRD), BF)], axis=1
        )
        own[...] = jnp.concatenate(
            [wot[...], jnp.zeros((rows, OUT_PAD - THIRD), BF), wu[...], wdt[...]], axis=1
        )
        v[z, y, x] = jnp.zeros((16, 128), F32)
        for j, vector in enumerate(vectors):
            v[z, y, x, j : j + 1, :rows] = vector[...].astype(F32)
        v[z, y, x, 8:9, : bup_in.shape[1]] = bup_in[...].astype(F32)
        greet(along, other)
        keep.start()
        norms(0, n // 4)
        met(along)
        copies.start("v1", "n1")
        norms(n // 4, n // 2)
        copies.arrived("v1", "n1")
        copies.start("v2", "n2l", "n2h", "w1", "ns1")
        norms(n // 2, (3 * n) // 4)
        copies.arrived("v2", "n2l", "n2h")
        copies.start("v3", "n3l", "n3h", "ns2l", "ns2h")
        norms((3 * n) // 4, n)
        copies.arrived("v3", "n3l")
        copies.start("ns3l")
        copies.arrived("n3h")
        copies.start("ns3h")
        keep.wait()
        copies.arrived("w1")
        copies.start("w2l", "w2h", "ws1")
        spots = [(a, b, c) for a in range(nz) for b in range(ny) for c in range(nx)]
        vec_ref[...] = jnp.concatenate([v[s][0:8, :rows] for s in spots], axis=1)
        bup_ref[...] = jnp.concatenate([v[s][8:9, : bup_in.shape[1]] for s in spots], axis=1)
        copies.arrived("ns1", "ns2l", "ns2h", "ns3l", "ns3h")
        group = 48 // rows
        for t in range(len(spots) // group):
            block = [
                jnp.concatenate(
                    [narrow[(m,) + s].astype(F32) for s in spots[t * group : (t + 1) * group]], axis=0
                )
                for m in range(2)
            ]
            for j in range(3):
                cols = slice(THIRD * j, THIRD * (j + 1))
                w_ref[48 * t : 48 * (t + 1), D * j : D * (j + 1)] = jnp.concatenate(
                    [half[:, cols] for half in block], axis=1
                ).astype(BF)

    @pl.when(i == 3)
    def _():
        copies.arrived("w2l", "w2h")
        copies.start("w3l", "w3h", "ws2l", "ws2h")

    normed = normed_all[i]
    normed_ref[0] = normed
    inv_ref[0] = inv_all[i]
    tokp_ref[0] = tok_all[i]
    cotp_ref[0] = cot_all[i]
    h1 = (normed * vec_ref[0:1, :] + vec_ref[1:2, :]).astype(BF)
    q = ((dot_nn(h1, w_ref[:, 0:D]) + vec_ref[2:3, :]) * Q_SCALE).astype(BF)
    k = dot_nn(h1, w_ref[:, D : 2 * D]).astype(BF)
    value = (dot_nn(h1, w_ref[:, 2 * D :]) + vec_ref[3:4, :]).astype(BF)
    qkv_ref[0, :, 0:D] = q
    qkv_ref[0, :, D : 2 * D] = k
    qkv_ref[0, :, 2 * D :] = value
    lane = lax.broadcasted_iota(jnp.int32, (SP, 2 * HD), 1)
    is_key = lax.broadcasted_iota(jnp.int32, (SP, SP), 1) < S
    zero = jnp.zeros((SP, 2 * HD), BF)
    one = jnp.ones((SP, 2 * HD), BF)
    for p in range(PAIRS):
        cols = slice(2 * HD * p, 2 * HD * (p + 1))
        total = None
        for h in range(2):
            mine = (lane < HD) if h == 0 else (lane >= HD)
            kh = jnp.where(mine, k[:, cols], zero)
            vh = jnp.where(mine, value[:, cols], zero)
            scores = dot_nt(q[:, cols], kh)
            scores = jnp.where(is_key, scores, -1e30)
            top = jnp.max(scores, axis=-1, keepdims=True)
            e = jnp.exp2(scores - top).astype(BF)
            e_ref[0, 2 * p + h] = e
            part = dot_nn(e, jnp.concatenate([vh, jnp.where(mine, one, zero)], axis=1))
            total = part if total is None else total + part
        linv = 1.0 / total[:, 2 * HD :]
        linv_ref[0, :, cols] = linv
        mixed_ref[0, :, cols] = (total[:, : 2 * HD] * linv).astype(BF)

    @pl.when(i == n - 5)
    def _():
        copies.arrived("w3l", "w3h")
        copies.start("ws3l", "ws3h")

    @pl.when(i == n - 1)
    def _():
        copies.arrived("ws1", "ws2l", "ws2h", "ws3l", "ws3h")
        copies.left(*copies.groups)


def attn_fwd(mats, vectors, bup, tokens, cot, dp):
    dims = chip_grid(dp)
    nz, ny, nx = dims
    rows = D // dp
    n = tokens.shape[0] // S
    count = 2 * (nz - 1 + 4 * (ny - 1) + 4 * (nx - 1) + 1) + nz + ny + nx - 3
    inputs = (*mats, *vectors, bup, tokens, cot)
    return pl.pallas_call(
        functools.partial(attn_fwd_kernel, dims, n),
        grid=(n,),
        in_specs=[whole(a.shape) for a in inputs],
        out_specs=[
            per_image(SP, 3 * D), per_image(HEADS, SP, SP), per_image(SP, D), per_image(SP, D),
            per_image(SP, D), per_image(SP, 128), per_image(SP, D), per_image(SP, D),
            whole((D, 3 * D)), whole((8, D)), whole((1, FF)), pl.BlockSpec(memory_space=pl.ANY),
        ],
        out_shape=[
            jax.ShapeDtypeStruct((n, SP, 3 * D), BF),
            jax.ShapeDtypeStruct((n, HEADS, SP, SP), BF),
            jax.ShapeDtypeStruct((n, SP, D), BF),
            jax.ShapeDtypeStruct((n, SP, D), F32),
            jax.ShapeDtypeStruct((n, SP, D), F32),
            jax.ShapeDtypeStruct((n, SP, 128), F32),
            jax.ShapeDtypeStruct((n, SP, D), BF),
            jax.ShapeDtypeStruct((n, SP, D), BF),
            jax.ShapeDtypeStruct((D, 3 * D), BF),
            jax.ShapeDtypeStruct((8, D), F32),
            jax.ShapeDtypeStruct((1, FF), F32),
            jax.ShapeDtypeStruct((2, nz, ny, nx, rows, WIDE), BF),
        ],
        scratch_shapes=[
            pltpu.VMEM((2, nz, ny, nx, rows, NARROW), BF),
            pltpu.VMEM((nz, ny, nx, 16, 128), F32),
            pltpu.VMEM((rows, WIDE), BF),
            pltpu.VMEM((n, SP, D), F32),
            pltpu.VMEM((n, SP, 128), F32),
            pltpu.VMEM((n, SP, D), BF),
            pltpu.VMEM((n, SP, D), BF),
            pltpu.SemaphoreType.DMA((count,)),
            pltpu.SemaphoreType.DMA((count,)),
            pltpu.SemaphoreType.DMA,
        ],
        compiler_params=params(collective_id=0),
        name="attn_fwd",
    )(*inputs)


def fold(x):
    return jnp.sum(x.reshape(x.shape[0] // 8, 8, x.shape[1]), axis=0)


CHUNK = 16


def mlp_kernel(
    dims, n, tok_ref, cot_ref, mixed_ref, w_ref, vec_ref, bup_ref,
    out_ref, gres_ref, gmix_ref, grads_ref, dvec_ref, dbup_ref,
    act_ref, gp_ref, wot_ref, dwot_ref, dwup_ref, dwdt_ref,
    h2_ref, h2t_ref, cott_ref, mix_ref, gr_ref, outf_ref, out_old, gh2_ref, cotf_ref, norm_ref,
    inv_ref, sums_ref, upsum_ref,
):
    i = pl.program_id(0)
    step = 256
    tiles = FF // step
    chunks = [slice(c, c + CHUNK) for c in range(0, SP, CHUNK)]

    @pl.when(i == 0)
    def _():
        wot_ref[...] = jnp.concatenate([w_ref[0, :, :THIRD], w_ref[1, :, :THIRD]], axis=1)
        for ref in (
            dwot_ref, dwup_ref, dwdt_ref, act_ref, gp_ref, h2t_ref, cott_ref, mix_ref, out_old,
            gh2_ref, cotf_ref, norm_ref, inv_ref, sums_ref, upsum_ref,
        ):
            ref[...] = jnp.zeros_like(ref)

    def weight_tile(j):
        cols = slice(step * j, step * (j + 1))
        dwup_ref[:, cols] += dot_nn(h2t_ref[...], gp_ref[:, cols])
        dwdt_ref[:, cols] += dot_nn(cott_ref[...], act_ref[:, cols])

    def finish(image, beside):
        beside(0)
        slot = image % 2
        for at in chunks:
            gh2, normed, cot = gh2_ref[at, :], norm_ref[at, :], cotf_ref[at, :]
            gres = cot + norm_backward(gh2, normed, inv_ref[at, 0:1], vec_ref[5:6, :])
            gres_ref[slot, at, :] = gres
            gr_ref[at, :] = gres.astype(BF)
            sums_ref[0] += fold(gres)
            sums_ref[1] += fold(gh2 * normed)
            sums_ref[2] += fold(gh2)
            sums_ref[3] += fold(cot)
        beside(1)
        gmix_ref[slot] = dot_nn(gr_ref[...], wot_ref[...]).astype(BF)
        beside(2)
        store_image(outf_ref, image, out_old[...])
        dwot_ref[...] += dot_tn(gr_ref[...], mix_ref[...])
        beside(3)

    finish(jnp.maximum(i - 1, 0), weight_tile)
    weight_tile(4)
    attended = dot_nt(mixed_ref[0], wot_ref[...])
    for at in chunks:
        cot = cot_ref[0, at, :].astype(F32)
        resid = tok_ref[0, at, :].astype(F32) + attended[at] + vec_ref[4:5, :]
        normed, inv = norm_stats(resid)
        h2_ref[at, :] = (normed * vec_ref[5:6, :] + vec_ref[6:7, :]).astype(BF)
        cotf_ref[at, :] = cot
        norm_ref[at, :] = normed
        inv_ref[at, :] = jnp.broadcast_to(inv, (CHUNK, 128))
        out_old[at, :] = resid + vec_ref[7:8, :]
    weight_tile(5)
    mix_ref[...] = mixed_ref[0]
    h2 = h2_ref[...]
    cot = cot_ref[0]
    h2t_ref[...] = h2.T
    cott_ref[...] = cot.T
    for j in range(tiles):
        cols = slice(step * j, step * (j + 1))
        m, at = divmod(step * j, HALF)
        u = dot_nn(h2, w_ref[m, :, OUT_PAD + at : OUT_PAD + at + step]) + bup_ref[:, cols]
        ga = dot_nn(cot, w_ref[m, :, OUT_PAD + HALF + at : OUT_PAD + HALF + at + step])
        cdf = 0.5 * (1.0 + lax.erf(u * RSQRT2))
        act_ref[:, cols] = (u * cdf).astype(BF)
        gp = ga * (cdf + u * jnp.exp(-0.5 * u * u) * RSQRT_TAU)
        upsum_ref[:, cols] += fold(gp)
        gp_ref[:, cols] = gp.astype(BF)
    out = out_old[...]
    gh2 = None
    for m in range(2):
        cols = slice(HALF * m, HALF * (m + 1))
        out = out + dot_nt(act_ref[:, cols], w_ref[m, :, OUT_PAD + HALF :])
        part = dot_nt(gp_ref[:, cols], w_ref[m, :, OUT_PAD : OUT_PAD + HALF])
        gh2 = part if gh2 is None else gh2 + part
    out_old[...] = out
    gh2_ref[...] = gh2

    @pl.when(i == n - 1)
    def _():
        finish(i, weight_tile)
        weight_tile(4)
        weight_tile(5)
        out_ref[...] = outf_ref[...].astype(BF)
        for k in range(4):
            dvec_ref[k : k + 1, :] = row_sum(sums_ref[k])
        dvec_ref[4:8, :] = jnp.zeros((4, D), F32)
        dbup_ref[...] = row_sum(upsum_ref[...])
        nz, ny, nx = dims
        rows = grads_ref.shape[4]
        spots = [(a, b, c) for a in range(nz) for b in range(ny) for c in range(nx)]
        group = 48 // rows
        for t in range(len(spots) // group):
            at = slice(48 * t, 48 * (t + 1))
            for m in range(2):
                parts = [
                    dwot_ref[at, THIRD * m : THIRD * (m + 1)],
                    jnp.zeros((48, OUT_PAD - THIRD), F32),
                    dwup_ref[at, HALF * m : HALF * (m + 1)],
                    dwdt_ref[at, HALF * m : HALF * (m + 1)],
                ]
                block = jnp.concatenate(parts, axis=1)
                for g in range(group):
                    grads_ref[(m,) + spots[t * group + g]] = block[
                        g * rows : (g + 1) * rows
                    ].astype(BF)


def mlp(tok, cot, mixed, wide, vec, bup, rows, dp):
    dims = chip_grid(dp)
    n = rows // S
    packed = (2, *dims, D // dp, WIDE)
    late = pl.BlockSpec((2, SP, D), lambda i: (jnp.maximum(i - 1, 0) // 2, 0, 0))
    return pl.pallas_call(
        functools.partial(mlp_kernel, dims, n),
        grid=(n,),
        in_specs=[
            per_image(SP, D), per_image(SP, D), per_image(SP, D), whole((2, D, WIDE)), whole((8, D)),
            whole((1, FF)),
        ],
        out_specs=[whole((rows, D)), late, late, whole(packed), whole((8, D)), whole((1, FF))],
        out_shape=[
            jax.ShapeDtypeStruct((rows, D), BF),
            jax.ShapeDtypeStruct((n, SP, D), F32),
            jax.ShapeDtypeStruct((n, SP, D), BF),
            jax.ShapeDtypeStruct(packed, BF),
            jax.ShapeDtypeStruct((8, D), F32),
            jax.ShapeDtypeStruct((1, FF), F32),
        ],
        scratch_shapes=[
            pltpu.VMEM((SP, FF), BF), pltpu.VMEM((SP, FF), BF), pltpu.VMEM((D, D), BF),
            pltpu.VMEM((D, D), F32), pltpu.VMEM((D, FF), F32), pltpu.VMEM((D, FF), F32),
            pltpu.VMEM((SP, D), BF), pltpu.VMEM((D, SP), BF), pltpu.VMEM((D, SP), BF),
            pltpu.VMEM((SP, D), BF), pltpu.VMEM((SP, D), BF), pltpu.VMEM((rows, D), F32),
            pltpu.VMEM((SP, D), F32), pltpu.VMEM((SP, D), F32), pltpu.VMEM((SP, D), F32),
            pltpu.VMEM((SP, D), F32), pltpu.VMEM((SP, 128), F32), pltpu.VMEM((4, 8, D), F32),
            pltpu.VMEM((8, FF), F32),
        ],
        compiler_params=params(),
        name="mlp",
    )(tok, cot, mixed, wide, vec, bup)


class Reduction:
    def __init__(self, dims, copies, tag, packed, bufs, cut):
        self.dims, self.copies, self.packed, self.cut = dims, copies, packed, cut
        self.place = place_of(dims)
        self.along, self.other = peers_of(dims, self.place)
        z, y, x, mp = self.place
        self.p, self.a1, self.b1, self.ra1, self.rb1, self.ra2, self.rb2, self.f, self.rz = bufs
        low, high = pl.ds(0, cut), pl.ds(cut, packed.shape[-1] - cut)
        along = self.along
        copies.plan(tag + "pair", [lambda: (packed.at[1 - mp], self.p, self.other)])
        copies.plan(tag + "1l", [
            lambda o=o, c=c, d=d: (self.p.at[EVERY, EVERY, c, EVERY, low], self.ra1.at[o], d)
            for o, (c, d) in enumerate(along["x"])
        ])
        copies.plan(tag + "1h", [
            lambda o=o, b=b, d=d: (self.p.at[EVERY, b, EVERY, EVERY, high], self.rb1.at[o], d)
            for o, (b, d) in enumerate(along["y"])
        ])
        copies.plan(tag + "2l", [
            lambda o=o, b=b, d=d: (self.a1.at[EVERY, b], self.ra2.at[o], d)
            for o, (b, d) in enumerate(along["y"])
        ])
        copies.plan(tag + "2h", [
            lambda o=o, c=c, d=d: (self.b1.at[EVERY, c], self.rb2.at[o], d)
            for o, (c, d) in enumerate(along["x"])
        ])
        copies.plan(tag + "3", [
            lambda o=o, a=a, d=d: (self.f.at[a], self.rz.at[o], d)
            for o, (a, d) in enumerate(along["z"])
        ])

    @staticmethod
    def count(dims):
        nz, ny, nx = dims
        return 1 + 2 * (ny - 1) + 2 * (nx - 1) + nz - 1

    @staticmethod
    def scratch(dims, rows, width, cut):
        nz, ny, nx = dims

        def buf(w, *shape):
            return pltpu.VMEM((*shape, rows, w), BF)

        rest = width - cut
        return [
            buf(width, nz, ny, nx), buf(cut, nz, ny), buf(rest, nz, nx),
            buf(cut, nx - 1, nz, ny), buf(rest, ny - 1, nz, nx),
            buf(cut, ny - 1, nz), buf(rest, nx - 1, nz), buf(width, nz), buf(width, nz - 1),
        ]

    def add_pair(self, mine):
        nz, ny, nx = self.dims
        for i in range(nz):
            for j in range(ny):
                for k in range(nx):
                    total = mine[i, j, k].astype(F32) + self.p[i, j, k].astype(F32)
                    self.p[i, j, k] = total.astype(BF)

    def add_first_low(self):
        nz, ny, nx = self.dims
        x = self.place[2]
        for i in range(nz):
            for j in range(ny):
                total = self.p[i, j, x, :, : self.cut].astype(F32)
                for o in range(nx - 1):
                    total = total + self.ra1[o, i, j].astype(F32)
                self.a1[i, j] = total.astype(BF)

    def add_first_high(self):
        nz, ny, nx = self.dims
        y = self.place[1]
        for i in range(nz):
            for k in range(nx):
                total = self.p[i, y, k, :, self.cut :].astype(F32)
                for o in range(ny - 1):
                    total = total + self.rb1[o, i, k].astype(F32)
                self.b1[i, k] = total.astype(BF)

    def add_second(self):
        nz, ny, nx = self.dims
        _, y, x, _ = self.place
        for i in range(nz):
            total = self.a1[i, y].astype(F32)
            for o in range(ny - 1):
                total = total + self.ra2[o, i].astype(F32)
            self.f[i, :, : self.cut] = total.astype(BF)
            total = self.b1[i, x].astype(F32)
            for o in range(nx - 1):
                total = total + self.rb2[o, i].astype(F32)
            self.f[i, :, self.cut :] = total.astype(BF)

    def add_third(self):
        total = self.f[self.place[0]].astype(F32)
        for o in range(self.dims[0] - 1):
            total = total + self.rz[o].astype(F32)
        return total


def backward_kernel(
    dims, n, qkv_ref, e_ref, mixed_ref, linv_ref, gmix_ref, normed_ref, inv_ref, gres_ref, w_ref,
    vec_ref, dvec2_ref, dbup_ref, packed, gtok_ref, narrow_ref, wide_ref, total_ref, *refs,
):
    g_ref, acc_ref, gsum_ref, narrow, sums, vs, vr = refs[:7]
    wide_bufs, mine, narrow_bufs = refs[7:16], refs[16], refs[17:26]
    send, recv, sem = refs[26:]
    i = pl.program_id(0)
    copies = Copies(send, recv)
    wide = Reduction(dims, copies, "w", packed, wide_bufs, WIDE_CUT)
    thin = Reduction(dims, copies, "n", narrow, narrow_bufs, NARROW_CUT)
    mp = wide.place[3]
    keep = pltpu.make_async_copy(packed.at[mp], mine, sem)
    stages = [[wide.other], *([d for _, d in wide.along[axis]] for axis in "xyz")]
    bases = [sum(len(s) for s in stages[:k]) for k in range(4)]
    for k, devices in enumerate(stages):
        copies.plan("v%d" % k, [
            lambda k=k, o=o, d=d: (sums if k == 0 else vs.at[k - 1], vr.at[bases[k] + o], d)
            for o, d in enumerate(devices)
        ])

    def vec_add(k):
        total = sums[...] if k == 0 else vs[k - 1]
        for o in range(len(stages[k])):
            total = total + vr[bases[k] + o]
        if k < 3:
            vs[k] = total
        else:
            total_ref[...] = total

    @pl.when(i == 0)
    def _():
        greet(wide.along, wide.other)
        keep.start()
        acc_ref[...] = jnp.zeros_like(acc_ref)
        gsum_ref[...] = jnp.zeros_like(gsum_ref)
        met(wide.along)
        copies.start("wpair")

    @pl.when(i == 2)
    def _():
        keep.wait()
        copies.arrived("wpair")
        wide.add_pair(mine)
        copies.start("w1l", "w1h")

    @pl.when(i == n // 2)
    def _():
        copies.arrived("w1l", "w1h")
        wide.add_first_low()
        wide.add_first_high()
        copies.start("w2l", "w2h")

    @pl.when(i == (3 * n) // 4)
    def _():
        copies.arrived("w2l", "w2h")
        wide.add_second()
        copies.start("w3")

    @pl.when(i < n)
    def _():
        lane = lax.broadcasted_iota(jnp.int32, (SP, 2 * HD), 1)
        zero = jnp.zeros((SP, 2 * HD), BF)
        minus = jnp.full((SP, 2 * HD), -1.0, BF)
        for p in range(PAIRS):
            lo, hi = 2 * HD * p, 2 * HD * (p + 1)
            q = qkv_ref[0, :, lo:hi]
            k = qkv_ref[0, :, D + lo : D + hi]
            v = qkv_ref[0, :, 2 * D + lo : 2 * D + hi]
            go_f = gmix_ref[0, :, lo:hi].astype(F32) * linv_ref[0, :, lo:hi]
            go = go_f.astype(BF)
            god = jnp.concatenate(
                [go, (go_f * mixed_ref[0, :, lo:hi].astype(F32)).astype(BF)], axis=1
            )
            gq = gk = gv = None
            for h in range(2):
                own = (lane < HD) if h == 0 else (lane >= HD)
                e = e_ref[0, 2 * p + h]
                vd = jnp.concatenate(
                    [jnp.where(own, v, zero), jnp.where(own, minus, zero)], axis=1
                )
                ds = e * dot_nt(god, vd).astype(BF)
                part_q = dot_nn(ds, jnp.where(own, k, zero))
                part_k = dot_tn(ds, jnp.where(own, q, zero))
                part_v = dot_tn(e, jnp.where(own, go, zero))
                gq = part_q if gq is None else gq + part_q
                gk = part_k if gk is None else gk + part_k
                gv = part_v if gv is None else gv + part_v
            gq = gq * (1.0 / math.sqrt(HD))
            gk = gk * (1.0 / LOG2E)
            for j, grad in enumerate((gq, gk, gv)):
                gsum_ref[:, D * j + lo : D * j + hi] += fold(grad)
                g_ref[i, :, D * j + lo : D * j + hi] = grad.astype(BF)
        acc_ref[...] += dot_tn(normed_ref[0].astype(BF), g_ref[i])

    @pl.when(i == n - 1)
    def _():
        nz, ny, nx = dims
        rows = narrow.shape[4]
        spots = [(a, b, c) for a in range(nz) for b in range(ny) for c in range(nx)]
        group = 48 // rows
        turned = vec_ref[...].T
        gsum = row_sum(gsum_ref[...])
        gains = []
        for t in range(len(spots) // group):
            at = slice(48 * t, 48 * (t + 1))
            acc = acc_ref[at, :]
            gains.append(jnp.sum(acc * w_ref[at, :].astype(F32), axis=1, keepdims=True))
            dw = acc * turned[at, 0:1] + turned[at, 1:2] * gsum
            for m in range(2):
                parts = [dw[:, D * j + THIRD * m : D * j + THIRD * (m + 1)] for j in range(3)]
                parts.append(jnp.zeros((48, NARROW - 3 * THIRD), F32))
                block = jnp.concatenate(parts, axis=1)
                for k in range(group):
                    narrow[(m,) + spots[t * group + k]] = block[
                        k * rows : (k + 1) * rows
                    ].astype(BF)
        high = gsum.astype(BF)
        low = (gsum - high.astype(F32)).astype(BF)
        row = lax.broadcasted_iota(jnp.int32, (16, 3 * D), 0)
        both = jnp.where(row == 0, high, jnp.where(row == 1, low, jnp.zeros((16, 3 * D), BF)))
        sums[0:1] = gsum[:, :D]
        sums[1:2] = gsum[:, 2 * D :]
        gain = jnp.broadcast_to(jnp.concatenate(gains, axis=0), (D, 128)).T
        sums[2:3] = gain[0:1, :]
        sums[3:4] = row_sum(dot_nt(both, w_ref[...]))
        sums[4:8] = dvec2_ref[0:4]
        for j in range(FF // D):
            sums[8 + j : 9 + j] = dbup_ref[:, D * j : D * (j + 1)]
        sums[12:16] = jnp.zeros((4, D), F32)
        copies.start("npair", "v0")

    @pl.when(i == n + 3)
    def _():
        copies.arrived("npair", "v0")
        thin.add_pair(narrow.at[mp])
        vec_add(0)
        copies.start("n1l", "n1h", "v1")

    @pl.when(i == n + 5)
    def _():
        copies.arrived("w3")
        wide_ref[...] = wide.add_third()

    @pl.when(i == n + 8)
    def _():
        copies.arrived("n1l", "v1")
        thin.add_first_low()
        vec_add(1)
        copies.start("n2l", "v2")
        copies.arrived("n1h")
        thin.add_first_high()
        copies.start("n2h")

    @pl.when(i == n + 12)
    def _():
        copies.arrived("n2l", "n2h", "v2")
        thin.add_second()
        vec_add(2)
        copies.start("n3", "v3")

    @pl.when(i >= n)
    def _():
        image = i - n
        inv = inv_ref[0]
        inv = jnp.concatenate([inv, inv, inv], axis=1)
        gh1 = dot_nt(g_ref[jnp.maximum(image, 0)], w_ref[...])
        gtok = gres_ref[0] + norm_backward(gh1, normed_ref[0], inv, vec_ref[0:1, :])
        store_image(gtok_ref, jnp.maximum(image, 0), gtok)

    @pl.when(i == 2 * n - 1)
    def _():
        copies.arrived("n3", "v3")
        narrow_ref[...] = thin.add_third()
        vec_add(3)
        copies.left(*copies.groups)


def backward(qkv, e, mixed, linv, gmix, normed, inv, gres, wqkv, vec, dvec2, dbup, packed, tall, dp):
    dims = chip_grid(dp)
    nz, ny, nx = dims
    n = qkv.shape[0]
    rows = D // dp
    count = 2 * Reduction.count(dims) + nz + ny + nx - 2

    def heads(*shape):
        return pl.BlockSpec((1, *shape), lambda i: (jnp.minimum(i, n - 1),) + (0,) * len(shape))

    def after(*shape):
        return pl.BlockSpec((1, *shape), lambda i: (jnp.maximum(i - n, 0),) + (0,) * len(shape))

    def twice(*shape):
        return pl.BlockSpec((1, *shape), lambda i: (i % n,) + (0,) * len(shape))

    return pl.pallas_call(
        functools.partial(backward_kernel, dims, n),
        grid=(2 * n,),
        in_specs=[
            heads(SP, 3 * D), heads(HEADS, SP, SP), heads(SP, D), heads(SP, D), heads(SP, D),
            twice(SP, D), after(SP, 128), after(SP, D), whole((D, 3 * D)), whole((8, D)),
            whole((8, D)), whole((1, FF)), pl.BlockSpec(memory_space=pl.ANY),
        ],
        out_specs=[
            whole((tall, D)), whole((rows, NARROW)), whole((rows, WIDE)), whole((16, D)),
        ],
        out_shape=[
            jax.ShapeDtypeStruct((tall, D), F32),
            jax.ShapeDtypeStruct((rows, NARROW), F32),
            jax.ShapeDtypeStruct((rows, WIDE), F32),
            jax.ShapeDtypeStruct((16, D), F32),
        ],
        scratch_shapes=[
            pltpu.VMEM((n, SP, 3 * D), BF),
            pltpu.VMEM((D, 3 * D), F32),
            pltpu.VMEM((8, 3 * D), F32),
            pltpu.VMEM((2, *dims, rows, NARROW), BF),
            pltpu.VMEM((16, D), F32),
            pltpu.VMEM((3, 16, D), F32),
            pltpu.VMEM((nz + ny + nx - 2, 16, D), F32),
            *Reduction.scratch(dims, rows, WIDE, WIDE_CUT),
            pltpu.VMEM((*dims, rows, WIDE), BF),
            *Reduction.scratch(dims, rows, NARROW, NARROW_CUT),
            pltpu.SemaphoreType.DMA((count,)),
            pltpu.SemaphoreType.DMA((count,)),
            pltpu.SemaphoreType.DMA,
        ],
        compiler_params=params(collective_id=1),
        name="backward",
    )(qkv, e, mixed, linv, gmix, normed, inv, gres, wqkv, vec, dvec2, dbup, packed)


def split_kernel(n, narrow_ref, wide_ref, vec_ref, *outs):
    for j in range(3):
        outs[j][...] = narrow_ref[:, THIRD * j : THIRD * (j + 1)]
    outs[3][...] = wide_ref[:, :THIRD]
    outs[4][...] = wide_ref[:, OUT_PAD : OUT_PAD + HALF]
    outs[5][...] = wide_ref[:, OUT_PAD + HALF :]
    index = lax.axis_index("dp") * 2 + lax.axis_index("mp")
    per = D // n
    vec = pltpu.roll(vec_ref[...], D - index * per, axis=1)
    for row, out in zip((2, 3, 0, 1, 4, 5, 6, 7), outs[6:]):
        out[...] = vec[row : row + 1, :per]
    wide = jnp.concatenate([vec_ref[8 + j : 9 + j, :] for j in range(FF // D)], axis=1)
    wide = pltpu.roll(jnp.broadcast_to(wide, (8, FF)), FF - index * (FF // n), axis=1)
    outs[14][...] = wide[0:1, : FF // n]


def split(narrow, wide, vec, n):
    rows = narrow.shape[0]
    vmem = pl.BlockSpec(memory_space=pltpu.VMEM)
    shapes = [(rows, THIRD)] * 4 + [(rows, HALF)] * 2 + [(1, D // n)] * 8 + [(1, FF // n)]
    return pl.pallas_call(
        functools.partial(split_kernel, n),
        in_specs=[vmem] * 3,
        out_specs=[vmem] * 15,
        out_shape=[jax.ShapeDtypeStruct(s, F32) for s in shapes],
        name="split",
    )(narrow, wide, vec)


def whole(shape):
    return pl.BlockSpec(shape, lambda i: (0,) * len(shape))


def per_image(*shape):
    return pl.BlockSpec((1, *shape), lambda i: (i,) + (0,) * len(shape))


def params(collective_id=None):
    return pltpu.CompilerParams(
        dimension_semantics=("arbitrary",), vmem_limit_bytes=62 * 1024 * 1024,
        collective_id=collective_id, has_side_effects=collective_id is not None,
    )


def on_device(
    tokens, w_query, w_key, w_value, w_out, w_up, w_down, ln1_gain, ln1_bias, b_query, b_value,
    b_out, ln2_gain, ln2_bias, b_up, b_down, cotangent,
):
    dp = lax.axis_size("dp")
    vectors = (ln1_gain, ln1_bias, b_query, b_value, b_out, ln2_gain, ln2_bias, b_down)
    qkv, e, mixed, linv, normed, inv, tok, cot, wqkv, vec, bup, wide = attn_fwd(
        (w_query, w_key, w_value, w_out.T, w_up, w_down.T), [v[None] for v in vectors], b_up[None],
        tokens, cotangent, dp,
    )
    out, gres, gmix, packed, dvec2, dbup = mlp(
        tok, cot, mixed, wide.reshape(2, D, WIDE), vec, bup, tokens.shape[0], dp
    )
    gtok, narrow_sum, wide_sum, sums = backward(
        qkv, e, mixed, linv, gmix, normed, inv, gres, wqkv, vec, dvec2, dbup, packed,
        tokens.shape[0], dp,
    )
    grads = split(narrow_sum, wide_sum, sums, dp * lax.axis_size("mp"))
    vecs = [v.reshape(-1) for v in grads[6:]]
    return (
        out, gtok, grads[0], grads[1], grads[2], grads[3].T, grads[4], grads[5].T,
        *vecs[:7], vecs[8], vecs[7],
    )


def solution(mesh):
    row, mat, tam, vec = P(("dp", "mp"), None), P("dp", "mp"), P("mp", "dp"), P("dp")
    part = P(("dp", "mp"))
    return jax.shard_map(
        on_device,
        mesh=mesh,
        in_specs=(row, mat, mat, mat, tam, mat, tam, *([vec] * 9), row),
        out_specs=(row, row, mat, mat, mat, tam, mat, tam, *([part] * 9)),
        check_vma=False,
    )
```

```python
import functools
import math

import jax
import jax.numpy as jnp
from jax import lax
from jax.experimental import pallas as pl
from jax.experimental.pallas import tpu as pltpu
from jax.sharding import PartitionSpec as P

D = 384
HD = 64
FF = 1536
S = 197
HEADS = D // HD
PAIRS = HEADS // 2

SP = 208
WIN = 224
G = 2

EPS = 1e-06
RSQRT2 = 0.7071067811865476
RSQRT_TAU = 0.3989422804014327
LOG2E = 1.4426950408889634
Q_SCALE = LOG2E / math.sqrt(HD)
BF = jnp.bfloat16
F32 = jnp.float32


def dot_nn(a, b):
    return lax.dot_general(a, b, (((1,), (0,)), ((), ())), preferred_element_type=F32)


def dot_nt(a, b):
    return lax.dot_general(a, b, (((1,), (1,)), ((), ())), preferred_element_type=F32)


def dot_tn(a, b):
    return lax.dot_general(a, b, (((0,), (0,)), ((), ())), preferred_element_type=F32)


def window_of(i, rows):
    start = i * S
    base = jnp.minimum((start // 16) * 16, rows - WIN)
    return pl.multiple_of(base, 16), start - base


def load_image(ref, i):
    base, off = window_of(i, ref.shape[0])
    rows = ref[pl.ds(base, WIN), :].astype(F32)
    rows = pltpu.roll(rows, WIN - off, axis=0)[:SP]
    live = lax.broadcasted_iota(jnp.int32, rows.shape, 0) < S
    return jnp.where(live, rows, 0.0)


def store_image(ref, i, rows):
    start = i * S
    r = start % 8
    base = start - r
    total = ref.shape[0]
    groups = SP // 8
    turned = pltpu.roll(rows.reshape(groups, 8, D), r, axis=1)
    first = lax.broadcasted_iota(jnp.int32, (8, D), 0) < r
    old = ref[pl.ds(pl.multiple_of(base, 8), 8), :]
    ref[pl.ds(pl.multiple_of(base, 8), 8), :] = jnp.where(first, old, turned[0])
    for g in range(1, groups - 1):
        ref[pl.ds(pl.multiple_of(base + 8 * g, 8), 8), :] = jnp.where(
            first, turned[g - 1], turned[g]
        )
    over = base + SP > total
    here = jnp.where(over, total - 8, base + SP - 8)
    tail = [jnp.where(first, turned[g - 1], turned[g]) for g in (groups - 2, groups - 1)]
    ref[pl.ds(pl.multiple_of(here, 8), 8), :] = jnp.where(over, tail[0], tail[1])


def norm_stats(x):
    mean = jnp.mean(x, axis=-1, keepdims=True)
    centred = x - mean
    inv = lax.rsqrt(jnp.mean(centred * centred, axis=-1, keepdims=True) + EPS)
    return centred * inv, inv


def norm_backward(grad, normed, inv, gain):
    e = grad * gain
    return inv * (
        e
        - jnp.mean(e, axis=-1, keepdims=True)
        - normed * jnp.mean(e * normed, axis=-1, keepdims=True)
    )


def row_sum(x):
    return jnp.sum(x, axis=0, keepdims=True)


THIRD = D // 2
HALF = FF // 2
NARROW = 640
NARROW_CUT = 384
OUT_PAD = 256
WIDE = OUT_PAD + 2 * HALF
WIDE_CUT = 896
MESH = pl.DeviceIdType.MESH
EVERY = slice(None)


def chip_grid(dp):
    side = math.isqrt(dp // 4)
    return 4, side, side


def place_of(dims):
    _, ny, nx = dims
    dp, mp = lax.axis_index("dp"), lax.axis_index("mp")
    return dp // (ny * nx), (dp // nx) % ny, dp % nx, mp


def peers_of(dims, place):
    (nz, ny, nx), (z, y, x, mp) = dims, place

    def at(a, b, c, m):
        return ((a * ny + b) * nx + c, m)

    along = {
        "z": [((z + o) % nz, at((z + o) % nz, y, x, mp)) for o in range(1, nz)],
        "y": [((y + o) % ny, at(z, (y + o) % ny, x, mp)) for o in range(1, ny)],
        "x": [((x + o) % nx, at(z, y, (x + o) % nx, mp)) for o in range(1, nx)],
    }
    return along, at(z, y, x, 1 - mp)


def greet(along, other):
    for device in [d for peers in along.values() for _, d in peers] + [other]:
        pl.semaphore_signal(
            pltpu.get_barrier_semaphore(), inc=1, device_id=device, device_id_type=MESH
        )


def met(along):
    count = sum(len(peers) for peers in along.values()) + 1
    pl.semaphore_wait(pltpu.get_barrier_semaphore(), count)


class Copies:
    def __init__(self, send, recv):
        self.send, self.recv, self.groups, self.count = send, recv, {}, 0

    def plan(self, name, makers):
        self.groups[name] = [(self.count + i, m) for i, m in enumerate(makers)]
        self.count += len(makers)

    def each(self, names):
        for name in names:
            for index, make in self.groups[name]:
                src, dst, device = make()
                yield pltpu.make_async_remote_copy(
                    src_ref=src, dst_ref=dst, send_sem=self.send.at[index],
                    recv_sem=self.recv.at[index], device_id=device, device_id_type=MESH,
                )

    def start(self, *names):
        for copy in self.each(names):
            copy.start()

    def arrived(self, *names):
        for copy in self.each(names):
            copy.wait_recv()

    def left(self, *names):
        for copy in self.each(names):
            copy.wait_send()


def plan_gather(copies, tag, w, own, cut, along, other, place):
    z, y, x, mp = place
    low, high = pl.ds(0, cut), pl.ds(cut, w.shape[-1] - cut)

    def same(index, device):
        return lambda: (w.at[index], w.at[index], device)

    def spread(index, axis):
        return [same(index, d) for _, d in along[axis]]

    def shares(indices):
        return [same(index, other) for index in indices]

    copies.plan(tag + "1", [lambda d=d: (own, w.at[mp, z, y, x], d) for _, d in along["z"]])
    copies.plan(tag + "2l", spread((mp, EVERY, y, x, EVERY, low), "y"))
    copies.plan(tag + "2h", spread((mp, EVERY, y, x, EVERY, high), "x"))
    copies.plan(tag + "3l", spread((mp, EVERY, EVERY, x, EVERY, low), "x"))
    copies.plan(tag + "3h", spread((mp, EVERY, y, EVERY, EVERY, high), "y"))
    copies.plan(tag + "s1", shares([(mp, EVERY, y, x)]))
    copies.plan(tag + "s2l", shares([(mp, EVERY, b, x, EVERY, low) for b, _ in along["y"]]))
    copies.plan(tag + "s2h", shares([(mp, EVERY, y, c, EVERY, high) for c, _ in along["x"]]))
    copies.plan(tag + "s3l", shares([(mp, EVERY, EVERY, c, EVERY, low) for c, _ in along["x"]]))
    copies.plan(tag + "s3h", shares([(mp, EVERY, b, EVERY, EVERY, high) for b, _ in along["y"]]))


def attn_fwd_kernel(dims, n, *refs):
    (wq, wk, wv, wot, wu, wdt), vectors, bup_in = refs[:6], refs[6:14], refs[14]
    tok_ref, cot_ref = refs[15:17]
    (
        qkv_ref, e_ref, mixed_ref, linv_ref, normed_ref, inv_ref, tokp_ref, cotp_ref, w_ref, vec_ref,
        bup_ref, wide,
    ) = refs[17:29]
    narrow, v, own, normed_all, inv_all, tok_all, cot_all, send, recv, sem = refs[29:]
    i = pl.program_id(0)
    steps = n // G
    nz, ny, nx = dims
    place = place_of(dims)
    z, y, x, mp = place
    rows = own.shape[0]
    along, other = peers_of(dims, place)
    copies = Copies(send, recv)
    plan_gather(copies, "n", narrow, narrow.at[mp, z, y, x], NARROW_CUT, along, other, place)
    plan_gather(copies, "w", wide, own, WIDE_CUT, along, other, place)

    def vec_spread(index, axis):
        return [lambda d=d: (v.at[index], v.at[index], d) for _, d in along[axis]]

    copies.plan("v1", vec_spread((z, y, x), "z"))
    copies.plan("v2", vec_spread((EVERY, y, x), "y"))
    copies.plan("v3", vec_spread((EVERY, EVERY, x), "x"))
    keep = pltpu.make_async_copy(own, wide.at[mp, z, y, x], sem)

    def norms(first, last):
        @pl.loop(first, last)
        def _(j):
            tok = load_image(tok_ref, j)
            normed, inv = norm_stats(tok)
            tok_all[j] = tok.astype(BF)
            cot_all[j] = load_image(cot_ref, j).astype(BF)
            normed_all[j] = normed
            inv_all[j] = jnp.broadcast_to(inv, (SP, 128))

    @pl.when(i == 0)
    def _():
        narrow[mp, z, y, x] = jnp.concatenate(
            [wq[...], wk[...], wv[...], jnp.zeros((rows, NARROW - 3 * THIRD), BF)], axis=1
        )
        own[...] = jnp.concatenate(
            [wot[...], jnp.zeros((rows, OUT_PAD - THIRD), BF), wu[...], wdt[...]], axis=1
        )
        v[z, y, x] = jnp.zeros((16, 128), F32)
        for j, vector in enumerate(vectors):
            v[z, y, x, j : j + 1, :rows] = vector[...].astype(F32)
        v[z, y, x, 8:9, : bup_in.shape[1]] = bup_in[...].astype(F32)
        greet(along, other)
        keep.start()
        norms(0, n // 4)
        met(along)
        copies.start("v1", "n1")
        norms(n // 4, n // 2)
        copies.arrived("v1", "n1")
        copies.start("v2", "n2l", "n2h", "w1", "ns1")
        norms(n // 2, (3 * n) // 4)
        copies.arrived("v2", "n2l", "n2h")
        copies.start("v3", "n3l", "n3h", "ns2l", "ns2h")
        norms((3 * n) // 4, n)
        copies.arrived("v3", "n3l")
        copies.start("ns3l")
        copies.arrived("n3h")
        copies.start("ns3h")
        keep.wait()
        copies.arrived("w1")
        copies.start("w2l", "w2h", "ws1")
        spots = [(a, b, c) for a in range(nz) for b in range(ny) for c in range(nx)]
        vec_ref[...] = jnp.concatenate([v[s][0:8, :rows] for s in spots], axis=1)
        bup_ref[...] = jnp.concatenate([v[s][8:9, : bup_in.shape[1]] for s in spots], axis=1)
        copies.arrived("ns1", "ns2l", "ns2h", "ns3l", "ns3h")
        group = 48 // rows
        for t in range(len(spots) // group):
            block = [
                jnp.concatenate(
                    [narrow[(m,) + s].astype(F32) for s in spots[t * group : (t + 1) * group]], axis=0
                )
                for m in range(2)
            ]
            for j in range(3):
                cols = slice(THIRD * j, THIRD * (j + 1))
                w_ref[48 * t : 48 * (t + 1), D * j : D * (j + 1)] = jnp.concatenate(
                    [half[:, cols] for half in block], axis=1
                ).astype(BF)

    @pl.when(i == 2)
    def _():
        copies.arrived("w2l", "w2h")
        copies.start("w3l", "w3h", "ws2l", "ws2h")

    images = pl.ds(G * i, G)
    normed = normed_all[images]
    normed_ref[...] = normed
    inv_ref[...] = inv_all[images]
    tokp_ref[...] = tok_all[images]
    cotp_ref[...] = cot_all[images]
    h1 = (normed * vec_ref[0:1, :] + vec_ref[1:2, :]).astype(BF).reshape(G * SP, D)
    q = ((dot_nn(h1, w_ref[:, 0:D]) + vec_ref[2:3, :]) * Q_SCALE).astype(BF)
    k = dot_nn(h1, w_ref[:, D : 2 * D]).astype(BF)
    value = (dot_nn(h1, w_ref[:, 2 * D :]) + vec_ref[3:4, :]).astype(BF)
    for j, x in enumerate((q, k, value)):
        for b in range(G):
            qkv_ref[b, :, D * j : D * (j + 1)] = x[SP * b : SP * (b + 1)]
    lane = lax.broadcasted_iota(jnp.int32, (SP, 2 * HD), 1)
    is_key = lax.broadcasted_iota(jnp.int32, (SP, SP), 1) < S
    zero = jnp.zeros((SP, 2 * HD), BF)
    one = jnp.ones((SP, 2 * HD), BF)
    for p in range(PAIRS):
        cols = slice(2 * HD * p, 2 * HD * (p + 1))
        for b in range(G):
            qp, kp, vp = (x[SP * b : SP * (b + 1), cols] for x in (q, k, value))
            total = None
            for h in range(2):
                mine = (lane < HD) if h == 0 else (lane >= HD)
                kh = jnp.where(mine, kp, zero)
                vh = jnp.where(mine, vp, zero)
                scores = dot_nt(qp, kh)
                scores = jnp.where(is_key, scores, -1e30)
                top = jnp.max(scores, axis=-1, keepdims=True)
                e = jnp.exp2(scores - top).astype(BF)
                e_ref[b, 2 * p + h] = e
                part = dot_nn(e, jnp.concatenate([vh, jnp.where(mine, one, zero)], axis=1))
                total = part if total is None else total + part
            linv = 1.0 / total[:, 2 * HD :]
            linv_ref[b, :, cols] = linv
            mixed_ref[b, :, cols] = (total[:, : 2 * HD] * linv).astype(BF)

    @pl.when(i == steps - 2)
    def _():
        copies.arrived("w3l", "w3h")
        copies.start("ws3l", "ws3h")

    @pl.when(i == steps - 1)
    def _():
        copies.arrived("ws1", "ws2l", "ws2h", "ws3l", "ws3h")
        copies.left(*copies.groups)


def attn_fwd(mats, vectors, bup, tokens, cot, dp):
    dims = chip_grid(dp)
    nz, ny, nx = dims
    rows = D // dp
    n = tokens.shape[0] // S
    count = 2 * (nz - 1 + 4 * (ny - 1) + 4 * (nx - 1) + 1) + nz + ny + nx - 3
    inputs = (*mats, *vectors, bup, tokens, cot)
    return pl.pallas_call(
        functools.partial(attn_fwd_kernel, dims, n),
        grid=(n // G,),
        in_specs=[whole(a.shape) for a in inputs],
        out_specs=[
            per_step(SP, 3 * D), per_step(HEADS, SP, SP), per_step(SP, D), per_step(SP, D),
            per_step(SP, D), per_step(SP, 128), per_step(SP, D), per_step(SP, D),
            whole((D, 3 * D)), whole((8, D)), whole((1, FF)), pl.BlockSpec(memory_space=pl.ANY),
        ],
        out_shape=[
            jax.ShapeDtypeStruct((n, SP, 3 * D), BF),
            jax.ShapeDtypeStruct((n, HEADS, SP, SP), BF),
            jax.ShapeDtypeStruct((n, SP, D), BF),
            jax.ShapeDtypeStruct((n, SP, D), F32),
            jax.ShapeDtypeStruct((n, SP, D), F32),
            jax.ShapeDtypeStruct((n, SP, 128), F32),
            jax.ShapeDtypeStruct((n, SP, D), BF),
            jax.ShapeDtypeStruct((n, SP, D), BF),
            jax.ShapeDtypeStruct((D, 3 * D), BF),
            jax.ShapeDtypeStruct((8, D), F32),
            jax.ShapeDtypeStruct((1, FF), F32),
            jax.ShapeDtypeStruct((2, nz, ny, nx, rows, WIDE), BF),
        ],
        scratch_shapes=[
            pltpu.VMEM((2, nz, ny, nx, rows, NARROW), BF),
            pltpu.VMEM((nz, ny, nx, 16, 128), F32),
            pltpu.VMEM((rows, WIDE), BF),
            pltpu.VMEM((n, SP, D), F32),
            pltpu.VMEM((n, SP, 128), F32),
            pltpu.VMEM((n, SP, D), BF),
            pltpu.VMEM((n, SP, D), BF),
            pltpu.SemaphoreType.DMA((count,)),
            pltpu.SemaphoreType.DMA((count,)),
            pltpu.SemaphoreType.DMA,
        ],
        compiler_params=params(collective_id=0),
        name="attn_fwd",
    )(*inputs)


def fold(x):
    return jnp.sum(x.reshape(x.shape[0] // 8, 8, x.shape[1]), axis=0)


CHUNK = 16


def mlp_kernel(
    dims, n, tok_ref, cot_ref, mixed_ref, w_ref, vec_ref, bup_ref,
    out_ref, gres_ref, gmix_ref, grads_ref, dvec_ref, dbup_ref,
    act_ref, gp_ref, wot_ref, dwot_ref, dwup_ref, dwdt_ref,
    h2_ref, h2t_ref, cott_ref, mix_ref, gr_ref, outf_ref, out_old, gh2_ref, cotf_ref, norm_ref,
    inv_ref, sums_ref, upsum_ref,
):
    i = pl.program_id(0)
    step = 256
    tiles = FF // step
    chunks = [slice(c, c + CHUNK) for c in range(0, SP, CHUNK)]

    @pl.when(i == 0)
    def _():
        wot_ref[...] = jnp.concatenate([w_ref[0, :, :THIRD], w_ref[1, :, :THIRD]], axis=1)
        for ref in (
            dwot_ref, dwup_ref, dwdt_ref, act_ref, gp_ref, h2t_ref, cott_ref, mix_ref, out_old,
            gh2_ref, cotf_ref, norm_ref, inv_ref, sums_ref, upsum_ref,
        ):
            ref[...] = jnp.zeros_like(ref)

    def weight_tile(j):
        cols = slice(step * j, step * (j + 1))
        dwup_ref[:, cols] += dot_nn(h2t_ref[...], gp_ref[:, cols])
        dwdt_ref[:, cols] += dot_nn(cott_ref[...], act_ref[:, cols])

    def finish(image, beside):
        beside(0)
        slot = image % 2
        for at in chunks:
            gh2, normed, cot = gh2_ref[at, :], norm_ref[at, :], cotf_ref[at, :]
            gres = cot + norm_backward(gh2, normed, inv_ref[at, 0:1], vec_ref[5:6, :])
            gres_ref[slot, at, :] = gres
            gr_ref[at, :] = gres.astype(BF)
            sums_ref[0] += fold(gres)
            sums_ref[1] += fold(gh2 * normed)
            sums_ref[2] += fold(gh2)
            sums_ref[3] += fold(cot)
        beside(1)
        gmix_ref[slot] = dot_nn(gr_ref[...], wot_ref[...]).astype(BF)
        beside(2)
        store_image(outf_ref, image, out_old[...])
        dwot_ref[...] += dot_tn(gr_ref[...], mix_ref[...])
        beside(3)

    finish(jnp.maximum(i - 1, 0), weight_tile)
    weight_tile(4)
    attended = dot_nt(mixed_ref[0], wot_ref[...])
    for at in chunks:
        cot = cot_ref[0, at, :].astype(F32)
        resid = tok_ref[0, at, :].astype(F32) + attended[at] + vec_ref[4:5, :]
        normed, inv = norm_stats(resid)
        h2_ref[at, :] = (normed * vec_ref[5:6, :] + vec_ref[6:7, :]).astype(BF)
        cotf_ref[at, :] = cot
        norm_ref[at, :] = normed
        inv_ref[at, :] = jnp.broadcast_to(inv, (CHUNK, 128))
        out_old[at, :] = resid + vec_ref[7:8, :]
    weight_tile(5)
    mix_ref[...] = mixed_ref[0]
    h2 = h2_ref[...]
    cot = cot_ref[0]
    h2t_ref[...] = h2.T
    cott_ref[...] = cot.T
    for j in range(tiles):
        cols = slice(step * j, step * (j + 1))
        m, at = divmod(step * j, HALF)
        u = dot_nn(h2, w_ref[m, :, OUT_PAD + at : OUT_PAD + at + step]) + bup_ref[:, cols]
        ga = dot_nn(cot, w_ref[m, :, OUT_PAD + HALF + at : OUT_PAD + HALF + at + step])
        cdf = 0.5 * (1.0 + lax.erf(u * RSQRT2))
        act_ref[:, cols] = (u * cdf).astype(BF)
        gp = ga * (cdf + u * jnp.exp(-0.5 * u * u) * RSQRT_TAU)
        upsum_ref[:, cols] += fold(gp)
        gp_ref[:, cols] = gp.astype(BF)
    out = out_old[...]
    gh2 = None
    for m in range(2):
        cols = slice(HALF * m, HALF * (m + 1))
        out = out + dot_nt(act_ref[:, cols], w_ref[m, :, OUT_PAD + HALF :])
        part = dot_nt(gp_ref[:, cols], w_ref[m, :, OUT_PAD : OUT_PAD + HALF])
        gh2 = part if gh2 is None else gh2 + part
    out_old[...] = out
    gh2_ref[...] = gh2

    @pl.when(i == n - 1)
    def _():
        finish(i, weight_tile)
        weight_tile(4)
        weight_tile(5)
        out_ref[...] = outf_ref[...].astype(BF)
        for k in range(4):
            dvec_ref[k : k + 1, :] = row_sum(sums_ref[k])
        dvec_ref[4:8, :] = jnp.zeros((4, D), F32)
        dbup_ref[...] = row_sum(upsum_ref[...])
        nz, ny, nx = dims
        rows = grads_ref.shape[4]
        spots = [(a, b, c) for a in range(nz) for b in range(ny) for c in range(nx)]
        group = 48 // rows
        for t in range(len(spots) // group):
            at = slice(48 * t, 48 * (t + 1))
            for m in range(2):
                parts = [
                    dwot_ref[at, THIRD * m : THIRD * (m + 1)],
                    jnp.zeros((48, OUT_PAD - THIRD), F32),
                    dwup_ref[at, HALF * m : HALF * (m + 1)],
                    dwdt_ref[at, HALF * m : HALF * (m + 1)],
                ]
                block = jnp.concatenate(parts, axis=1)
                for g in range(group):
                    grads_ref[(m,) + spots[t * group + g]] = block[
                        g * rows : (g + 1) * rows
                    ].astype(BF)


def mlp(tok, cot, mixed, wide, vec, bup, rows, dp):
    dims = chip_grid(dp)
    n = rows // S
    packed = (2, *dims, D // dp, WIDE)
    late = pl.BlockSpec((2, SP, D), lambda i: (jnp.maximum(i - 1, 0) // 2, 0, 0))
    return pl.pallas_call(
        functools.partial(mlp_kernel, dims, n),
        grid=(n,),
        in_specs=[
            per_image(SP, D), per_image(SP, D), per_image(SP, D), whole((2, D, WIDE)), whole((8, D)),
            whole((1, FF)),
        ],
        out_specs=[whole((rows, D)), late, late, whole(packed), whole((8, D)), whole((1, FF))],
        out_shape=[
            jax.ShapeDtypeStruct((rows, D), BF),
            jax.ShapeDtypeStruct((n, SP, D), F32),
            jax.ShapeDtypeStruct((n, SP, D), BF),
            jax.ShapeDtypeStruct(packed, BF),
            jax.ShapeDtypeStruct((8, D), F32),
            jax.ShapeDtypeStruct((1, FF), F32),
        ],
        scratch_shapes=[
            pltpu.VMEM((SP, FF), BF), pltpu.VMEM((SP, FF), BF), pltpu.VMEM((D, D), BF),
            pltpu.VMEM((D, D), F32), pltpu.VMEM((D, FF), F32), pltpu.VMEM((D, FF), F32),
            pltpu.VMEM((SP, D), BF), pltpu.VMEM((D, SP), BF), pltpu.VMEM((D, SP), BF),
            pltpu.VMEM((SP, D), BF), pltpu.VMEM((SP, D), BF), pltpu.VMEM((rows, D), F32),
            pltpu.VMEM((SP, D), F32), pltpu.VMEM((SP, D), F32), pltpu.VMEM((SP, D), F32),
            pltpu.VMEM((SP, D), F32), pltpu.VMEM((SP, 128), F32), pltpu.VMEM((4, 8, D), F32),
            pltpu.VMEM((8, FF), F32),
        ],
        compiler_params=params(),
        name="mlp",
    )(tok, cot, mixed, wide, vec, bup)


class Reduction:
    def __init__(self, dims, copies, tag, packed, bufs, cut):
        self.dims, self.copies, self.packed, self.cut = dims, copies, packed, cut
        self.place = place_of(dims)
        self.along, self.other = peers_of(dims, self.place)
        z, y, x, mp = self.place
        self.p, self.a1, self.b1, self.ra1, self.rb1, self.ra2, self.rb2, self.f, self.rz = bufs
        low, high = pl.ds(0, cut), pl.ds(cut, packed.shape[-1] - cut)
        along = self.along
        copies.plan(tag + "pair", [lambda: (packed.at[1 - mp], self.p, self.other)])
        copies.plan(tag + "1l", [
            lambda o=o, c=c, d=d: (self.p.at[EVERY, EVERY, c, EVERY, low], self.ra1.at[o], d)
            for o, (c, d) in enumerate(along["x"])
        ])
        copies.plan(tag + "1h", [
            lambda o=o, b=b, d=d: (self.p.at[EVERY, b, EVERY, EVERY, high], self.rb1.at[o], d)
            for o, (b, d) in enumerate(along["y"])
        ])
        copies.plan(tag + "2l", [
            lambda o=o, b=b, d=d: (self.a1.at[EVERY, b], self.ra2.at[o], d)
            for o, (b, d) in enumerate(along["y"])
        ])
        copies.plan(tag + "2h", [
            lambda o=o, c=c, d=d: (self.b1.at[EVERY, c], self.rb2.at[o], d)
            for o, (c, d) in enumerate(along["x"])
        ])
        copies.plan(tag + "3", [
            lambda o=o, a=a, d=d: (self.f.at[a], self.rz.at[o], d)
            for o, (a, d) in enumerate(along["z"])
        ])

    @staticmethod
    def count(dims):
        nz, ny, nx = dims
        return 1 + 2 * (ny - 1) + 2 * (nx - 1) + nz - 1

    @staticmethod
    def scratch(dims, rows, width, cut):
        nz, ny, nx = dims

        def buf(w, *shape):
            return pltpu.VMEM((*shape, rows, w), BF)

        rest = width - cut
        return [
            buf(width, nz, ny, nx), buf(cut, nz, ny), buf(rest, nz, nx),
            buf(cut, nx - 1, nz, ny), buf(rest, ny - 1, nz, nx),
            buf(cut, ny - 1, nz), buf(rest, nx - 1, nz), buf(width, nz), buf(width, nz - 1),
        ]

    def add_pair(self, mine):
        nz, ny, nx = self.dims
        for i in range(nz):
            for j in range(ny):
                for k in range(nx):
                    total = mine[i, j, k].astype(F32) + self.p[i, j, k].astype(F32)
                    self.p[i, j, k] = total.astype(BF)

    def add_first_low(self):
        nz, ny, nx = self.dims
        x = self.place[2]
        for i in range(nz):
            for j in range(ny):
                total = self.p[i, j, x, :, : self.cut].astype(F32)
                for o in range(nx - 1):
                    total = total + self.ra1[o, i, j].astype(F32)
                self.a1[i, j] = total.astype(BF)

    def add_first_high(self):
        nz, ny, nx = self.dims
        y = self.place[1]
        for i in range(nz):
            for k in range(nx):
                total = self.p[i, y, k, :, self.cut :].astype(F32)
                for o in range(ny - 1):
                    total = total + self.rb1[o, i, k].astype(F32)
                self.b1[i, k] = total.astype(BF)

    def add_second(self):
        nz, ny, nx = self.dims
        _, y, x, _ = self.place
        for i in range(nz):
            total = self.a1[i, y].astype(F32)
            for o in range(ny - 1):
                total = total + self.ra2[o, i].astype(F32)
            self.f[i, :, : self.cut] = total.astype(BF)
            total = self.b1[i, x].astype(F32)
            for o in range(nx - 1):
                total = total + self.rb2[o, i].astype(F32)
            self.f[i, :, self.cut :] = total.astype(BF)

    def add_third(self):
        total = self.f[self.place[0]].astype(F32)
        for o in range(self.dims[0] - 1):
            total = total + self.rz[o].astype(F32)
        return total


def backward_kernel(
    dims, n, qkv_ref, e_ref, mixed_ref, linv_ref, gmix_ref, normed_ref, inv_ref, gres_ref, w_ref,
    vec_ref, dvec2_ref, dbup_ref, packed, gtok_ref, narrow_ref, wide_ref, total_ref, *refs,
):
    g_ref, acc_ref, gsum_ref, narrow, sums, vs, vr = refs[:7]
    wide_bufs, mine, narrow_bufs = refs[7:16], refs[16], refs[17:26]
    send, recv, sem = refs[26:]
    i = pl.program_id(0)
    steps = n // G
    copies = Copies(send, recv)
    wide = Reduction(dims, copies, "w", packed, wide_bufs, WIDE_CUT)
    thin = Reduction(dims, copies, "n", narrow, narrow_bufs, NARROW_CUT)
    mp = wide.place[3]
    keep = pltpu.make_async_copy(packed.at[mp], mine, sem)
    stages = [[wide.other], *([d for _, d in wide.along[axis]] for axis in "xyz")]
    bases = [sum(len(s) for s in stages[:k]) for k in range(4)]
    for k, devices in enumerate(stages):
        copies.plan("v%d" % k, [
            lambda k=k, o=o, d=d: (sums if k == 0 else vs.at[k - 1], vr.at[bases[k] + o], d)
            for o, d in enumerate(devices)
        ])

    def vec_add(k):
        total = sums[...] if k == 0 else vs[k - 1]
        for o in range(len(stages[k])):
            total = total + vr[bases[k] + o]
        if k < 3:
            vs[k] = total
        else:
            total_ref[...] = total

    @pl.when(i == 0)
    def _():
        greet(wide.along, wide.other)
        keep.start()
        acc_ref[...] = jnp.zeros_like(acc_ref)
        gsum_ref[...] = jnp.zeros_like(gsum_ref)
        met(wide.along)
        copies.start("wpair")

    @pl.when(i == 1)
    def _():
        keep.wait()
        copies.arrived("wpair")
        wide.add_pair(mine)
        copies.start("w1l", "w1h")

    @pl.when(i == steps // 2)
    def _():
        copies.arrived("w1l", "w1h")
        wide.add_first_low()
        wide.add_first_high()
        copies.start("w2l", "w2h")

    @pl.when(i == (3 * steps) // 4)
    def _():
        copies.arrived("w2l", "w2h")
        wide.add_second()
        copies.start("w3")

    @pl.when(i < steps)
    def _():
        lane = lax.broadcasted_iota(jnp.int32, (SP, 2 * HD), 1)
        zero = jnp.zeros((SP, 2 * HD), BF)
        minus = jnp.full((SP, 2 * HD), -1.0, BF)
        for p in range(PAIRS):
            lo, hi = 2 * HD * p, 2 * HD * (p + 1)
            for b in range(G):
                q = qkv_ref[b, :, lo:hi]
                k = qkv_ref[b, :, D + lo : D + hi]
                v = qkv_ref[b, :, 2 * D + lo : 2 * D + hi]
                go_f = gmix_ref[b, :, lo:hi].astype(F32) * linv_ref[b, :, lo:hi]
                go = go_f.astype(BF)
                god = jnp.concatenate(
                    [go, (go_f * mixed_ref[b, :, lo:hi].astype(F32)).astype(BF)], axis=1
                )
                gq = gk = gv = None
                for h in range(2):
                    own = (lane < HD) if h == 0 else (lane >= HD)
                    e = e_ref[b, 2 * p + h]
                    vd = jnp.concatenate(
                        [jnp.where(own, v, zero), jnp.where(own, minus, zero)], axis=1
                    )
                    ds = e * dot_nt(god, vd).astype(BF)
                    part_q = dot_nn(ds, jnp.where(own, k, zero))
                    part_k = dot_tn(ds, jnp.where(own, q, zero))
                    part_v = dot_tn(e, jnp.where(own, go, zero))
                    gq = part_q if gq is None else gq + part_q
                    gk = part_k if gk is None else gk + part_k
                    gv = part_v if gv is None else gv + part_v
                gq = gq * (1.0 / math.sqrt(HD))
                gk = gk * (1.0 / LOG2E)
                for j, grad in enumerate((gq, gk, gv)):
                    gsum_ref[:, D * j + lo : D * j + hi] += fold(grad)
                    g_ref[i, SP * b : SP * (b + 1), D * j + lo : D * j + hi] = grad.astype(BF)
        acc_ref[...] += dot_tn(normed_ref[...].reshape(G * SP, D).astype(BF), g_ref[i])

    @pl.when(i == steps - 1)
    def _():
        nz, ny, nx = dims
        rows = narrow.shape[4]
        spots = [(a, b, c) for a in range(nz) for b in range(ny) for c in range(nx)]
        group = 48 // rows
        turned = vec_ref[...].T
        gsum = row_sum(gsum_ref[...])
        gains = []
        for t in range(len(spots) // group):
            at = slice(48 * t, 48 * (t + 1))
            acc = acc_ref[at, :]
            gains.append(jnp.sum(acc * w_ref[at, :].astype(F32), axis=1, keepdims=True))
            dw = acc * turned[at, 0:1] + turned[at, 1:2] * gsum
            for m in range(2):
                parts = [dw[:, D * j + THIRD * m : D * j + THIRD * (m + 1)] for j in range(3)]
                parts.append(jnp.zeros((48, NARROW - 3 * THIRD), F32))
                block = jnp.concatenate(parts, axis=1)
                for k in range(group):
                    narrow[(m,) + spots[t * group + k]] = block[
                        k * rows : (k + 1) * rows
                    ].astype(BF)
        high = gsum.astype(BF)
        low = (gsum - high.astype(F32)).astype(BF)
        row = lax.broadcasted_iota(jnp.int32, (16, 3 * D), 0)
        both = jnp.where(row == 0, high, jnp.where(row == 1, low, jnp.zeros((16, 3 * D), BF)))
        sums[0:1] = gsum[:, :D]
        sums[1:2] = gsum[:, 2 * D :]
        gain = jnp.broadcast_to(jnp.concatenate(gains, axis=0), (D, 128)).T
        sums[2:3] = gain[0:1, :]
        sums[3:4] = row_sum(dot_nt(both, w_ref[...]))
        sums[4:8] = dvec2_ref[0:4]
        for j in range(FF // D):
            sums[8 + j : 9 + j] = dbup_ref[:, D * j : D * (j + 1)]
        sums[12:16] = jnp.zeros((4, D), F32)
        copies.start("npair", "v0")

    @pl.when(i == steps + 2)
    def _():
        copies.arrived("npair", "v0")
        thin.add_pair(narrow.at[mp])
        vec_add(0)
        copies.start("n1l", "n1h", "v1")

    @pl.when(i == steps + 3)
    def _():
        copies.arrived("w3")
        wide_ref[...] = wide.add_third()

    @pl.when(i == steps + 4)
    def _():
        copies.arrived("n1l", "v1")
        thin.add_first_low()
        vec_add(1)
        copies.start("n2l", "v2")
        copies.arrived("n1h")
        thin.add_first_high()
        copies.start("n2h")

    @pl.when(i == steps + 6)
    def _():
        copies.arrived("n2l", "n2h", "v2")
        thin.add_second()
        vec_add(2)
        copies.start("n3", "v3")

    @pl.when(i >= steps)
    def _():
        group = jnp.maximum(i - steps, 0)
        gh1 = dot_nt(g_ref[group], w_ref[...])
        for b in range(G):
            parts = []
            for c in range(0, SP, CHUNK):
                at = slice(c, c + CHUNK)
                back = norm_backward(
                    gh1[SP * b + c : SP * b + c + CHUNK], normed_ref[b, at, :],
                    inv_ref[b, at, 0:1], vec_ref[0:1, :],
                )
                parts.append(gres_ref[b, at, :] + back)
            store_image(gtok_ref, G * group + b, jnp.concatenate(parts, axis=0))

    @pl.when(i == 2 * steps - 1)
    def _():
        copies.arrived("n3", "v3")
        narrow_ref[...] = thin.add_third()
        vec_add(3)
        copies.left(*copies.groups)


def backward(qkv, e, mixed, linv, gmix, normed, inv, gres, wqkv, vec, dvec2, dbup, packed, tall, dp):
    dims = chip_grid(dp)
    nz, ny, nx = dims
    n = qkv.shape[0]
    steps = n // G
    rows = D // dp
    count = 2 * Reduction.count(dims) + nz + ny + nx - 2

    def heads(*shape):
        return pl.BlockSpec((G, *shape), lambda i: (jnp.minimum(i, steps - 1),) + (0,) * len(shape))

    def after(*shape):
        return pl.BlockSpec((G, *shape), lambda i: (jnp.maximum(i - steps, 0),) + (0,) * len(shape))

    def twice(*shape):
        return pl.BlockSpec((G, *shape), lambda i: (i % steps,) + (0,) * len(shape))

    return pl.pallas_call(
        functools.partial(backward_kernel, dims, n),
        grid=(2 * steps,),
        in_specs=[
            heads(SP, 3 * D), heads(HEADS, SP, SP), heads(SP, D), heads(SP, D), heads(SP, D),
            twice(SP, D), after(SP, 128), after(SP, D), whole((D, 3 * D)), whole((8, D)),
            whole((8, D)), whole((1, FF)), pl.BlockSpec(memory_space=pl.ANY),
        ],
        out_specs=[
            whole((tall, D)), whole((rows, NARROW)), whole((rows, WIDE)), whole((16, D)),
        ],
        out_shape=[
            jax.ShapeDtypeStruct((tall, D), F32),
            jax.ShapeDtypeStruct((rows, NARROW), F32),
            jax.ShapeDtypeStruct((rows, WIDE), F32),
            jax.ShapeDtypeStruct((16, D), F32),
        ],
        scratch_shapes=[
            pltpu.VMEM((steps, G * SP, 3 * D), BF),
            pltpu.VMEM((D, 3 * D), F32),
            pltpu.VMEM((8, 3 * D), F32),
            pltpu.VMEM((2, *dims, rows, NARROW), BF),
            pltpu.VMEM((16, D), F32),
            pltpu.VMEM((3, 16, D), F32),
            pltpu.VMEM((nz + ny + nx - 2, 16, D), F32),
            *Reduction.scratch(dims, rows, WIDE, WIDE_CUT),
            pltpu.VMEM((*dims, rows, WIDE), BF),
            *Reduction.scratch(dims, rows, NARROW, NARROW_CUT),
            pltpu.SemaphoreType.DMA((count,)),
            pltpu.SemaphoreType.DMA((count,)),
            pltpu.SemaphoreType.DMA,
        ],
        compiler_params=params(collective_id=1),
        name="backward",
    )(qkv, e, mixed, linv, gmix, normed, inv, gres, wqkv, vec, dvec2, dbup, packed)


def split_kernel(n, narrow_ref, wide_ref, vec_ref, *outs):
    for j in range(3):
        outs[j][...] = narrow_ref[:, THIRD * j : THIRD * (j + 1)]
    outs[3][...] = wide_ref[:, :THIRD]
    outs[4][...] = wide_ref[:, OUT_PAD : OUT_PAD + HALF]
    outs[5][...] = wide_ref[:, OUT_PAD + HALF :]
    index = lax.axis_index("dp") * 2 + lax.axis_index("mp")
    per = D // n
    vec = pltpu.roll(vec_ref[...], D - index * per, axis=1)
    for row, out in zip((2, 3, 0, 1, 4, 5, 6, 7), outs[6:]):
        out[...] = vec[row : row + 1, :per]
    wide = jnp.concatenate([vec_ref[8 + j : 9 + j, :] for j in range(FF // D)], axis=1)
    wide = pltpu.roll(jnp.broadcast_to(wide, (8, FF)), FF - index * (FF // n), axis=1)
    outs[14][...] = wide[0:1, : FF // n]


def split(narrow, wide, vec, n):
    rows = narrow.shape[0]
    vmem = pl.BlockSpec(memory_space=pltpu.VMEM)
    shapes = [(rows, THIRD)] * 4 + [(rows, HALF)] * 2 + [(1, D // n)] * 8 + [(1, FF // n)]
    return pl.pallas_call(
        functools.partial(split_kernel, n),
        in_specs=[vmem] * 3,
        out_specs=[vmem] * 15,
        out_shape=[jax.ShapeDtypeStruct(s, F32) for s in shapes],
        name="split",
    )(narrow, wide, vec)


def whole(shape):
    return pl.BlockSpec(shape, lambda i: (0,) * len(shape))


def per_image(*shape):
    return pl.BlockSpec((1, *shape), lambda i: (i,) + (0,) * len(shape))


def per_step(*shape):
    return pl.BlockSpec((G, *shape), lambda i: (i,) + (0,) * len(shape))


def params(collective_id=None):
    return pltpu.CompilerParams(
        dimension_semantics=("arbitrary",), vmem_limit_bytes=62 * 1024 * 1024,
        collective_id=collective_id, has_side_effects=collective_id is not None,
    )


def on_device(
    tokens, w_query, w_key, w_value, w_out, w_up, w_down, ln1_gain, ln1_bias, b_query, b_value,
    b_out, ln2_gain, ln2_bias, b_up, b_down, cotangent,
):
    dp = lax.axis_size("dp")
    vectors = (ln1_gain, ln1_bias, b_query, b_value, b_out, ln2_gain, ln2_bias, b_down)
    qkv, e, mixed, linv, normed, inv, tok, cot, wqkv, vec, bup, wide = attn_fwd(
        (w_query, w_key, w_value, w_out.T, w_up, w_down.T), [v[None] for v in vectors], b_up[None],
        tokens, cotangent, dp,
    )
    out, gres, gmix, packed, dvec2, dbup = mlp(
        tok, cot, mixed, wide.reshape(2, D, WIDE), vec, bup, tokens.shape[0], dp
    )
    gtok, narrow_sum, wide_sum, sums = backward(
        qkv, e, mixed, linv, gmix, normed, inv, gres, wqkv, vec, dvec2, dbup, packed,
        tokens.shape[0], dp,
    )
    grads = split(narrow_sum, wide_sum, sums, dp * lax.axis_size("mp"))
    vecs = [v.reshape(-1) for v in grads[6:]]
    return (
        out, gtok, grads[0], grads[1], grads[2], grads[3].T, grads[4], grads[5].T,
        *vecs[:7], vecs[8], vecs[7],
    )


def solution(mesh):
    row, mat, tam, vec = P(("dp", "mp"), None), P("dp", "mp"), P("mp", "dp"), P("dp")
    part = P(("dp", "mp"))
    return jax.shard_map(
        on_device,
        mesh=mesh,
        in_specs=(row, mat, mat, mat, tam, mat, tam, *([vec] * 9), row),
        out_specs=(row, row, mat, mat, mat, tam, mat, tam, *([part] * 9)),
        check_vma=False,
    )
```

```python
import functools
import math

import jax
import jax.numpy as jnp
from jax import lax
from jax.experimental import pallas as pl
from jax.experimental.pallas import tpu as pltpu
from jax.sharding import PartitionSpec as P

D = 384
HD = 64
FF = 1536
S = 197
HEADS = D // HD
PAIRS = HEADS // 2

SP = 208
WIN = 224
G = 2

EPS = 1e-06
RSQRT2 = 0.7071067811865476
RSQRT_TAU = 0.3989422804014327
LOG2E = 1.4426950408889634
Q_SCALE = LOG2E / math.sqrt(HD)
BF = jnp.bfloat16
F32 = jnp.float32


def dot_nn(a, b):
    return lax.dot_general(a, b, (((1,), (0,)), ((), ())), preferred_element_type=F32)


def dot_nt(a, b):
    return lax.dot_general(a, b, (((1,), (1,)), ((), ())), preferred_element_type=F32)


def dot_tn(a, b):
    return lax.dot_general(a, b, (((0,), (0,)), ((), ())), preferred_element_type=F32)


def window_of(i, rows):
    start = i * S
    base = jnp.minimum((start // 16) * 16, rows - WIN)
    return pl.multiple_of(base, 16), start - base


def load_image(ref, i):
    base, off = window_of(i, ref.shape[0])
    rows = ref[pl.ds(base, WIN), :].astype(F32)
    rows = pltpu.roll(rows, WIN - off, axis=0)[:SP]
    live = lax.broadcasted_iota(jnp.int32, rows.shape, 0) < S
    return jnp.where(live, rows, 0.0)


def store_image(ref, i, rows):
    start = i * S
    r = start % 8
    base = start - r
    total = ref.shape[0]
    groups = SP // 8
    turned = pltpu.roll(rows.reshape(groups, 8, D), r, axis=1)
    first = lax.broadcasted_iota(jnp.int32, (8, D), 0) < r
    old = ref[pl.ds(pl.multiple_of(base, 8), 8), :]
    ref[pl.ds(pl.multiple_of(base, 8), 8), :] = jnp.where(first, old, turned[0])
    for g in range(1, groups - 1):
        ref[pl.ds(pl.multiple_of(base + 8 * g, 8), 8), :] = jnp.where(
            first, turned[g - 1], turned[g]
        )
    over = base + SP > total
    here = jnp.where(over, total - 8, base + SP - 8)
    tail = [jnp.where(first, turned[g - 1], turned[g]) for g in (groups - 2, groups - 1)]
    ref[pl.ds(pl.multiple_of(here, 8), 8), :] = jnp.where(over, tail[0], tail[1])


def norm_stats(x):
    mean = jnp.mean(x, axis=-1, keepdims=True)
    centred = x - mean
    inv = lax.rsqrt(jnp.mean(centred * centred, axis=-1, keepdims=True) + EPS)
    return centred * inv, inv


def norm_backward(grad, normed, inv, gain):
    e = grad * gain
    return inv * (
        e
        - jnp.mean(e, axis=-1, keepdims=True)
        - normed * jnp.mean(e * normed, axis=-1, keepdims=True)
    )


def row_sum(x):
    return jnp.sum(x, axis=0, keepdims=True)


THIRD = D // 2
HALF = FF // 2
NARROW = 640
NARROW_CUT = 384
OUT_PAD = 256
WIDE = OUT_PAD + 2 * HALF
WIDE_CUT = 896
MESH = pl.DeviceIdType.MESH
EVERY = slice(None)


def chip_grid(dp):
    side = math.isqrt(dp // 4)
    return 4, side, side


def place_of(dims):
    _, ny, nx = dims
    dp, mp = lax.axis_index("dp"), lax.axis_index("mp")
    return dp // (ny * nx), (dp // nx) % ny, dp % nx, mp


def peers_of(dims, place):
    (nz, ny, nx), (z, y, x, mp) = dims, place

    def at(a, b, c, m):
        return ((a * ny + b) * nx + c, m)

    along = {
        "z": [((z + o) % nz, at((z + o) % nz, y, x, mp)) for o in range(1, nz)],
        "y": [((y + o) % ny, at(z, (y + o) % ny, x, mp)) for o in range(1, ny)],
        "x": [((x + o) % nx, at(z, y, (x + o) % nx, mp)) for o in range(1, nx)],
    }
    return along, at(z, y, x, 1 - mp)


def greet(along, other):
    for device in [d for peers in along.values() for _, d in peers] + [other]:
        pl.semaphore_signal(
            pltpu.get_barrier_semaphore(), inc=1, device_id=device, device_id_type=MESH
        )


def met(along):
    count = sum(len(peers) for peers in along.values()) + 1
    pl.semaphore_wait(pltpu.get_barrier_semaphore(), count)


class Copies:
    def __init__(self, send, recv):
        self.send, self.recv, self.groups, self.count = send, recv, {}, 0

    def plan(self, name, makers):
        self.groups[name] = [(self.count + i, m) for i, m in enumerate(makers)]
        self.count += len(makers)

    def each(self, names):
        for name in names:
            for index, make in self.groups[name]:
                src, dst, device = make()
                yield pltpu.make_async_remote_copy(
                    src_ref=src, dst_ref=dst, send_sem=self.send.at[index],
                    recv_sem=self.recv.at[index], device_id=device, device_id_type=MESH,
                )

    def start(self, *names):
        for copy in self.each(names):
            copy.start()

    def arrived(self, *names):
        for copy in self.each(names):
            copy.wait_recv()

    def left(self, *names):
        for copy in self.each(names):
            copy.wait_send()


def plan_gather(copies, tag, w, own, cut, along, other, place):
    z, y, x, mp = place
    low, high = pl.ds(0, cut), pl.ds(cut, w.shape[-1] - cut)

    def same(index, device):
        return lambda: (w.at[index], w.at[index], device)

    def spread(index, axis):
        return [same(index, d) for _, d in along[axis]]

    def shares(indices):
        return [same(index, other) for index in indices]

    copies.plan(tag + "1", [lambda d=d: (own, w.at[mp, z, y, x], d) for _, d in along["z"]])
    copies.plan(tag + "2l", spread((mp, EVERY, y, x, EVERY, low), "y"))
    copies.plan(tag + "2h", spread((mp, EVERY, y, x, EVERY, high), "x"))
    copies.plan(tag + "3l", spread((mp, EVERY, EVERY, x, EVERY, low), "x"))
    copies.plan(tag + "3h", spread((mp, EVERY, y, EVERY, EVERY, high), "y"))
    copies.plan(tag + "s1", shares([(mp, EVERY, y, x)]))
    copies.plan(tag + "s2l", shares([(mp, EVERY, b, x, EVERY, low) for b, _ in along["y"]]))
    copies.plan(tag + "s2h", shares([(mp, EVERY, y, c, EVERY, high) for c, _ in along["x"]]))
    copies.plan(tag + "s3l", shares([(mp, EVERY, EVERY, c, EVERY, low) for c, _ in along["x"]]))
    copies.plan(tag + "s3h", shares([(mp, EVERY, b, EVERY, EVERY, high) for b, _ in along["y"]]))


def attn_fwd_kernel(dims, n, *refs):
    (wq, wk, wv, wot, wu, wdt), vectors, bup_in = refs[:6], refs[6:14], refs[14]
    tok_hbm, cot_hbm = refs[15:17]
    (
        qkv_ref, e_ref, mixed_ref, linv_ref, normed_ref, inv_ref, tokp_ref, cotp_ref, w_ref, vec_ref,
        bup_ref, wide,
    ) = refs[17:29]
    narrow, v, own, normed_all, inv_all, tok_all, cot_all, tok_ref, cot_ref, send, recv, sem = refs[29:]
    i = pl.program_id(0)
    steps = n // G
    nz, ny, nx = dims
    place = place_of(dims)
    z, y, x, mp = place
    rows = own.shape[0]
    along, other = peers_of(dims, place)
    copies = Copies(send, recv)
    plan_gather(copies, "n", narrow, narrow.at[mp, z, y, x], NARROW_CUT, along, other, place)
    plan_gather(copies, "w", wide, own, WIDE_CUT, along, other, place)

    def vec_spread(index, axis):
        return [lambda d=d: (v.at[index], v.at[index], d) for _, d in along[axis]]

    copies.plan("v1", vec_spread((z, y, x), "z"))
    copies.plan("v2", vec_spread((EVERY, y, x), "y"))
    copies.plan("v3", vec_spread((EVERY, EVERY, x), "x"))
    keep = pltpu.make_async_copy(own, wide.at[mp, z, y, x], sem.at[0])
    fetch = [
        pltpu.make_async_copy(tok_hbm, tok_ref, sem.at[1]),
        pltpu.make_async_copy(cot_hbm, cot_ref, sem.at[2]),
    ]

    def norms(first, last):
        @pl.loop(first, last)
        def _(j):
            tok = load_image(tok_ref, j)
            normed, inv = norm_stats(tok)
            tok_all[j] = tok.astype(BF)
            cot_all[j] = load_image(cot_ref, j).astype(BF)
            normed_all[j] = normed
            inv_all[j] = jnp.broadcast_to(inv, (SP, 128))

    @pl.when(i == 0)
    def _():
        for copy in fetch:
            copy.start()
        narrow[mp, z, y, x] = jnp.concatenate(
            [wq[...], wk[...], wv[...], jnp.zeros((rows, NARROW - 3 * THIRD), BF)], axis=1
        )
        own[...] = jnp.concatenate(
            [wot[...], jnp.zeros((rows, OUT_PAD - THIRD), BF), wu[...], wdt[...]], axis=1
        )
        v[z, y, x] = jnp.zeros((16, 128), F32)
        for j, vector in enumerate(vectors):
            v[z, y, x, j : j + 1, :rows] = vector[...].astype(F32)
        v[z, y, x, 8:9, : bup_in.shape[1]] = bup_in[...].astype(F32)
        greet(along, other)
        keep.start()
        for copy in fetch:
            copy.wait()
        norms(0, n // 4)
        met(along)
        copies.start("v1", "n1")
        norms(n // 4, n // 2)
        copies.arrived("v1", "n1")
        copies.start("v2", "n2l", "n2h", "w1", "ns1")
        norms(n // 2, (3 * n) // 4)
        copies.arrived("v2", "n2l", "n2h")
        copies.start("v3", "n3l", "n3h", "ns2l", "ns2h")
        norms((3 * n) // 4, n)
        copies.arrived("v3", "n3l")
        copies.start("ns3l")
        copies.arrived("n3h")
        copies.start("ns3h")
        keep.wait()
        copies.arrived("w1")
        copies.start("w2l", "w2h", "ws1")
        spots = [(a, b, c) for a in range(nz) for b in range(ny) for c in range(nx)]
        vec_ref[...] = jnp.concatenate([v[s][0:8, :rows] for s in spots], axis=1)
        bup_ref[...] = jnp.concatenate([v[s][8:9, : bup_in.shape[1]] for s in spots], axis=1)
        copies.arrived("ns1", "ns2l", "ns2h", "ns3l", "ns3h")
        group = 48 // rows
        for t in range(len(spots) // group):
            block = [
                jnp.concatenate(
                    [narrow[(m,) + s].astype(F32) for s in spots[t * group : (t + 1) * group]], axis=0
                )
                for m in range(2)
            ]
            for j in range(3):
                cols = slice(THIRD * j, THIRD * (j + 1))
                w_ref[48 * t : 48 * (t + 1), D * j : D * (j + 1)] = jnp.concatenate(
                    [half[:, cols] for half in block], axis=1
                ).astype(BF)

    @pl.when(i == 2)
    def _():
        copies.arrived("w2l", "w2h")
        copies.start("w3l", "w3h", "ws2l", "ws2h")

    images = pl.ds(G * i, G)
    normed = normed_all[images]
    normed_ref[...] = normed
    inv_ref[...] = inv_all[images]
    tokp_ref[...] = tok_all[images]
    cotp_ref[...] = cot_all[images]
    h1 = (normed * vec_ref[0:1, :] + vec_ref[1:2, :]).astype(BF).reshape(G * SP, D)
    q = ((dot_nn(h1, w_ref[:, 0:D]) + vec_ref[2:3, :]) * Q_SCALE).astype(BF)
    k = dot_nn(h1, w_ref[:, D : 2 * D]).astype(BF)
    value = (dot_nn(h1, w_ref[:, 2 * D :]) + vec_ref[3:4, :]).astype(BF)
    for j, x in enumerate((q, k, value)):
        for b in range(G):
            qkv_ref[b, :, D * j : D * (j + 1)] = x[SP * b : SP * (b + 1)]
    lane = lax.broadcasted_iota(jnp.int32, (SP, 2 * HD), 1)
    is_key = lax.broadcasted_iota(jnp.int32, (SP, SP), 1) < S
    zero = jnp.zeros((SP, 2 * HD), BF)
    one = jnp.ones((SP, 2 * HD), BF)
    for p in range(PAIRS):
        cols = slice(2 * HD * p, 2 * HD * (p + 1))
        for b in range(G):
            qp, kp, vp = (x[SP * b : SP * (b + 1), cols] for x in (q, k, value))
            total = None
            for h in range(2):
                mine = (lane < HD) if h == 0 else (lane >= HD)
                kh = jnp.where(mine, kp, zero)
                vh = jnp.where(mine, vp, zero)
                scores = dot_nt(qp, kh)
                scores = jnp.where(is_key, scores, -1e30)
                top = jnp.max(scores, axis=-1, keepdims=True)
                e = jnp.exp2(scores - top).astype(BF)
                e_ref[b, 2 * p + h] = e
                part = dot_nn(e, jnp.concatenate([vh, jnp.where(mine, one, zero)], axis=1))
                total = part if total is None else total + part
            linv = 1.0 / total[:, 2 * HD :]
            linv_ref[b, :, cols] = linv
            mixed_ref[b, :, cols] = (total[:, : 2 * HD] * linv).astype(BF)

    @pl.when(i == steps - 2)
    def _():
        copies.arrived("w3l", "w3h")
        copies.start("ws3l", "ws3h")

    @pl.when(i == steps - 1)
    def _():
        copies.arrived("ws1", "ws2l", "ws2h", "ws3l", "ws3h")
        copies.left(*copies.groups)


def attn_fwd(mats, vectors, bup, tokens, cot, dp):
    dims = chip_grid(dp)
    nz, ny, nx = dims
    rows = D // dp
    n = tokens.shape[0] // S
    count = 2 * (nz - 1 + 4 * (ny - 1) + 4 * (nx - 1) + 1) + nz + ny + nx - 3
    inputs = (*mats, *vectors, bup, tokens, cot)
    return pl.pallas_call(
        functools.partial(attn_fwd_kernel, dims, n),
        grid=(n // G,),
        in_specs=[whole(a.shape) for a in inputs[:-2]] + [pl.BlockSpec(memory_space=pl.ANY)] * 2,
        out_specs=[
            per_step(SP, 3 * D), per_step(HEADS, SP, SP), per_step(SP, D), per_step(SP, D),
            per_step(SP, D), per_step(SP, 128), per_step(SP, D), per_step(SP, D),
            whole((D, 3 * D)), whole((8, D)), whole((1, FF)), pl.BlockSpec(memory_space=pl.ANY),
        ],
        out_shape=[
            jax.ShapeDtypeStruct((n, SP, 3 * D), BF),
            jax.ShapeDtypeStruct((n, HEADS, SP, SP), BF),
            jax.ShapeDtypeStruct((n, SP, D), BF),
            jax.ShapeDtypeStruct((n, SP, D), F32),
            jax.ShapeDtypeStruct((n, SP, D), F32),
            jax.ShapeDtypeStruct((n, SP, 128), F32),
            jax.ShapeDtypeStruct((n, SP, D), BF),
            jax.ShapeDtypeStruct((n, SP, D), BF),
            jax.ShapeDtypeStruct((D, 3 * D), BF),
            jax.ShapeDtypeStruct((8, D), F32),
            jax.ShapeDtypeStruct((1, FF), F32),
            jax.ShapeDtypeStruct((2, nz, ny, nx, rows, WIDE), BF),
        ],
        scratch_shapes=[
            pltpu.VMEM((2, nz, ny, nx, rows, NARROW), BF),
            pltpu.VMEM((nz, ny, nx, 16, 128), F32),
            pltpu.VMEM((rows, WIDE), BF),
            pltpu.VMEM((n, SP, D), F32),
            pltpu.VMEM((n, SP, 128), F32),
            pltpu.VMEM((n, SP, D), BF),
            pltpu.VMEM((n, SP, D), BF),
            pltpu.VMEM(tokens.shape, BF),
            pltpu.VMEM(tokens.shape, BF),
            pltpu.SemaphoreType.DMA((count,)),
            pltpu.SemaphoreType.DMA((count,)),
            pltpu.SemaphoreType.DMA((3,)),
        ],
        compiler_params=params(collective_id=0),
        name="attn_fwd",
    )(*inputs)


def fold(x):
    return jnp.sum(x.reshape(x.shape[0] // 8, 8, x.shape[1]), axis=0)


CHUNK = 16


def mlp_kernel(
    dims, n, tok_ref, cot_ref, mixed_ref, w_ref, vec_ref, bup_ref,
    out_ref, gres_ref, gmix_ref, grads_ref, dvec_ref, dbup_ref,
    act_ref, gp_ref, wot_ref, dwot_ref, dwup_ref, dwdt_ref,
    h2_ref, h2t_ref, cott_ref, mix_ref, gr_ref, outf_ref, out_old, gh2_ref, cotf_ref, norm_ref,
    inv_ref, sums_ref, upsum_ref,
):
    i = pl.program_id(0)
    step = 256
    tiles = FF // step
    steps = n // G
    chunks = [slice(c, c + CHUNK) for c in range(0, G * SP, CHUNK)]

    def spot(c):
        image, row = divmod(c.start, SP)
        return image, slice(row, row + CHUNK)

    @pl.when(i == 0)
    def _():
        wot_ref[...] = jnp.concatenate([w_ref[0, :, :THIRD], w_ref[1, :, :THIRD]], axis=1)
        for ref in (
            dwot_ref, dwup_ref, dwdt_ref, act_ref, gp_ref, h2t_ref, cott_ref, mix_ref, out_old,
            gh2_ref, cotf_ref, norm_ref, inv_ref, sums_ref, upsum_ref,
        ):
            ref[...] = jnp.zeros_like(ref)

    def weight_tile(j):
        cols = slice(step * j, step * (j + 1))
        dwup_ref[:, cols] += dot_nn(h2t_ref[...], gp_ref[:, cols])
        dwdt_ref[:, cols] += dot_nn(cott_ref[...], act_ref[:, cols])

    def finish(group, beside):
        beside(0)
        slot = G * (group % 2)
        for at in chunks:
            gh2, normed, cot = gh2_ref[at, :], norm_ref[at, :], cotf_ref[at, :]
            gres = cot + norm_backward(gh2, normed, inv_ref[at, 0:1], vec_ref[5:6, :])
            image, row = spot(at)
            gres_ref[slot + image, row, :] = gres
            gr_ref[at, :] = gres.astype(BF)
            sums_ref[0] += fold(gres)
            sums_ref[1] += fold(gh2 * normed)
            sums_ref[2] += fold(gh2)
            sums_ref[3] += fold(cot)
        beside(1)
        gmix = dot_nn(gr_ref[...], wot_ref[...]).astype(BF)
        for b in range(G):
            gmix_ref[slot + b] = gmix[SP * b : SP * (b + 1)]
        beside(2)
        for b in range(G):
            store_image(outf_ref, G * group + b, out_old[SP * b : SP * (b + 1), :])
        dwot_ref[...] += dot_tn(gr_ref[...], mix_ref[...])
        beside(3)

    finish(jnp.maximum(i - 1, 0), weight_tile)
    weight_tile(4)
    mixed = mixed_ref[...].reshape(G * SP, D)
    attended = dot_nt(mixed, wot_ref[...])
    for at in chunks:
        image, row = spot(at)
        cot = cot_ref[image, row, :].astype(F32)
        resid = tok_ref[image, row, :].astype(F32) + attended[at] + vec_ref[4:5, :]
        normed, inv = norm_stats(resid)
        h2_ref[at, :] = (normed * vec_ref[5:6, :] + vec_ref[6:7, :]).astype(BF)
        cotf_ref[at, :] = cot
        norm_ref[at, :] = normed
        inv_ref[at, :] = jnp.broadcast_to(inv, (CHUNK, 128))
        out_old[at, :] = resid + vec_ref[7:8, :]
    weight_tile(5)
    mix_ref[...] = mixed
    h2 = h2_ref[...]
    cot = cot_ref[...].reshape(G * SP, D)
    h2t_ref[...] = h2.T
    cott_ref[...] = cot.T
    for j in range(tiles):
        cols = slice(step * j, step * (j + 1))
        m, at = divmod(step * j, HALF)
        u = dot_nn(h2, w_ref[m, :, OUT_PAD + at : OUT_PAD + at + step]) + bup_ref[:, cols]
        ga = dot_nn(cot, w_ref[m, :, OUT_PAD + HALF + at : OUT_PAD + HALF + at + step])
        cdf = 0.5 * (1.0 + lax.erf(u * RSQRT2))
        act_ref[:, cols] = (u * cdf).astype(BF)
        gp = ga * (cdf + u * jnp.exp(-0.5 * u * u) * RSQRT_TAU)
        upsum_ref[:, cols] += fold(gp)
        gp_ref[:, cols] = gp.astype(BF)
    out = out_old[...]
    gh2 = None
    for m in range(2):
        cols = slice(HALF * m, HALF * (m + 1))
        out = out + dot_nt(act_ref[:, cols], w_ref[m, :, OUT_PAD + HALF :])
        part = dot_nt(gp_ref[:, cols], w_ref[m, :, OUT_PAD : OUT_PAD + HALF])
        gh2 = part if gh2 is None else gh2 + part
    out_old[...] = out
    gh2_ref[...] = gh2

    @pl.when(i == steps - 1)
    def _():
        finish(i, weight_tile)
        weight_tile(4)
        weight_tile(5)
        out_ref[...] = outf_ref[...].astype(BF)
        for k in range(4):
            dvec_ref[k : k + 1, :] = row_sum(sums_ref[k])
        dvec_ref[4:8, :] = jnp.zeros((4, D), F32)
        dbup_ref[...] = row_sum(upsum_ref[...])
        nz, ny, nx = dims
        rows = grads_ref.shape[4]
        spots = [(a, b, c) for a in range(nz) for b in range(ny) for c in range(nx)]
        group = 48 // rows
        for t in range(len(spots) // group):
            at = slice(48 * t, 48 * (t + 1))
            for m in range(2):
                parts = [
                    dwot_ref[at, THIRD * m : THIRD * (m + 1)],
                    jnp.zeros((48, OUT_PAD - THIRD), F32),
                    dwup_ref[at, HALF * m : HALF * (m + 1)],
                    dwdt_ref[at, HALF * m : HALF * (m + 1)],
                ]
                block = jnp.concatenate(parts, axis=1)
                for g in range(group):
                    grads_ref[(m,) + spots[t * group + g]] = block[
                        g * rows : (g + 1) * rows
                    ].astype(BF)


def mlp(tok, cot, mixed, wide, vec, bup, rows, dp):
    dims = chip_grid(dp)
    n = rows // S
    packed = (2, *dims, D // dp, WIDE)
    late = pl.BlockSpec((2 * G, SP, D), lambda i: (jnp.maximum(i - 1, 0) // 2, 0, 0))
    return pl.pallas_call(
        functools.partial(mlp_kernel, dims, n),
        grid=(n // G,),
        in_specs=[
            per_step(SP, D), per_step(SP, D), per_step(SP, D), whole((2, D, WIDE)), whole((8, D)),
            whole((1, FF)),
        ],
        out_specs=[whole((rows, D)), late, late, whole(packed), whole((8, D)), whole((1, FF))],
        out_shape=[
            jax.ShapeDtypeStruct((rows, D), BF),
            jax.ShapeDtypeStruct((n, SP, D), F32),
            jax.ShapeDtypeStruct((n, SP, D), BF),
            jax.ShapeDtypeStruct(packed, BF),
            jax.ShapeDtypeStruct((8, D), F32),
            jax.ShapeDtypeStruct((1, FF), F32),
        ],
        scratch_shapes=[
            pltpu.VMEM((G * SP, FF), BF), pltpu.VMEM((G * SP, FF), BF), pltpu.VMEM((D, D), BF),
            pltpu.VMEM((D, D), F32), pltpu.VMEM((D, FF), F32), pltpu.VMEM((D, FF), F32),
            pltpu.VMEM((G * SP, D), BF), pltpu.VMEM((D, G * SP), BF), pltpu.VMEM((D, G * SP), BF),
            pltpu.VMEM((G * SP, D), BF), pltpu.VMEM((G * SP, D), BF), pltpu.VMEM((rows, D), F32),
            pltpu.VMEM((G * SP, D), F32), pltpu.VMEM((G * SP, D), F32), pltpu.VMEM((G * SP, D), F32),
            pltpu.VMEM((G * SP, D), F32), pltpu.VMEM((G * SP, 128), F32), pltpu.VMEM((4, 8, D), F32),
            pltpu.VMEM((8, FF), F32),
        ],
        compiler_params=params(),
        name="mlp",
    )(tok, cot, mixed, wide, vec, bup)


class Reduction:
    def __init__(self, dims, copies, tag, packed, bufs, cut):
        self.dims, self.copies, self.packed, self.cut = dims, copies, packed, cut
        self.place = place_of(dims)
        self.along, self.other = peers_of(dims, self.place)
        z, y, x, mp = self.place
        self.p, self.a1, self.b1, self.ra1, self.rb1, self.ra2, self.rb2, self.f, self.rz = bufs
        low, high = pl.ds(0, cut), pl.ds(cut, packed.shape[-1] - cut)
        along = self.along
        copies.plan(tag + "pair", [lambda: (packed.at[1 - mp], self.p, self.other)])
        copies.plan(tag + "1l", [
            lambda o=o, c=c, d=d: (self.p.at[EVERY, EVERY, c, EVERY, low], self.ra1.at[o], d)
            for o, (c, d) in enumerate(along["x"])
        ])
        copies.plan(tag + "1h", [
            lambda o=o, b=b, d=d: (self.p.at[EVERY, b, EVERY, EVERY, high], self.rb1.at[o], d)
            for o, (b, d) in enumerate(along["y"])
        ])
        copies.plan(tag + "2l", [
            lambda o=o, b=b, d=d: (self.a1.at[EVERY, b], self.ra2.at[o], d)
            for o, (b, d) in enumerate(along["y"])
        ])
        copies.plan(tag + "2h", [
            lambda o=o, c=c, d=d: (self.b1.at[EVERY, c], self.rb2.at[o], d)
            for o, (c, d) in enumerate(along["x"])
        ])
        copies.plan(tag + "3", [
            lambda o=o, a=a, d=d: (self.f.at[a], self.rz.at[o], d)
            for o, (a, d) in enumerate(along["z"])
        ])

    @staticmethod
    def count(dims):
        nz, ny, nx = dims
        return 1 + 2 * (ny - 1) + 2 * (nx - 1) + nz - 1

    @staticmethod
    def scratch(dims, rows, width, cut):
        nz, ny, nx = dims

        def buf(w, *shape):
            return pltpu.VMEM((*shape, rows, w), BF)

        rest = width - cut
        return [
            buf(width, nz, ny, nx), buf(cut, nz, ny), buf(rest, nz, nx),
            buf(cut, nx - 1, nz, ny), buf(rest, ny - 1, nz, nx),
            buf(cut, ny - 1, nz), buf(rest, nx - 1, nz), buf(width, nz), buf(width, nz - 1),
        ]

    def add_pair(self, mine):
        nz, ny, nx = self.dims
        for i in range(nz):
            for j in range(ny):
                for k in range(nx):
                    total = mine[i, j, k].astype(F32) + self.p[i, j, k].astype(F32)
                    self.p[i, j, k] = total.astype(BF)

    def add_first_low(self):
        nz, ny, nx = self.dims
        x = self.place[2]
        for i in range(nz):
            for j in range(ny):
                total = self.p[i, j, x, :, : self.cut].astype(F32)
                for o in range(nx - 1):
                    total = total + self.ra1[o, i, j].astype(F32)
                self.a1[i, j] = total.astype(BF)

    def add_first_high(self):
        nz, ny, nx = self.dims
        y = self.place[1]
        for i in range(nz):
            for k in range(nx):
                total = self.p[i, y, k, :, self.cut :].astype(F32)
                for o in range(ny - 1):
                    total = total + self.rb1[o, i, k].astype(F32)
                self.b1[i, k] = total.astype(BF)

    def add_second(self):
        nz, ny, nx = self.dims
        _, y, x, _ = self.place
        for i in range(nz):
            total = self.a1[i, y].astype(F32)
            for o in range(ny - 1):
                total = total + self.ra2[o, i].astype(F32)
            self.f[i, :, : self.cut] = total.astype(BF)
            total = self.b1[i, x].astype(F32)
            for o in range(nx - 1):
                total = total + self.rb2[o, i].astype(F32)
            self.f[i, :, self.cut :] = total.astype(BF)

    def add_third(self):
        total = self.f[self.place[0]].astype(F32)
        for o in range(self.dims[0] - 1):
            total = total + self.rz[o].astype(F32)
        return total


def backward_kernel(
    dims, n, qkv_ref, e_ref, mixed_ref, linv_ref, gmix_ref, normed_ref, inv_ref, gres_ref, w_ref,
    vec_ref, dvec2_ref, dbup_ref, packed, gtok_ref, narrow_ref, wide_ref, total_ref, *refs,
):
    g_ref, acc_ref, gsum_ref, narrow, sums, vs, vr = refs[:7]
    wide_bufs, mine, narrow_bufs = refs[7:16], refs[16], refs[17:26]
    send, recv, sem = refs[26:]
    i = pl.program_id(0)
    steps = n // G
    copies = Copies(send, recv)
    wide = Reduction(dims, copies, "w", packed, wide_bufs, WIDE_CUT)
    thin = Reduction(dims, copies, "n", narrow, narrow_bufs, NARROW_CUT)
    mp = wide.place[3]
    keep = pltpu.make_async_copy(packed.at[mp], mine, sem)
    stages = [[wide.other], *([d for _, d in wide.along[axis]] for axis in "xyz")]
    bases = [sum(len(s) for s in stages[:k]) for k in range(4)]
    for k, devices in enumerate(stages):
        copies.plan("v%d" % k, [
            lambda k=k, o=o, d=d: (sums if k == 0 else vs.at[k - 1], vr.at[bases[k] + o], d)
            for o, d in enumerate(devices)
        ])

    def vec_add(k):
        total = sums[...] if k == 0 else vs[k - 1]
        for o in range(len(stages[k])):
            total = total + vr[bases[k] + o]
        if k < 3:
            vs[k] = total
        else:
            total_ref[...] = total

    @pl.when(i == 0)
    def _():
        greet(wide.along, wide.other)
        keep.start()
        acc_ref[...] = jnp.zeros_like(acc_ref)
        gsum_ref[...] = jnp.zeros_like(gsum_ref)
        met(wide.along)
        copies.start("wpair")

    @pl.when(i == 1)
    def _():
        keep.wait()
        copies.arrived("wpair")
        wide.add_pair(mine)
        copies.start("w1l", "w1h")

    @pl.when(i == steps // 2)
    def _():
        copies.arrived("w1l", "w1h")
        wide.add_first_low()
        wide.add_first_high()
        copies.start("w2l", "w2h")

    @pl.when(i == (3 * steps) // 4)
    def _():
        copies.arrived("w2l", "w2h")
        wide.add_second()
        copies.start("w3")

    @pl.when(i < steps)
    def _():
        lane = lax.broadcasted_iota(jnp.int32, (SP, 2 * HD), 1)
        zero = jnp.zeros((SP, 2 * HD), BF)
        minus = jnp.full((SP, 2 * HD), -1.0, BF)
        for p in range(PAIRS):
            lo, hi = 2 * HD * p, 2 * HD * (p + 1)
            for b in range(G):
                q = qkv_ref[b, :, lo:hi]
                k = qkv_ref[b, :, D + lo : D + hi]
                v = qkv_ref[b, :, 2 * D + lo : 2 * D + hi]
                go_f = gmix_ref[b, :, lo:hi].astype(F32) * linv_ref[b, :, lo:hi]
                go = go_f.astype(BF)
                god = jnp.concatenate(
                    [go, (go_f * mixed_ref[b, :, lo:hi].astype(F32)).astype(BF)], axis=1
                )
                gq = gk = gv = None
                for h in range(2):
                    own = (lane < HD) if h == 0 else (lane >= HD)
                    e = e_ref[b, 2 * p + h]
                    vd = jnp.concatenate(
                        [jnp.where(own, v, zero), jnp.where(own, minus, zero)], axis=1
                    )
                    ds = e * dot_nt(god, vd).astype(BF)
                    part_q = dot_nn(ds, jnp.where(own, k, zero))
                    part_k = dot_tn(ds, jnp.where(own, q, zero))
                    part_v = dot_tn(e, jnp.where(own, go, zero))
                    gq = part_q if gq is None else gq + part_q
                    gk = part_k if gk is None else gk + part_k
                    gv = part_v if gv is None else gv + part_v
                gq = gq * (1.0 / math.sqrt(HD))
                gk = gk * (1.0 / LOG2E)
                for j, grad in enumerate((gq, gk, gv)):
                    gsum_ref[:, D * j + lo : D * j + hi] += fold(grad)
                    g_ref[i, SP * b : SP * (b + 1), D * j + lo : D * j + hi] = grad.astype(BF)
        acc_ref[...] += dot_tn(normed_ref[...].reshape(G * SP, D).astype(BF), g_ref[i])

    @pl.when(i == steps - 1)
    def _():
        nz, ny, nx = dims
        rows = narrow.shape[4]
        spots = [(a, b, c) for a in range(nz) for b in range(ny) for c in range(nx)]
        group = 48 // rows
        turned = vec_ref[...].T
        gsum = row_sum(gsum_ref[...])
        gains = []
        for t in range(len(spots) // group):
            at = slice(48 * t, 48 * (t + 1))
            acc = acc_ref[at, :]
            gains.append(jnp.sum(acc * w_ref[at, :].astype(F32), axis=1, keepdims=True))
            dw = acc * turned[at, 0:1] + turned[at, 1:2] * gsum
            for m in range(2):
                parts = [dw[:, D * j + THIRD * m : D * j + THIRD * (m + 1)] for j in range(3)]
                parts.append(jnp.zeros((48, NARROW - 3 * THIRD), F32))
                block = jnp.concatenate(parts, axis=1)
                for k in range(group):
                    narrow[(m,) + spots[t * group + k]] = block[
                        k * rows : (k + 1) * rows
                    ].astype(BF)
        high = gsum.astype(BF)
        low = (gsum - high.astype(F32)).astype(BF)
        row = lax.broadcasted_iota(jnp.int32, (16, 3 * D), 0)
        both = jnp.where(row == 0, high, jnp.where(row == 1, low, jnp.zeros((16, 3 * D), BF)))
        sums[0:1] = gsum[:, :D]
        sums[1:2] = gsum[:, 2 * D :]
        gain = jnp.broadcast_to(jnp.concatenate(gains, axis=0), (D, 128)).T
        sums[2:3] = gain[0:1, :]
        sums[3:4] = row_sum(dot_nt(both, w_ref[...]))
        sums[4:8] = dvec2_ref[0:4]
        for j in range(FF // D):
            sums[8 + j : 9 + j] = dbup_ref[:, D * j : D * (j + 1)]
        sums[12:16] = jnp.zeros((4, D), F32)
        copies.start("npair", "v0")

    @pl.when(i == steps + 2)
    def _():
        copies.arrived("npair", "v0")
        thin.add_pair(narrow.at[mp])
        vec_add(0)
        copies.start("n1l", "n1h", "v1")

    @pl.when(i == steps + 3)
    def _():
        copies.arrived("w3")
        wide_ref[...] = wide.add_third()

    @pl.when(i == steps + 4)
    def _():
        copies.arrived("n1l", "v1")
        thin.add_first_low()
        vec_add(1)
        copies.start("n2l", "v2")
        copies.arrived("n1h")
        thin.add_first_high()
        copies.start("n2h")

    @pl.when(i == steps + 6)
    def _():
        copies.arrived("n2l", "n2h", "v2")
        thin.add_second()
        vec_add(2)
        copies.start("n3", "v3")

    @pl.when(i >= steps)
    def _():
        group = jnp.maximum(i - steps, 0)
        gh1 = dot_nt(g_ref[group], w_ref[...])
        for b in range(G):
            parts = []
            for c in range(0, SP, CHUNK):
                at = slice(c, c + CHUNK)
                back = norm_backward(
                    gh1[SP * b + c : SP * b + c + CHUNK], normed_ref[b, at, :],
                    inv_ref[b, at, 0:1], vec_ref[0:1, :],
                )
                parts.append(gres_ref[b, at, :] + back)
            store_image(gtok_ref, G * group + b, jnp.concatenate(parts, axis=0))

    @pl.when(i == 2 * steps - 1)
    def _():
        copies.arrived("n3", "v3")
        narrow_ref[...] = thin.add_third()
        vec_add(3)
        copies.left(*copies.groups)


def backward(qkv, e, mixed, linv, gmix, normed, inv, gres, wqkv, vec, dvec2, dbup, packed, tall, dp):
    dims = chip_grid(dp)
    nz, ny, nx = dims
    n = qkv.shape[0]
    steps = n // G
    rows = D // dp
    count = 2 * Reduction.count(dims) + nz + ny + nx - 2

    def heads(*shape):
        return pl.BlockSpec((G, *shape), lambda i: (jnp.minimum(i, steps - 1),) + (0,) * len(shape))

    def after(*shape):
        return pl.BlockSpec((G, *shape), lambda i: (jnp.maximum(i - steps, 0),) + (0,) * len(shape))

    def twice(*shape):
        return pl.BlockSpec((G, *shape), lambda i: (i % steps,) + (0,) * len(shape))

    return pl.pallas_call(
        functools.partial(backward_kernel, dims, n),
        grid=(2 * steps,),
        in_specs=[
            heads(SP, 3 * D), heads(HEADS, SP, SP), heads(SP, D), heads(SP, D), heads(SP, D),
            twice(SP, D), after(SP, 128), after(SP, D), whole((D, 3 * D)), whole((8, D)),
            whole((8, D)), whole((1, FF)), pl.BlockSpec(memory_space=pl.ANY),
        ],
        out_specs=[
            whole((tall, D)), whole((rows, NARROW)), whole((rows, WIDE)), whole((16, D)),
        ],
        out_shape=[
            jax.ShapeDtypeStruct((tall, D), F32),
            jax.ShapeDtypeStruct((rows, NARROW), F32),
            jax.ShapeDtypeStruct((rows, WIDE), F32),
            jax.ShapeDtypeStruct((16, D), F32),
        ],
        scratch_shapes=[
            pltpu.VMEM((steps, G * SP, 3 * D), BF),
            pltpu.VMEM((D, 3 * D), F32),
            pltpu.VMEM((8, 3 * D), F32),
            pltpu.VMEM((2, *dims, rows, NARROW), BF),
            pltpu.VMEM((16, D), F32),
            pltpu.VMEM((3, 16, D), F32),
            pltpu.VMEM((nz + ny + nx - 2, 16, D), F32),
            *Reduction.scratch(dims, rows, WIDE, WIDE_CUT),
            pltpu.VMEM((*dims, rows, WIDE), BF),
            *Reduction.scratch(dims, rows, NARROW, NARROW_CUT),
            pltpu.SemaphoreType.DMA((count,)),
            pltpu.SemaphoreType.DMA((count,)),
            pltpu.SemaphoreType.DMA,
        ],
        compiler_params=params(collective_id=1),
        name="backward",
    )(qkv, e, mixed, linv, gmix, normed, inv, gres, wqkv, vec, dvec2, dbup, packed)


def split_kernel(n, gtok_in, narrow_ref, wide_ref, vec_ref, gtok_ref, *outs):
    gtok_ref[...] = gtok_in[...]

    @pl.when(pl.program_id(0) == 0)
    def _():
        for j in range(3):
            outs[j][...] = narrow_ref[:, THIRD * j : THIRD * (j + 1)]
        outs[3][...] = wide_ref[:, :THIRD]
        outs[4][...] = wide_ref[:, OUT_PAD : OUT_PAD + HALF]
        outs[5][...] = wide_ref[:, OUT_PAD + HALF :]
        index = lax.axis_index("dp") * 2 + lax.axis_index("mp")
        per = D // n
        vec = pltpu.roll(vec_ref[...], D - index * per, axis=1)
        for row, out in zip((2, 3, 0, 1, 4, 5, 6, 7), outs[6:]):
            out[...] = vec[row : row + 1, :per]
        wide = jnp.concatenate([vec_ref[8 + j : 9 + j, :] for j in range(FF // D)], axis=1)
        wide = pltpu.roll(jnp.broadcast_to(wide, (8, FF)), FF - index * (FF // n), axis=1)
        outs[14][...] = wide[0:1, : FF // n]


def split(gtok, narrow, wide, vec, n):
    rows = narrow.shape[0]
    tall = gtok.shape[0]
    shapes = [(rows, THIRD)] * 4 + [(rows, HALF)] * 2 + [(1, D // n)] * 8 + [(1, FF // n)]
    half = pl.BlockSpec((tall // 2, D), lambda i: (i, 0))
    return pl.pallas_call(
        functools.partial(split_kernel, n),
        grid=(2,),
        in_specs=[half] + [whole(a.shape) for a in (narrow, wide, vec)],
        out_specs=[half] + [whole(s) for s in shapes],
        out_shape=[jax.ShapeDtypeStruct(s, F32) for s in [(tall, D), *shapes]],
        compiler_params=params(),
        name="split",
    )(gtok, narrow, wide, vec)


def whole(shape):
    return pl.BlockSpec(shape, lambda i: (0,) * len(shape))


def per_image(*shape):
    return pl.BlockSpec((1, *shape), lambda i: (i,) + (0,) * len(shape))


def per_step(*shape):
    return pl.BlockSpec((G, *shape), lambda i: (i,) + (0,) * len(shape))


def params(collective_id=None):
    return pltpu.CompilerParams(
        dimension_semantics=("arbitrary",), vmem_limit_bytes=62 * 1024 * 1024,
        collective_id=collective_id, has_side_effects=collective_id is not None,
    )


def on_device(
    tokens, w_query, w_key, w_value, w_out, w_up, w_down, ln1_gain, ln1_bias, b_query, b_value,
    b_out, ln2_gain, ln2_bias, b_up, b_down, cotangent,
):
    dp = lax.axis_size("dp")
    vectors = (ln1_gain, ln1_bias, b_query, b_value, b_out, ln2_gain, ln2_bias, b_down)
    qkv, e, mixed, linv, normed, inv, tok, cot, wqkv, vec, bup, wide = attn_fwd(
        (w_query, w_key, w_value, w_out.T, w_up, w_down.T), [v[None] for v in vectors], b_up[None],
        tokens, cotangent, dp,
    )
    out, gres, gmix, packed, dvec2, dbup = mlp(
        tok, cot, mixed, wide.reshape(2, D, WIDE), vec, bup, tokens.shape[0], dp
    )
    gtok, narrow_sum, wide_sum, sums = backward(
        qkv, e, mixed, linv, gmix, normed, inv, gres, wqkv, vec, dvec2, dbup, packed,
        tokens.shape[0], dp,
    )
    gtok, *grads = split(gtok, narrow_sum, wide_sum, sums, dp * lax.axis_size("mp"))
    vecs = [v.reshape(-1) for v in grads[6:]]
    return (
        out, gtok, grads[0], grads[1], grads[2], grads[3].T, grads[4], grads[5].T,
        *vecs[:7], vecs[8], vecs[7],
    )


def solution(mesh):
    row, mat, tam, vec = P(("dp", "mp"), None), P("dp", "mp"), P("mp", "dp"), P("dp")
    part = P(("dp", "mp"))
    return jax.shard_map(
        on_device,
        mesh=mesh,
        in_specs=(row, mat, mat, mat, tam, mat, tam, *([vec] * 9), row),
        out_specs=(row, row, mat, mat, mat, tam, mat, tam, *([part] * 9)),
        check_vma=False,
    )
```

```python
import functools
import math

import jax
import jax.numpy as jnp
from jax import lax
from jax.experimental import pallas as pl
from jax.experimental.pallas import tpu as pltpu
from jax.sharding import PartitionSpec as P

D = 384
HD = 64
FF = 1536
S = 197
HEADS = D // HD
PAIRS = HEADS // 2

SP = 208
WIN = 224
G = 2

EPS = 1e-06
RSQRT2 = 0.7071067811865476
RSQRT_TAU = 0.3989422804014327
LOG2E = 1.4426950408889634
Q_SCALE = LOG2E / math.sqrt(HD)
BF = jnp.bfloat16
F32 = jnp.float32


def dot_nn(a, b):
    return lax.dot_general(a, b, (((1,), (0,)), ((), ())), preferred_element_type=F32)


def dot_nt(a, b):
    return lax.dot_general(a, b, (((1,), (1,)), ((), ())), preferred_element_type=F32)


def dot_tn(a, b):
    return lax.dot_general(a, b, (((0,), (0,)), ((), ())), preferred_element_type=F32)


def window_of(i, rows):
    start = i * S
    base = jnp.minimum((start // 16) * 16, rows - WIN)
    return pl.multiple_of(base, 16), start - base


def load_image(ref, i):
    base, off = window_of(i, ref.shape[0])
    rows = ref[pl.ds(base, WIN), :].astype(F32)
    rows = pltpu.roll(rows, WIN - off, axis=0)[:SP]
    live = lax.broadcasted_iota(jnp.int32, rows.shape, 0) < S
    return jnp.where(live, rows, 0.0)


def store_image(ref, i, rows):
    start = i * S
    r = start % 8
    base = start - r
    total = ref.shape[0]
    groups = SP // 8
    turned = pltpu.roll(rows.reshape(groups, 8, D), r, axis=1)
    first = lax.broadcasted_iota(jnp.int32, (8, D), 0) < r
    old = ref[pl.ds(pl.multiple_of(base, 8), 8), :]
    ref[pl.ds(pl.multiple_of(base, 8), 8), :] = jnp.where(first, old, turned[0])
    for g in range(1, groups - 1):
        ref[pl.ds(pl.multiple_of(base + 8 * g, 8), 8), :] = jnp.where(
            first, turned[g - 1], turned[g]
        )
    over = base + SP > total
    here = jnp.where(over, total - 8, base + SP - 8)
    tail = [jnp.where(first, turned[g - 1], turned[g]) for g in (groups - 2, groups - 1)]
    ref[pl.ds(pl.multiple_of(here, 8), 8), :] = jnp.where(over, tail[0], tail[1])


def norm_stats(x):
    mean = jnp.mean(x, axis=-1, keepdims=True)
    centred = x - mean
    inv = lax.rsqrt(jnp.mean(centred * centred, axis=-1, keepdims=True) + EPS)
    return centred * inv, inv


def norm_backward(grad, normed, inv, gain):
    e = grad * gain
    return inv * (
        e
        - jnp.mean(e, axis=-1, keepdims=True)
        - normed * jnp.mean(e * normed, axis=-1, keepdims=True)
    )


def row_sum(x):
    return jnp.sum(x, axis=0, keepdims=True)


THIRD = D // 2
HALF = FF // 2
NARROW = 640
NARROW_CUT = 384
OUT_PAD = 256
WIDE = OUT_PAD + 2 * HALF
WIDE_CUT = 896
MESH = pl.DeviceIdType.MESH
EVERY = slice(None)


def chip_grid(dp):
    side = math.isqrt(dp // 4)
    return 4, side, side


def place_of(dims):
    _, ny, nx = dims
    dp, mp = lax.axis_index("dp"), lax.axis_index("mp")
    return dp // (ny * nx), (dp // nx) % ny, dp % nx, mp


def peers_of(dims, place):
    (nz, ny, nx), (z, y, x, mp) = dims, place

    def at(a, b, c, m):
        return ((a * ny + b) * nx + c, m)

    along = {
        "z": [((z + o) % nz, at((z + o) % nz, y, x, mp)) for o in range(1, nz)],
        "y": [((y + o) % ny, at(z, (y + o) % ny, x, mp)) for o in range(1, ny)],
        "x": [((x + o) % nx, at(z, y, (x + o) % nx, mp)) for o in range(1, nx)],
    }
    return along, at(z, y, x, 1 - mp)


def greet(along, other):
    for device in [d for peers in along.values() for _, d in peers] + [other]:
        pl.semaphore_signal(
            pltpu.get_barrier_semaphore(), inc=1, device_id=device, device_id_type=MESH
        )


def met(along):
    count = sum(len(peers) for peers in along.values()) + 1
    pl.semaphore_wait(pltpu.get_barrier_semaphore(), count)


class Copies:
    def __init__(self, send, recv):
        self.send, self.recv, self.groups, self.count = send, recv, {}, 0

    def plan(self, name, makers):
        self.groups[name] = [(self.count + i, m) for i, m in enumerate(makers)]
        self.count += len(makers)

    def each(self, names):
        for name in names:
            for index, make in self.groups[name]:
                src, dst, device = make()
                yield pltpu.make_async_remote_copy(
                    src_ref=src, dst_ref=dst, send_sem=self.send.at[index],
                    recv_sem=self.recv.at[index], device_id=device, device_id_type=MESH,
                )

    def start(self, *names):
        for copy in self.each(names):
            copy.start()

    def arrived(self, *names):
        for copy in self.each(names):
            copy.wait_recv()

    def left(self, *names):
        for copy in self.each(names):
            copy.wait_send()


def plan_gather(copies, tag, w, own, cut, along, other, place):
    z, y, x, mp = place
    low, high = pl.ds(0, cut), pl.ds(cut, w.shape[-1] - cut)

    def same(index, device):
        return lambda: (w.at[index], w.at[index], device)

    def spread(index, axis):
        return [same(index, d) for _, d in along[axis]]

    def shares(indices):
        return [same(index, other) for index in indices]

    copies.plan(tag + "1", [lambda d=d: (own, w.at[mp, z, y, x], d) for _, d in along["z"]])
    copies.plan(tag + "2l", spread((mp, EVERY, y, x, EVERY, low), "y"))
    copies.plan(tag + "2h", spread((mp, EVERY, y, x, EVERY, high), "x"))
    copies.plan(tag + "3l", spread((mp, EVERY, EVERY, x, EVERY, low), "x"))
    copies.plan(tag + "3h", spread((mp, EVERY, y, EVERY, EVERY, high), "y"))
    copies.plan(tag + "s1", shares([(mp, EVERY, y, x)]))
    copies.plan(tag + "s2l", shares([(mp, EVERY, b, x, EVERY, low) for b, _ in along["y"]]))
    copies.plan(tag + "s2h", shares([(mp, EVERY, y, c, EVERY, high) for c, _ in along["x"]]))
    copies.plan(tag + "s3l", shares([(mp, EVERY, EVERY, c, EVERY, low) for c, _ in along["x"]]))
    copies.plan(tag + "s3h", shares([(mp, EVERY, b, EVERY, EVERY, high) for b, _ in along["y"]]))


def attn_fwd_kernel(dims, n, *refs):
    (wq, wk, wv, wot, wu, wdt), vectors, bup_in = refs[:6], refs[6:14], refs[14]
    tok_hbm, cot_hbm = refs[15:17]
    (
        qkv_ref, e_ref, mixed_ref, linv_ref, normed_ref, inv_ref, tokp_ref, cotp_ref, w_ref, vec_ref,
        bup_ref, wide,
    ) = refs[17:29]
    narrow, v, own, normed_all, inv_all, tok_all, cot_all, tok_ref, cot_ref, send, recv, sem = refs[29:]
    i = pl.program_id(0)
    steps = n // G
    nz, ny, nx = dims
    place = place_of(dims)
    z, y, x, mp = place
    rows = own.shape[0]
    along, other = peers_of(dims, place)
    copies = Copies(send, recv)
    plan_gather(copies, "n", narrow, narrow.at[mp, z, y, x], NARROW_CUT, along, other, place)
    plan_gather(copies, "w", wide, own, WIDE_CUT, along, other, place)

    def vec_spread(index, axis):
        return [lambda d=d: (v.at[index], v.at[index], d) for _, d in along[axis]]

    copies.plan("v1", vec_spread((z, y, x), "z"))
    copies.plan("v2", vec_spread((EVERY, y, x), "y"))
    copies.plan("v3", vec_spread((EVERY, EVERY, x), "x"))
    keep = pltpu.make_async_copy(own, wide.at[mp, z, y, x], sem.at[0])
    fetch = [
        pltpu.make_async_copy(tok_hbm, tok_ref, sem.at[1]),
        pltpu.make_async_copy(cot_hbm, cot_ref, sem.at[2]),
    ]

    def norms(first, last):
        @pl.loop(first, last)
        def _(j):
            tok = load_image(tok_ref, j)
            normed, inv = norm_stats(tok)
            tok_all[j] = tok.astype(BF)
            cot_all[j] = load_image(cot_ref, j).astype(BF)
            normed_all[j] = normed
            inv_all[j] = jnp.broadcast_to(inv, (SP, 128))

    @pl.when(i == 0)
    def _():
        for copy in fetch:
            copy.start()
        narrow[mp, z, y, x] = jnp.concatenate(
            [wq[...], wk[...], wv[...], jnp.zeros((rows, NARROW - 3 * THIRD), BF)], axis=1
        )
        own[...] = jnp.concatenate(
            [wot[...], jnp.zeros((rows, OUT_PAD - THIRD), BF), wu[...], wdt[...]], axis=1
        )
        v[z, y, x] = jnp.zeros((16, 128), F32)
        for j, vector in enumerate(vectors):
            v[z, y, x, j : j + 1, :rows] = vector[...].astype(F32)
        v[z, y, x, 8:9, : bup_in.shape[1]] = bup_in[...].astype(F32)
        greet(along, other)
        keep.start()
        for copy in fetch:
            copy.wait()
        norms(0, n // 4)
        met(along)
        copies.start("v1", "n1")
        norms(n // 4, n // 2)
        copies.arrived("v1", "n1")
        copies.start("v2", "n2l", "n2h", "w1", "ns1")
        norms(n // 2, (3 * n) // 4)
        copies.arrived("v2", "n2l", "n2h")
        copies.start("v3", "n3l", "n3h", "ns2l", "ns2h")
        norms((3 * n) // 4, n)
        copies.arrived("v3", "n3l")
        copies.start("ns3l")
        copies.arrived("n3h")
        copies.start("ns3h")
        keep.wait()
        copies.arrived("w1")
        copies.start("w2l", "w2h", "ws1")
        spots = [(a, b, c) for a in range(nz) for b in range(ny) for c in range(nx)]
        vec_ref[...] = jnp.concatenate([v[s][0:8, :rows] for s in spots], axis=1)
        bup_ref[...] = jnp.concatenate([v[s][8:9, : bup_in.shape[1]] for s in spots], axis=1)
        copies.arrived("ns1", "ns2l", "ns2h", "ns3l", "ns3h")
        group = 48 // rows
        for t in range(len(spots) // group):
            block = [
                jnp.concatenate(
                    [narrow[(m,) + s].astype(F32) for s in spots[t * group : (t + 1) * group]], axis=0
                )
                for m in range(2)
            ]
            for j in range(3):
                cols = slice(THIRD * j, THIRD * (j + 1))
                w_ref[48 * t : 48 * (t + 1), D * j : D * (j + 1)] = jnp.concatenate(
                    [half[:, cols] for half in block], axis=1
                ).astype(BF)

    @pl.when(i == 2)
    def _():
        copies.arrived("w2l", "w2h")
        copies.start("w3l", "w3h", "ws2l", "ws2h")

    images = pl.ds(G * i, G)
    normed = normed_all[images]
    normed_ref[...] = normed
    inv_ref[...] = inv_all[images]
    tokp_ref[...] = tok_all[images]
    cotp_ref[...] = cot_all[images]
    h1 = (normed * vec_ref[0:1, :] + vec_ref[1:2, :]).astype(BF).reshape(G * SP, D)
    q = ((dot_nn(h1, w_ref[:, 0:D]) + vec_ref[2:3, :]) * Q_SCALE).astype(BF)
    k = dot_nn(h1, w_ref[:, D : 2 * D]).astype(BF)
    value = (dot_nn(h1, w_ref[:, 2 * D :]) + vec_ref[3:4, :]).astype(BF)
    for j, x in enumerate((q, k, value)):
        for b in range(G):
            qkv_ref[b, :, D * j : D * (j + 1)] = x[SP * b : SP * (b + 1)]
    lane = lax.broadcasted_iota(jnp.int32, (SP, 2 * HD), 1)
    is_key = lax.broadcasted_iota(jnp.int32, (SP, SP), 1) < S
    zero = jnp.zeros((SP, 2 * HD), BF)
    one = jnp.ones((SP, 2 * HD), BF)
    work = [(p, b) for p in range(PAIRS) for b in range(G)]

    def own_lanes(h):
        return (lane < HD) if h == 0 else (lane >= HD)

    def weigh(turn):
        p, b = work[turn]
        cols = slice(2 * HD * p, 2 * HD * (p + 1))
        rows_of = slice(SP * b, SP * (b + 1))
        for h in range(2):
            scores = dot_nt(q[rows_of, cols], jnp.where(own_lanes(h), k[rows_of, cols], zero))
            scores = jnp.where(is_key, scores, -1e30)
            top = jnp.max(scores, axis=-1, keepdims=True)
            e_ref[b, 2 * p + h] = jnp.exp2(scores - top).astype(BF)

    def mix(turn):
        p, b = work[turn]
        cols = slice(2 * HD * p, 2 * HD * (p + 1))
        total = None
        for h in range(2):
            mine = own_lanes(h)
            vh = jnp.where(mine, value[SP * b : SP * (b + 1), cols], zero)
            part = dot_nn(
                e_ref[b, 2 * p + h],
                jnp.concatenate([vh, jnp.where(mine, one, zero)], axis=1),
            )
            total = part if total is None else total + part
        linv = 1.0 / total[:, 2 * HD :]
        linv_ref[b, :, cols] = linv
        mixed_ref[b, :, cols] = (total[:, : 2 * HD] * linv).astype(BF)

    weigh(0)
    for turn in range(len(work)):
        if turn + 1 < len(work):
            weigh(turn + 1)
        mix(turn)

    @pl.when(i == steps - 2)
    def _():
        copies.arrived("w3l", "w3h")
        copies.start("ws3l", "ws3h")

    @pl.when(i == steps - 1)
    def _():
        copies.arrived("ws1", "ws2l", "ws2h", "ws3l", "ws3h")
        copies.left(*copies.groups)


def attn_fwd(mats, vectors, bup, tokens, cot, dp):
    dims = chip_grid(dp)
    nz, ny, nx = dims
    rows = D // dp
    n = tokens.shape[0] // S
    count = 2 * (nz - 1 + 4 * (ny - 1) + 4 * (nx - 1) + 1) + nz + ny + nx - 3
    inputs = (*mats, *vectors, bup, tokens, cot)
    return pl.pallas_call(
        functools.partial(attn_fwd_kernel, dims, n),
        grid=(n // G,),
        in_specs=[whole(a.shape) for a in inputs[:-2]] + [pl.BlockSpec(memory_space=pl.ANY)] * 2,
        out_specs=[
            per_step(SP, 3 * D), per_step(HEADS, SP, SP), per_step(SP, D), per_step(SP, D),
            per_step(SP, D), per_step(SP, 128), per_step(SP, D), per_step(SP, D),
            whole((D, 3 * D)), whole((8, D)), whole((1, FF)), pl.BlockSpec(memory_space=pl.ANY),
        ],
        out_shape=[
            jax.ShapeDtypeStruct((n, SP, 3 * D), BF),
            jax.ShapeDtypeStruct((n, HEADS, SP, SP), BF),
            jax.ShapeDtypeStruct((n, SP, D), BF),
            jax.ShapeDtypeStruct((n, SP, D), F32),
            jax.ShapeDtypeStruct((n, SP, D), F32),
            jax.ShapeDtypeStruct((n, SP, 128), F32),
            jax.ShapeDtypeStruct((n, SP, D), BF),
            jax.ShapeDtypeStruct((n, SP, D), BF),
            jax.ShapeDtypeStruct((D, 3 * D), BF),
            jax.ShapeDtypeStruct((8, D), F32),
            jax.ShapeDtypeStruct((1, FF), F32),
            jax.ShapeDtypeStruct((2, nz, ny, nx, rows, WIDE), BF),
        ],
        scratch_shapes=[
            pltpu.VMEM((2, nz, ny, nx, rows, NARROW), BF),
            pltpu.VMEM((nz, ny, nx, 16, 128), F32),
            pltpu.VMEM((rows, WIDE), BF),
            pltpu.VMEM((n, SP, D), F32),
            pltpu.VMEM((n, SP, 128), F32),
            pltpu.VMEM((n, SP, D), BF),
            pltpu.VMEM((n, SP, D), BF),
            pltpu.VMEM(tokens.shape, BF),
            pltpu.VMEM(tokens.shape, BF),
            pltpu.SemaphoreType.DMA((count,)),
            pltpu.SemaphoreType.DMA((count,)),
            pltpu.SemaphoreType.DMA((3,)),
        ],
        compiler_params=params(collective_id=0),
        name="attn_fwd",
    )(*inputs)


def fold(x):
    return jnp.sum(x.reshape(x.shape[0] // 8, 8, x.shape[1]), axis=0)


CHUNK = 16


def mlp_kernel(
    dims, n, tok_ref, cot_ref, mixed_ref, w_ref, vec_ref, bup_ref,
    out_ref, gres_ref, gmix_ref, grads_ref, dvec_ref, dbup_ref,
    act_ref, gp_ref, wot_ref, dwot_ref, dwup_ref, dwdt_ref,
    h2_ref, h2t_ref, cott_ref, mix_ref, gr_ref, outf_ref, out_old, gh2_ref, cotf_ref, norm_ref,
    inv_ref, sums_ref, upsum_ref,
):
    i = pl.program_id(0)
    step = 256
    tiles = FF // step
    steps = n // G
    chunks = [slice(c, c + CHUNK) for c in range(0, G * SP, CHUNK)]

    def spot(c):
        image, row = divmod(c.start, SP)
        return image, slice(row, row + CHUNK)

    @pl.when(i == 0)
    def _():
        wot_ref[...] = jnp.concatenate([w_ref[0, :, :THIRD], w_ref[1, :, :THIRD]], axis=1)
        for ref in (
            dwot_ref, dwup_ref, dwdt_ref, act_ref, gp_ref, h2t_ref, cott_ref, mix_ref, out_old,
            gh2_ref, cotf_ref, norm_ref, inv_ref, sums_ref, upsum_ref,
        ):
            ref[...] = jnp.zeros_like(ref)

    def weight_tile(j):
        cols = slice(step * j, step * (j + 1))
        dwup_ref[:, cols] += dot_nn(h2t_ref[...], gp_ref[:, cols])
        dwdt_ref[:, cols] += dot_nn(cott_ref[...], act_ref[:, cols])

    def finish(group, beside):
        beside(0)
        slot = G * (group % 2)
        for at in chunks:
            gh2, normed, cot = gh2_ref[at, :], norm_ref[at, :], cotf_ref[at, :]
            gres = cot + norm_backward(gh2, normed, inv_ref[at, 0:1], vec_ref[5:6, :])
            image, row = spot(at)
            gres_ref[slot + image, row, :] = gres
            gr_ref[at, :] = gres.astype(BF)
            sums_ref[0] += fold(gres)
            sums_ref[1] += fold(gh2 * normed)
            sums_ref[2] += fold(gh2)
            sums_ref[3] += fold(cot)
        beside(1)
        gmix = dot_nn(gr_ref[...], wot_ref[...]).astype(BF)
        for b in range(G):
            gmix_ref[slot + b] = gmix[SP * b : SP * (b + 1)]
        beside(2)
        for b in range(G):
            store_image(outf_ref, G * group + b, out_old[SP * b : SP * (b + 1), :])
        dwot_ref[...] += dot_tn(gr_ref[...], mix_ref[...])
        beside(3)

    finish(jnp.maximum(i - 1, 0), weight_tile)
    weight_tile(4)
    mixed = mixed_ref[...].reshape(G * SP, D)
    attended = dot_nt(mixed, wot_ref[...])
    for at in chunks:
        image, row = spot(at)
        cot = cot_ref[image, row, :].astype(F32)
        resid = tok_ref[image, row, :].astype(F32) + attended[at] + vec_ref[4:5, :]
        normed, inv = norm_stats(resid)
        h2_ref[at, :] = (normed * vec_ref[5:6, :] + vec_ref[6:7, :]).astype(BF)
        cotf_ref[at, :] = cot
        norm_ref[at, :] = normed
        inv_ref[at, :] = jnp.broadcast_to(inv, (CHUNK, 128))
        out_old[at, :] = resid + vec_ref[7:8, :]
    weight_tile(5)
    mix_ref[...] = mixed
    h2 = h2_ref[...]
    cot = cot_ref[...].reshape(G * SP, D)
    h2t_ref[...] = h2.T
    cott_ref[...] = cot.T
    for j in range(tiles):
        cols = slice(step * j, step * (j + 1))
        m, at = divmod(step * j, HALF)
        u = dot_nn(h2, w_ref[m, :, OUT_PAD + at : OUT_PAD + at + step]) + bup_ref[:, cols]
        ga = dot_nn(cot, w_ref[m, :, OUT_PAD + HALF + at : OUT_PAD + HALF + at + step])
        cdf = 0.5 * (1.0 + lax.erf(u * RSQRT2))
        act_ref[:, cols] = (u * cdf).astype(BF)
        gp = ga * (cdf + u * jnp.exp(-0.5 * u * u) * RSQRT_TAU)
        upsum_ref[:, cols] += fold(gp)
        gp_ref[:, cols] = gp.astype(BF)
    out = out_old[...]
    gh2 = None
    for m in range(2):
        cols = slice(HALF * m, HALF * (m + 1))
        out = out + dot_nt(act_ref[:, cols], w_ref[m, :, OUT_PAD + HALF :])
        part = dot_nt(gp_ref[:, cols], w_ref[m, :, OUT_PAD : OUT_PAD + HALF])
        gh2 = part if gh2 is None else gh2 + part
    out_old[...] = out
    gh2_ref[...] = gh2

    @pl.when(i == steps - 1)
    def _():
        finish(i, weight_tile)
        weight_tile(4)
        weight_tile(5)
        out_ref[...] = outf_ref[...].astype(BF)
        for k in range(4):
            dvec_ref[k : k + 1, :] = row_sum(sums_ref[k])
        dvec_ref[4:8, :] = jnp.zeros((4, D), F32)
        dbup_ref[...] = row_sum(upsum_ref[...])
        nz, ny, nx = dims
        rows = grads_ref.shape[4]
        spots = [(a, b, c) for a in range(nz) for b in range(ny) for c in range(nx)]
        group = 48 // rows
        for t in range(len(spots) // group):
            at = slice(48 * t, 48 * (t + 1))
            for m in range(2):
                parts = [
                    dwot_ref[at, THIRD * m : THIRD * (m + 1)],
                    jnp.zeros((48, OUT_PAD - THIRD), F32),
                    dwup_ref[at, HALF * m : HALF * (m + 1)],
                    dwdt_ref[at, HALF * m : HALF * (m + 1)],
                ]
                block = jnp.concatenate(parts, axis=1)
                for g in range(group):
                    grads_ref[(m,) + spots[t * group + g]] = block[
                        g * rows : (g + 1) * rows
                    ].astype(BF)


def mlp(tok, cot, mixed, wide, vec, bup, rows, dp):
    dims = chip_grid(dp)
    n = rows // S
    packed = (2, *dims, D // dp, WIDE)
    late = pl.BlockSpec((2 * G, SP, D), lambda i: (jnp.maximum(i - 1, 0) // 2, 0, 0))
    return pl.pallas_call(
        functools.partial(mlp_kernel, dims, n),
        grid=(n // G,),
        in_specs=[
            per_step(SP, D), per_step(SP, D), per_step(SP, D), whole((2, D, WIDE)), whole((8, D)),
            whole((1, FF)),
        ],
        out_specs=[whole((rows, D)), late, late, whole(packed), whole((8, D)), whole((1, FF))],
        out_shape=[
            jax.ShapeDtypeStruct((rows, D), BF),
            jax.ShapeDtypeStruct((n, SP, D), F32),
            jax.ShapeDtypeStruct((n, SP, D), BF),
            jax.ShapeDtypeStruct(packed, BF),
            jax.ShapeDtypeStruct((8, D), F32),
            jax.ShapeDtypeStruct((1, FF), F32),
        ],
        scratch_shapes=[
            pltpu.VMEM((G * SP, FF), BF), pltpu.VMEM((G * SP, FF), BF), pltpu.VMEM((D, D), BF),
            pltpu.VMEM((D, D), F32), pltpu.VMEM((D, FF), F32), pltpu.VMEM((D, FF), F32),
            pltpu.VMEM((G * SP, D), BF), pltpu.VMEM((D, G * SP), BF), pltpu.VMEM((D, G * SP), BF),
            pltpu.VMEM((G * SP, D), BF), pltpu.VMEM((G * SP, D), BF), pltpu.VMEM((rows, D), F32),
            pltpu.VMEM((G * SP, D), F32), pltpu.VMEM((G * SP, D), F32), pltpu.VMEM((G * SP, D), F32),
            pltpu.VMEM((G * SP, D), F32), pltpu.VMEM((G * SP, 128), F32), pltpu.VMEM((4, 8, D), F32),
            pltpu.VMEM((8, FF), F32),
        ],
        compiler_params=params(),
        name="mlp",
    )(tok, cot, mixed, wide, vec, bup)


class Reduction:
    def __init__(self, dims, copies, tag, packed, bufs, cut):
        self.dims, self.copies, self.packed, self.cut = dims, copies, packed, cut
        self.place = place_of(dims)
        self.along, self.other = peers_of(dims, self.place)
        z, y, x, mp = self.place
        self.p, self.a1, self.b1, self.ra1, self.rb1, self.ra2, self.rb2, self.f, self.rz = bufs
        low, high = pl.ds(0, cut), pl.ds(cut, packed.shape[-1] - cut)
        along = self.along
        copies.plan(tag + "pair", [lambda: (packed.at[1 - mp], self.p, self.other)])
        copies.plan(tag + "1l", [
            lambda o=o, c=c, d=d: (self.p.at[EVERY, EVERY, c, EVERY, low], self.ra1.at[o], d)
            for o, (c, d) in enumerate(along["x"])
        ])
        copies.plan(tag + "1h", [
            lambda o=o, b=b, d=d: (self.p.at[EVERY, b, EVERY, EVERY, high], self.rb1.at[o], d)
            for o, (b, d) in enumerate(along["y"])
        ])
        copies.plan(tag + "2l", [
            lambda o=o, b=b, d=d: (self.a1.at[EVERY, b], self.ra2.at[o], d)
            for o, (b, d) in enumerate(along["y"])
        ])
        copies.plan(tag + "2h", [
            lambda o=o, c=c, d=d: (self.b1.at[EVERY, c], self.rb2.at[o], d)
            for o, (c, d) in enumerate(along["x"])
        ])
        copies.plan(tag + "3", [
            lambda o=o, a=a, d=d: (self.f.at[a], self.rz.at[o], d)
            for o, (a, d) in enumerate(along["z"])
        ])

    @staticmethod
    def count(dims):
        nz, ny, nx = dims
        return 1 + 2 * (ny - 1) + 2 * (nx - 1) + nz - 1

    @staticmethod
    def scratch(dims, rows, width, cut):
        nz, ny, nx = dims

        def buf(w, *shape):
            return pltpu.VMEM((*shape, rows, w), BF)

        rest = width - cut
        return [
            buf(width, nz, ny, nx), buf(cut, nz, ny), buf(rest, nz, nx),
            buf(cut, nx - 1, nz, ny), buf(rest, ny - 1, nz, nx),
            buf(cut, ny - 1, nz), buf(rest, nx - 1, nz), buf(width, nz), buf(width, nz - 1),
        ]

    def add_pair(self, mine):
        nz, ny, nx = self.dims
        for i in range(nz):
            for j in range(ny):
                for k in range(nx):
                    total = mine[i, j, k].astype(F32) + self.p[i, j, k].astype(F32)
                    self.p[i, j, k] = total.astype(BF)

    def add_first_low(self):
        nz, ny, nx = self.dims
        x = self.place[2]
        for i in range(nz):
            for j in range(ny):
                total = self.p[i, j, x, :, : self.cut].astype(F32)
                for o in range(nx - 1):
                    total = total + self.ra1[o, i, j].astype(F32)
                self.a1[i, j] = total.astype(BF)

    def add_first_high(self):
        nz, ny, nx = self.dims
        y = self.place[1]
        for i in range(nz):
            for k in range(nx):
                total = self.p[i, y, k, :, self.cut :].astype(F32)
                for o in range(ny - 1):
                    total = total + self.rb1[o, i, k].astype(F32)
                self.b1[i, k] = total.astype(BF)

    def add_second(self):
        nz, ny, nx = self.dims
        _, y, x, _ = self.place
        for i in range(nz):
            total = self.a1[i, y].astype(F32)
            for o in range(ny - 1):
                total = total + self.ra2[o, i].astype(F32)
            self.f[i, :, : self.cut] = total.astype(BF)
            total = self.b1[i, x].astype(F32)
            for o in range(nx - 1):
                total = total + self.rb2[o, i].astype(F32)
            self.f[i, :, self.cut :] = total.astype(BF)

    def add_third(self):
        total = self.f[self.place[0]].astype(F32)
        for o in range(self.dims[0] - 1):
            total = total + self.rz[o].astype(F32)
        return total


def backward_kernel(
    dims, n, qkv_ref, e_ref, mixed_ref, linv_ref, gmix_ref, normed_ref, inv_ref, gres_ref, w_ref,
    vec_ref, dvec2_ref, dbup_ref, packed, gtok_ref, narrow_ref, wide_ref, total_ref, *refs,
):
    g_ref, acc_ref, gsum_ref, ds_ref, go_ref, narrow, sums, vs, vr = refs[:9]
    wide_bufs, mine, narrow_bufs = refs[9:18], refs[18], refs[19:28]
    send, recv, sem = refs[28:]
    i = pl.program_id(0)
    steps = n // G
    copies = Copies(send, recv)
    wide = Reduction(dims, copies, "w", packed, wide_bufs, WIDE_CUT)
    thin = Reduction(dims, copies, "n", narrow, narrow_bufs, NARROW_CUT)
    mp = wide.place[3]
    keep = pltpu.make_async_copy(packed.at[mp], mine, sem)
    stages = [[wide.other], *([d for _, d in wide.along[axis]] for axis in "xyz")]
    bases = [sum(len(s) for s in stages[:k]) for k in range(4)]
    for k, devices in enumerate(stages):
        copies.plan("v%d" % k, [
            lambda k=k, o=o, d=d: (sums if k == 0 else vs.at[k - 1], vr.at[bases[k] + o], d)
            for o, d in enumerate(devices)
        ])

    def vec_add(k):
        total = sums[...] if k == 0 else vs[k - 1]
        for o in range(len(stages[k])):
            total = total + vr[bases[k] + o]
        if k < 3:
            vs[k] = total
        else:
            total_ref[...] = total

    @pl.when(i == 0)
    def _():
        greet(wide.along, wide.other)
        keep.start()
        acc_ref[...] = jnp.zeros_like(acc_ref)
        gsum_ref[...] = jnp.zeros_like(gsum_ref)
        met(wide.along)
        copies.start("wpair")

    @pl.when(i == 1)
    def _():
        keep.wait()
        copies.arrived("wpair")
        wide.add_pair(mine)
        copies.start("w1l", "w1h")

    @pl.when(i == steps // 2)
    def _():
        copies.arrived("w1l", "w1h")
        wide.add_first_low()
        wide.add_first_high()
        copies.start("w2l", "w2h")

    @pl.when(i == (3 * steps) // 4)
    def _():
        copies.arrived("w2l", "w2h")
        wide.add_second()
        copies.start("w3")

    @pl.when(i < steps)
    def _():
        lane = lax.broadcasted_iota(jnp.int32, (SP, 2 * HD), 1)
        zero = jnp.zeros((SP, 2 * HD), BF)
        minus = jnp.full((SP, 2 * HD), -1.0, BF)
        work = [(p, b) for p in range(PAIRS) for b in range(G)]

        def scores_grad(turn):
            p, b = work[turn]
            lo, hi = 2 * HD * p, 2 * HD * (p + 1)
            v = qkv_ref[b, :, 2 * D + lo : 2 * D + hi]
            go_f = gmix_ref[b, :, lo:hi].astype(F32) * linv_ref[b, :, lo:hi]
            go = go_f.astype(BF)
            go_ref[turn % 2] = go
            god = jnp.concatenate(
                [go, (go_f * mixed_ref[b, :, lo:hi].astype(F32)).astype(BF)], axis=1
            )
            for h in range(2):
                own = (lane < HD) if h == 0 else (lane >= HD)
                vd = jnp.concatenate(
                    [jnp.where(own, v, zero), jnp.where(own, minus, zero)], axis=1
                )
                ds_ref[turn % 2, h] = e_ref[b, 2 * p + h] * dot_nt(god, vd).astype(BF)

        def inputs_grad(turn):
            p, b = work[turn]
            lo, hi = 2 * HD * p, 2 * HD * (p + 1)
            q = qkv_ref[b, :, lo:hi]
            k = qkv_ref[b, :, D + lo : D + hi]
            go = go_ref[turn % 2]
            gq = gk = gv = None
            for h in range(2):
                own = (lane < HD) if h == 0 else (lane >= HD)
                ds = ds_ref[turn % 2, h]
                part_q = dot_nn(ds, jnp.where(own, k, zero))
                part_k = dot_tn(ds, jnp.where(own, q, zero))
                part_v = dot_tn(e_ref[b, 2 * p + h], jnp.where(own, go, zero))
                gq = part_q if gq is None else gq + part_q
                gk = part_k if gk is None else gk + part_k
                gv = part_v if gv is None else gv + part_v
            gq = gq * (1.0 / math.sqrt(HD))
            gk = gk * (1.0 / LOG2E)
            for j, grad in enumerate((gq, gk, gv)):
                gsum_ref[:, D * j + lo : D * j + hi] += fold(grad)
                g_ref[i, SP * b : SP * (b + 1), D * j + lo : D * j + hi] = grad.astype(BF)

        scores_grad(0)
        for turn in range(len(work)):
            if turn + 1 < len(work):
                scores_grad(turn + 1)
            inputs_grad(turn)
        acc_ref[...] += dot_tn(normed_ref[...].reshape(G * SP, D).astype(BF), g_ref[i])

    @pl.when(i == steps - 1)
    def _():
        nz, ny, nx = dims
        rows = narrow.shape[4]
        spots = [(a, b, c) for a in range(nz) for b in range(ny) for c in range(nx)]
        group = 48 // rows
        turned = vec_ref[...].T
        gsum = row_sum(gsum_ref[...])
        for t in range(len(spots) // group):
            at = slice(48 * t, 48 * (t + 1))
            dw = acc_ref[at, :] * turned[at, 0:1] + turned[at, 1:2] * gsum
            for m in range(2):
                parts = [dw[:, D * j + THIRD * m : D * j + THIRD * (m + 1)] for j in range(3)]
                parts.append(jnp.zeros((48, NARROW - 3 * THIRD), F32))
                block = jnp.concatenate(parts, axis=1)
                for k in range(group):
                    narrow[(m,) + spots[t * group + k]] = block[
                        k * rows : (k + 1) * rows
                    ].astype(BF)
        copies.start("npair")
        gains = [
            jnp.sum(
                acc_ref[c : c + 48, :] * w_ref[c : c + 48, :].astype(F32), axis=1, keepdims=True
            )
            for c in range(0, D, 48)
        ]
        high = gsum.astype(BF)
        low = (gsum - high.astype(F32)).astype(BF)
        row = lax.broadcasted_iota(jnp.int32, (16, 3 * D), 0)
        both = jnp.where(row == 0, high, jnp.where(row == 1, low, jnp.zeros((16, 3 * D), BF)))
        sums[0:1] = gsum[:, :D]
        sums[1:2] = gsum[:, 2 * D :]
        gain = jnp.broadcast_to(jnp.concatenate(gains, axis=0), (D, 128)).T
        sums[2:3] = gain[0:1, :]
        sums[3:4] = row_sum(dot_nt(both, w_ref[...]))
        sums[4:8] = dvec2_ref[0:4]
        for j in range(FF // D):
            sums[8 + j : 9 + j] = dbup_ref[:, D * j : D * (j + 1)]
        sums[12:16] = jnp.zeros((4, D), F32)
        copies.start("v0")

    @pl.when(i == steps + 2)
    def _():
        copies.arrived("npair", "v0")
        thin.add_pair(narrow.at[mp])
        vec_add(0)
        copies.start("n1l", "n1h", "v1")

    @pl.when(i == steps + 3)
    def _():
        copies.arrived("w3")
        wide_ref[...] = wide.add_third()

    @pl.when(i == steps + 4)
    def _():
        copies.arrived("n1l", "v1")
        thin.add_first_low()
        vec_add(1)
        copies.start("n2l", "v2")
        copies.arrived("n1h")
        thin.add_first_high()
        copies.start("n2h")

    @pl.when(i == steps + 6)
    def _():
        copies.arrived("n2l", "n2h", "v2")
        thin.add_second()
        vec_add(2)
        copies.start("n3", "v3")

    @pl.when(i >= steps)
    def _():
        group = jnp.maximum(i - steps, 0)
        gh1 = dot_nt(g_ref[group], w_ref[...])
        for b in range(G):
            parts = []
            for c in range(0, SP, CHUNK):
                at = slice(c, c + CHUNK)
                back = norm_backward(
                    gh1[SP * b + c : SP * b + c + CHUNK], normed_ref[b, at, :],
                    inv_ref[b, at, 0:1], vec_ref[0:1, :],
                )
                parts.append(gres_ref[b, at, :] + back)
            store_image(gtok_ref, G * group + b, jnp.concatenate(parts, axis=0))

    @pl.when(i == 2 * steps - 1)
    def _():
        copies.arrived("n3", "v3")
        narrow_ref[...] = thin.add_third()
        vec_add(3)
        copies.left(*copies.groups)


def backward(qkv, e, mixed, linv, gmix, normed, inv, gres, wqkv, vec, dvec2, dbup, packed, tall, dp):
    dims = chip_grid(dp)
    nz, ny, nx = dims
    n = qkv.shape[0]
    steps = n // G
    rows = D // dp
    count = 2 * Reduction.count(dims) + nz + ny + nx - 2

    def heads(*shape):
        return pl.BlockSpec((G, *shape), lambda i: (jnp.minimum(i, steps - 1),) + (0,) * len(shape))

    def after(*shape):
        return pl.BlockSpec((G, *shape), lambda i: (jnp.maximum(i - steps, 0),) + (0,) * len(shape))

    def twice(*shape):
        return pl.BlockSpec((G, *shape), lambda i: (i % steps,) + (0,) * len(shape))

    return pl.pallas_call(
        functools.partial(backward_kernel, dims, n),
        grid=(2 * steps,),
        in_specs=[
            heads(SP, 3 * D), heads(HEADS, SP, SP), heads(SP, D), heads(SP, D), heads(SP, D),
            twice(SP, D), after(SP, 128), after(SP, D), whole((D, 3 * D)), whole((8, D)),
            whole((8, D)), whole((1, FF)), pl.BlockSpec(memory_space=pl.ANY),
        ],
        out_specs=[
            whole((tall, D)), whole((rows, NARROW)), whole((rows, WIDE)), whole((16, D)),
        ],
        out_shape=[
            jax.ShapeDtypeStruct((tall, D), F32),
            jax.ShapeDtypeStruct((rows, NARROW), F32),
            jax.ShapeDtypeStruct((rows, WIDE), F32),
            jax.ShapeDtypeStruct((16, D), F32),
        ],
        scratch_shapes=[
            pltpu.VMEM((steps, G * SP, 3 * D), BF),
            pltpu.VMEM((D, 3 * D), F32),
            pltpu.VMEM((8, 3 * D), F32),
            pltpu.VMEM((2, 2, SP, SP), BF),
            pltpu.VMEM((2, SP, 2 * HD), BF),
            pltpu.VMEM((2, *dims, rows, NARROW), BF),
            pltpu.VMEM((16, D), F32),
            pltpu.VMEM((3, 16, D), F32),
            pltpu.VMEM((nz + ny + nx - 2, 16, D), F32),
            *Reduction.scratch(dims, rows, WIDE, WIDE_CUT),
            pltpu.VMEM((*dims, rows, WIDE), BF),
            *Reduction.scratch(dims, rows, NARROW, NARROW_CUT),
            pltpu.SemaphoreType.DMA((count,)),
            pltpu.SemaphoreType.DMA((count,)),
            pltpu.SemaphoreType.DMA,
        ],
        compiler_params=params(collective_id=1),
        name="backward",
    )(qkv, e, mixed, linv, gmix, normed, inv, gres, wqkv, vec, dvec2, dbup, packed)


def split_kernel(n, gtok_in, narrow_ref, wide_ref, vec_ref, gtok_ref, *outs):
    gtok_ref[...] = gtok_in[...]

    @pl.when(pl.program_id(0) == 0)
    def _():
        for j in range(3):
            outs[j][...] = narrow_ref[:, THIRD * j : THIRD * (j + 1)]
        outs[3][...] = wide_ref[:, :THIRD]
        outs[4][...] = wide_ref[:, OUT_PAD : OUT_PAD + HALF]
        outs[5][...] = wide_ref[:, OUT_PAD + HALF :]
        index = lax.axis_index("dp") * 2 + lax.axis_index("mp")
        per = D // n
        vec = pltpu.roll(vec_ref[...], D - index * per, axis=1)
        for row, out in zip((2, 3, 0, 1, 4, 5, 6, 7), outs[6:]):
            out[...] = vec[row : row + 1, :per]
        wide = jnp.concatenate([vec_ref[8 + j : 9 + j, :] for j in range(FF // D)], axis=1)
        wide = pltpu.roll(jnp.broadcast_to(wide, (8, FF)), FF - index * (FF // n), axis=1)
        outs[14][...] = wide[0:1, : FF // n]


def split(gtok, narrow, wide, vec, n):
    rows = narrow.shape[0]
    tall = gtok.shape[0]
    shapes = [(rows, THIRD)] * 4 + [(rows, HALF)] * 2 + [(1, D // n)] * 8 + [(1, FF // n)]
    half = pl.BlockSpec((tall // 2, D), lambda i: (i, 0))
    return pl.pallas_call(
        functools.partial(split_kernel, n),
        grid=(2,),
        in_specs=[half] + [whole(a.shape) for a in (narrow, wide, vec)],
        out_specs=[half] + [whole(s) for s in shapes],
        out_shape=[jax.ShapeDtypeStruct(s, F32) for s in [(tall, D), *shapes]],
        compiler_params=params(),
        name="split",
    )(gtok, narrow, wide, vec)


def whole(shape):
    return pl.BlockSpec(shape, lambda i: (0,) * len(shape))


def per_image(*shape):
    return pl.BlockSpec((1, *shape), lambda i: (i,) + (0,) * len(shape))


def per_step(*shape):
    return pl.BlockSpec((G, *shape), lambda i: (i,) + (0,) * len(shape))


def params(collective_id=None):
    return pltpu.CompilerParams(
        dimension_semantics=("arbitrary",), vmem_limit_bytes=62 * 1024 * 1024,
        collective_id=collective_id, has_side_effects=collective_id is not None,
    )


def on_device(
    tokens, w_query, w_key, w_value, w_out, w_up, w_down, ln1_gain, ln1_bias, b_query, b_value,
    b_out, ln2_gain, ln2_bias, b_up, b_down, cotangent,
):
    dp = lax.axis_size("dp")
    vectors = (ln1_gain, ln1_bias, b_query, b_value, b_out, ln2_gain, ln2_bias, b_down)
    qkv, e, mixed, linv, normed, inv, tok, cot, wqkv, vec, bup, wide = attn_fwd(
        (w_query, w_key, w_value, w_out.T, w_up, w_down.T), [v[None] for v in vectors], b_up[None],
        tokens, cotangent, dp,
    )
    out, gres, gmix, packed, dvec2, dbup = mlp(
        tok, cot, mixed, wide.reshape(2, D, WIDE), vec, bup, tokens.shape[0], dp
    )
    gtok, narrow_sum, wide_sum, sums = backward(
        qkv, e, mixed, linv, gmix, normed, inv, gres, wqkv, vec, dvec2, dbup, packed,
        tokens.shape[0], dp,
    )
    gtok, *grads = split(gtok, narrow_sum, wide_sum, sums, dp * lax.axis_size("mp"))
    vecs = [v.reshape(-1) for v in grads[6:]]
    return (
        out, gtok, grads[0], grads[1], grads[2], grads[3].T, grads[4], grads[5].T,
        *vecs[:7], vecs[8], vecs[7],
    )


def solution(mesh):
    row, mat, tam, vec = P(("dp", "mp"), None), P("dp", "mp"), P("mp", "dp"), P("dp")
    part = P(("dp", "mp"))
    return jax.shard_map(
        on_device,
        mesh=mesh,
        in_specs=(row, mat, mat, mat, tam, mat, tam, *([vec] * 9), row),
        out_specs=(row, row, mat, mat, mat, tam, mat, tam, *([part] * 9)),
        check_vma=False,
    )
```
